8 devices in a mesh: dp: 1 (over z), sp: 8 (over y, x, core).
Axes of the slice: x: 2, y: 2, z: 1, core: 2. Of those that a mesh axis runs over, the one named last changes fastest.
Arguments:
- x_one: bfloat16 [512, 1792], P(('dp', 'sp'))
- seg_one: int32 [512], P(('dp', 'sp'))
- pos_one: int32 [512], P(('dp', 'sp'))
- x_two: bfloat16 [512, 1792], P(('dp', 'sp'))
- seg_two: int32 [512], P(('dp', 'sp'))
- pos_two: int32 [512], P(('dp', 'sp'))
- w_qdown: bfloat16 [1792, 384], replicated
- gain_q: bfloat16 [384], replicated
- w_qup: bfloat16 [384, 6144], replicated
- w_kvdown: bfloat16 [1792, 576], replicated
- gain_kv: bfloat16 [512], replicated
- w_kvup: bfloat16 [512, 8192], replicated
- w_out: bfloat16 [4096, 1792], replicated
Outputs:
- output 1: bfloat16 [512, 1792], P(('dp', 'sp'))
- output 2: bfloat16 [512, 1792], P(('dp', 'sp'))
All inputs are finite; a program needn't handle non-finite values.
Results may differ from the reference program's by a relative error of at most 0.0139461.
Values are sent between devices in bfloat16 or wider.
A program may use at most 1 GiB of HBM per device.

```python
import jax
import jax.numpy as jnp
from jax import lax

TOKENS = 512
D_MODEL = 1792
HEADS = 32
Q_LAT = 384
KV_LAT = 512
ROPE_DIM = 64
NOPE_DIM = 128
V_DIM = 128
PROMPTS = 2
QK_DIM = NOPE_DIM + ROPE_DIM
KV_DOWN = KV_LAT + ROPE_DIM
ROPE_BASE = 10000.0
NORM_EPS = 1e-6


def draw_layout(draw_key):
    shuffled = jax.random.permutation(draw_key, TOKENS - 1) + 1
    cut_points = jnp.sort(shuffled[:PROMPTS - 1]).astype(jnp.int32)
    tok_index = jnp.arange(TOKENS, dtype=jnp.int32)
    prompt_ids = jnp.searchsorted(cut_points, tok_index, side='right').astype(jnp.int32)
    prompt_start = jnp.concatenate([jnp.zeros((1,), jnp.int32), cut_points])
    return prompt_ids, tok_index - prompt_start[prompt_ids]


def normal_weight(draw_key, arr_shape, fan_in, scale_by):
    return (jax.random.normal(draw_key, arr_shape, jnp.float32) * scale_by * fan_in ** -0.5).astype(jnp.bfloat16)


def setup_inputs(seed: int = 0, part: int = 0) -> dict:
    part_keys = jax.random.split(jax.random.fold_in(jax.random.key(seed), part), 4)
    weight_keys = jax.random.split(jax.random.key(seed + 1), 7)
    seg_one, pos_one = draw_layout(part_keys[0])
    seg_two, pos_two = draw_layout(part_keys[1])
    return {
        'x_one': jax.random.normal(part_keys[2], (TOKENS, D_MODEL), jnp.float32).astype(jnp.bfloat16),
        'seg_one': seg_one,
        'pos_one': pos_one,
        'x_two': jax.random.normal(part_keys[3], (TOKENS, D_MODEL), jnp.float32).astype(jnp.bfloat16),
        'seg_two': seg_two,
        'pos_two': pos_two,
        'w_qdown': normal_weight(weight_keys[0], (D_MODEL, Q_LAT), D_MODEL, 1.0),
        'gain_q': jax.random.uniform(weight_keys[1], (Q_LAT,), jnp.float32, 0.5, 1.5).astype(jnp.bfloat16),
        'w_qup': normal_weight(weight_keys[2], (Q_LAT, HEADS * QK_DIM), Q_LAT, 1.0),
        'w_kvdown': normal_weight(weight_keys[3], (D_MODEL, KV_DOWN), D_MODEL, 1.0),
        'gain_kv': jax.random.uniform(weight_keys[4], (KV_LAT,), jnp.float32, 0.5, 1.5).astype(jnp.bfloat16),
        'w_kvup': normal_weight(weight_keys[5], (KV_LAT, HEADS * (NOPE_DIM + V_DIM)), KV_LAT, 1.0),
        'w_out': normal_weight(weight_keys[6], (HEADS * V_DIM, D_MODEL), HEADS * V_DIM, 2.0),
    }


def rms_scale(pre_norm, gain_vec):
    mean_sq = jnp.mean(pre_norm * pre_norm, axis=-1, keepdims=True)
    return (pre_norm * lax.rsqrt(mean_sq + NORM_EPS) * gain_vec.astype(jnp.float32)).astype(jnp.bfloat16)


def rope_tables(positions):
    half_dim = ROPE_DIM // 2
    inv_freq = ROPE_BASE ** (-jnp.arange(half_dim, dtype=jnp.float32) / half_dim)
    angles = positions.astype(jnp.float32)[..., None] * inv_freq
    return jnp.cos(angles), jnp.sin(angles)


def rope_rotate(rot_in, cos_tab, sin_tab):
    half_dim = ROPE_DIM // 2
    first_half = rot_in[..., :half_dim]
    second_half = rot_in[..., half_dim:]
    return jnp.concatenate([first_half * cos_tab - second_half * sin_tab, second_half * cos_tab + first_half * sin_tab], axis=-1)


def mla_block(tokens_in, prompt_ids, positions, w_qdown, gain_q, w_qup, w_kvdown, gain_kv, w_kvup, w_out):
    q_latent = rms_scale(jnp.dot(tokens_in, w_qdown, preferred_element_type=jnp.float32), gain_q)
    kv_raw = jnp.dot(tokens_in, w_kvdown, preferred_element_type=jnp.float32)
    kv_latent = rms_scale(kv_raw[:, :KV_LAT], gain_kv)
    cos_tab, sin_tab = rope_tables(positions)
    k_rope = rope_rotate(kv_raw[:, KV_LAT:], cos_tab, sin_tab).astype(jnp.bfloat16)
    allowed = (prompt_ids[:, None] == prompt_ids[None, :]) & (positions[None, :] <= positions[:, None])
    wq_heads = w_qup.reshape(Q_LAT, HEADS, QK_DIM).transpose(1, 0, 2)
    wkv_heads = w_kvup.reshape(KV_LAT, HEADS, NOPE_DIM + V_DIM).transpose(1, 0, 2)

    def one_head(head_weights):
        wq_head, wkv_head = head_weights
        q_head = jnp.dot(q_latent, wq_head, preferred_element_type=jnp.float32)
        q_nope = q_head[:, :NOPE_DIM].astype(jnp.bfloat16)
        q_rope = rope_rotate(q_head[:, NOPE_DIM:], cos_tab, sin_tab).astype(jnp.bfloat16)
        kv_head = jnp.dot(kv_latent, wkv_head, preferred_element_type=jnp.float32).astype(jnp.bfloat16)
        q_cat = jnp.concatenate([q_nope, q_rope], axis=1)
        k_cat = jnp.concatenate([kv_head[:, :NOPE_DIM], k_rope], axis=1)
        scores = jnp.dot(q_cat, k_cat.T, preferred_element_type=jnp.float32) * QK_DIM ** -0.5
        attn_prob = jax.nn.softmax(jnp.where(allowed, scores, -1e30), axis=-1).astype(jnp.bfloat16)
        return jnp.dot(attn_prob, kv_head[:, NOPE_DIM:], preferred_element_type=jnp.float32).astype(jnp.bfloat16)

    head_out = lax.map(one_head, (wq_heads, wkv_heads))
    attn_flat = head_out.transpose(1, 0, 2).reshape(TOKENS, HEADS * V_DIM)
    return jnp.dot(attn_flat, w_out, preferred_element_type=jnp.float32).astype(jnp.bfloat16)


def reference(x_one, seg_one, pos_one, x_two, seg_two, pos_two, w_qdown, gain_q, w_qup, w_kvdown, gain_kv, w_kvup, w_out):
    y_one = mla_block(x_one, seg_one, pos_one, w_qdown, gain_q, w_qup, w_kvdown, gain_kv, w_kvup, w_out)
    y_two = mla_block(x_two, seg_two, pos_two, w_qdown, gain_q, w_qup, w_kvdown, gain_kv, w_kvup, w_out)
    return (y_one, y_two)
```

```python
import jax
import jax.numpy as jnp
from jax import lax
from jax.experimental import pallas as pl
from jax.experimental.pallas import tpu as pltpu
from jax.sharding import PartitionSpec as P

MESH = pl.DeviceIdType.MESH
F32 = jnp.float32
BF16 = jnp.bfloat16

D_MODEL = 1792
Q_LAT = 384
KV_LAT = 512
ROPE = 64
NOPE = 128
HEADS = 16
BLK = 64
CHIP = 2 * BLK
TOK = 512
NCHIP = 4
LN_BASE = 9.210340371976184
EPS = 1e-6
SCALE2 = 192 ** -0.5 * 1.4426950408889634
NEG = -1e30
BIG = 3.0e38


def norm_rows(z, gain):
    ms = jnp.mean(z * z, axis=-1, keepdims=True)
    return (z * lax.rsqrt(ms + EPS) * gain.astype(F32)[None, :]).astype(BF16)


def body(x1, p1, x2, p2, wqd, gq, wqu, wkvd, gkv, wkvu, wo, y,
         xv, posv, wqd_v, gq_v, wqu_v, wkvd_v, gkv_v, wkvu_v, wo_v,
         kvlat, ropeb, qlat, tabs, qbuf, kvb, bias, oall, oin,
         lsem, ds, dr, fs, fr, qs, qr, os_, or_):
    sp = lax.axis_index("sp")
    dp = lax.axis_index("dp")
    k = lax.rem(sp, 2)
    c = lax.div(sp, 2)
    pk = 1 - k

    def dev(chip, core):
        return (dp, chip * 2 + core)

    partner = dev(c, pk)

    def local(src, dst, i):
        cp = pltpu.make_async_copy(src, dst, lsem.at[i])
        cp.start()
        return cp

    l_x1 = local(x1, xv.at[pl.ds(0, BLK)], 0)
    l_x2 = local(x2, xv.at[pl.ds(BLK, BLK)], 1)
    l_p1 = local(p1, posv.at[0], 2)
    l_p2 = local(p2, posv.at[1], 3)
    l_gkv = local(gkv, gkv_v, 4)
    l_wkvd = local(wkvd, wkvd_v, 5)
    l_gq = local(gq, gq_v, 6)
    l_wqd = local(wqd, wqd_v, 7)
    l_wkvu = [local(wkvu.at[:, pl.ds(pl.multiple_of(k * 4096 + i * 1024, 1024), 1024)], wkvu_v.at[i], 8 + i) for i in range(4)]
    l_wqu = [local(wqu.at[:, pl.ds(pl.multiple_of(k * 3072 + i * 768, 256), 768)], wqu_v.at[i], 12 + i) for i in range(4)]
    l_wo = [local(wo.at[pl.ds(i * 1024, 1024)], wo_v.at[pl.ds(i * 1024, 1024)], 16 + i) for i in range(4)]

    barrier = pltpu.get_barrier_semaphore()
    pl.semaphore_signal(barrier, inc=1, device_id=partner, device_id_type=MESH)
    for j in range(1, NCHIP):
        pl.semaphore_signal(barrier, inc=1, device_id=dev(lax.rem(c + j, NCHIP), k), device_id_type=MESH)

    for b in range(1, NCHIP):
        @pl.when(c < b)
        def _():
            ropeb[pl.ds(b * CHIP, CHIP)] = jnp.zeros((CHIP, 128), BF16)

            def zero(h, _):
                for mb in range(2):
                    kvb[mb, h, pl.ds(b * CHIP, CHIP)] = jnp.zeros((CHIP, 256), BF16)
                return 0
            lax.fori_loop(0, HEADS, zero, 0)

    lane = lax.broadcasted_iota(jnp.int32, (1, 128), 1)
    lo64 = lane < 64
    lo32 = lax.rem(lane, 64) < 32

    l_p1.wait()
    l_p2.wait()
    own = pl.ds(pl.multiple_of(k * CHIP, CHIP), CHIP)
    eye = lax.broadcasted_iota(jnp.int32, (BLK, BLK), 0) == lax.broadcasted_iota(jnp.int32, (BLK, BLK), 1)
    cols = [jnp.sum(jnp.where(eye, posv[mb].astype(F32), 0.0), axis=1, keepdims=True) for mb in range(2)]
    pos_col = jnp.concatenate(cols, axis=0)
    freq = jnp.exp(lax.rem(lane, 32).astype(F32) * (-LN_BASE / 32))
    ang = pos_col * freq
    cos_t = jnp.cos(ang)
    sin_t = jnp.sin(ang)
    sin_t = jnp.where(lo32, -sin_t, sin_t)
    tabs[0, own] = cos_t
    tabs[1, own] = sin_t
    tabs[2, own] = pos_col + jnp.zeros((CHIP, 128), F32)

    def rot(z, cs, sn):
        sw = jnp.where(lo32, pltpu.roll(z, 96, 1), pltpu.roll(z, 32, 1))
        return z * cs + sw * sn

    with jax.named_scope("wait_x"):
        l_x1.wait()
        l_x2.wait()
        l_gkv.wait()
        l_wkvd.wait()
    u = lax.dot_general(xv[...], wkvd_v[...], (((1,), (1,)), ((), ())), preferred_element_type=F32)
    ckv = norm_rows(u[:, :KV_LAT], gkv_v[...])
    ur = u[:, KV_LAT:]
    kr = rot(jnp.concatenate([ur, ur], axis=1), cos_t, sin_t)
    kr = jnp.where(lo64, kr[:BLK], kr[BLK:]).astype(BF16)

    def rows(chip, core):
        return pl.ds(pl.multiple_of(chip * CHIP + core * BLK, BLK), BLK)

    def part(item, chip, core):
        r = rows(chip, core)
        return ropeb.at[r] if item == 0 else kvlat.at[item - 1, r]

    ropeb[rows(c, k)] = kr
    kvlat[0, rows(c, k)] = ckv[:BLK]
    kvlat[1, rows(c, k)] = ckv[BLK:]

    with jax.named_scope("barrier"):
        pl.semaphore_wait(barrier, 4)

    def direct(item, j):
        p = part(item, c, k)
        return pltpu.make_async_remote_copy(src_ref=p, dst_ref=p, send_sem=ds.at[item, j - 1], recv_sem=dr.at[item, c],
                                            device_id=dev(c + j, k), device_id_type=MESH)

    def direct_recv(item, chip):
        p = part(item, chip, k)
        return pltpu.make_async_remote_copy(src_ref=p, dst_ref=p, send_sem=ds.at[item, 0], recv_sem=dr.at[item, chip],
                                            device_id=partner, device_id_type=MESH)

    def forward(item, chip):
        p = part(item, chip, k)
        return pltpu.make_async_remote_copy(src_ref=p, dst_ref=p, send_sem=fs.at[item, chip], recv_sem=fr.at[item, chip],
                                            device_id=partner, device_id_type=MESH)

    def forward_recv(item, chip):
        p = part(item, chip, pk)
        return pltpu.make_async_remote_copy(src_ref=p, dst_ref=p, send_sem=fs.at[item, chip], recv_sem=fr.at[item, chip],
                                            device_id=partner, device_id_type=MESH)

    for item in range(3):
        for j in (3, 2, 1):
            @pl.when(c + j < NCHIP)
            def _():
                direct(item, j).start()
        forward(item, c).start()

    l_gq.wait()
    l_wqd.wait()
    with jax.named_scope("q_down"):
        qlat[own] = norm_rows(jnp.dot(xv[...], wqd_v[...], preferred_element_type=F32), gq_v[...])

    def q_copy(i, core):
        r = pl.ds(pl.multiple_of(core * CHIP, CHIP), CHIP)
        p = qlat.at[r] if i == 0 else tabs.at[:, r]
        return pltpu.make_async_remote_copy(src_ref=p, dst_ref=p, send_sem=qs.at[i], recv_sem=qr.at[i],
                                            device_id=partner, device_id_type=MESH)

    for i in range(2):
        q_copy(i, k).start()

    def kv_up(lhs, store):
        for i in range(4):
            kv = jnp.dot(lhs, wkvu_v[i], preferred_element_type=F32).astype(BF16)
            for h in range(4):
                store(i * 4 + h, kv[:, h * 256:(h + 1) * 256])

    def kv_up_device(core):
        r = rows(c, core)

        def store(h, val):
            kvb[0, h, r] = val[:BLK]
            kvb[1, h, r] = val[BLK:]
        kv_up(jnp.concatenate([kvlat[0, r], kvlat[1, r]], axis=0), store)

    def kv_up_chip(mb, chip):
        r = pl.ds(pl.multiple_of(chip * CHIP, CHIP), CHIP)

        def store(h, val):
            kvb[mb, h, r] = val
        kv_up(kvlat[mb, r], store)

    with jax.named_scope("wait_wkvu"):
        for cp in l_wkvu:
            cp.wait()
    with jax.named_scope("kv_own"):
        kv_up_device(k)
    for item in range(3):
        forward_recv(item, c).wait_recv()
    with jax.named_scope("kv_partner"):
        kv_up_device(pk)

    for i in range(2):
        q_copy(i, pk).wait_recv()
    for mb in range(2):
        for core in range(2):
            pos = tabs[2, pl.ds(core * CHIP + mb * BLK, BLK), 0:1].astype(jnp.int32)
            qi = c * CHIP + core * BLK + lax.broadcasted_iota(jnp.int32, (BLK, TOK), 0)
            ki = lax.broadcasted_iota(jnp.int32, (BLK, TOK), 1)
            keep = jnp.logical_and(ki <= qi, ki >= qi - pos)
            bias[mb, pl.ds(core * BLK, BLK)] = jnp.where(keep, BIG, NEG)
    for cp in l_wqu:
        cp.wait()

    def q_up(i, _):
        f = jnp.dot(qlat[...], wqu_v[i], preferred_element_type=F32)
        cs = tabs[0]
        sn = tabs[1]
        for pair in range(2):
            t0, t1, t2 = (f[:, pair * 384 + n * 128: pair * 384 + (n + 1) * 128] for n in range(3))
            n1 = pltpu.roll(jnp.where(lo64, t2, t1), 64, 1)
            r = rot(jnp.where(lo64, t1, t2), cs, sn)
            rw = pltpu.roll(r, 64, 1)
            nopes = (t0.astype(BF16), n1.astype(BF16))
            zero = jnp.zeros_like(r)
            ropes = ((jnp.where(lo64, r, zero).astype(BF16), jnp.where(lo64, rw, zero).astype(BF16)),
                     (jnp.where(lo64, zero, rw).astype(BF16), jnp.where(lo64, zero, r).astype(BF16)))
            for odd in range(2):
                h = i * 4 + pair * 2 + odd
                for mb in range(2):
                    for core in range(2):
                        s = slice(core * CHIP + mb * BLK, core * CHIP + (mb + 1) * BLK)
                        qbuf[mb, h, pl.ds(core * BLK, BLK), 0:128] = nopes[odd][s]
                        qbuf[mb, h, pl.ds(core * BLK, BLK), 128:256] = ropes[mb][odd][s]
        return 0
    with jax.named_scope("q_up"):
        lax.fori_loop(0, 4, q_up, 0)

    def pass_on(items):
        def step(j, _):
            for item in items:
                direct_recv(item, c - j).wait_recv()
                forward(item, c - j).start()
            return 0
        lax.fori_loop(1, c + 1, step, 0)

    def take(mb, items):
        def step(j, _):
            for item in items:
                forward_recv(item, c - j).wait_recv()
            kv_up_chip(mb, c - j)
            return 0
        lax.fori_loop(1, c + 1, step, 0)

    def head(mb, h):
        kv = kvb[mb, h]
        kcat = jnp.concatenate([kv[:, :NOPE], ropeb[...]], axis=1)
        s = lax.dot_general(qbuf[mb, h], kcat, (((1,), (1,)), ((), ())), preferred_element_type=F32)
        s = jnp.minimum(s, bias[mb])
        m = jnp.max(s, axis=1, keepdims=True)
        e = jnp.exp2((s - m) * SCALE2)
        p = (e * (1.0 / jnp.sum(e, axis=1, keepdims=True))).astype(BF16)
        return jnp.dot(p, kv[:, NOPE:], preferred_element_type=F32).astype(BF16)

    def heads(mb, lo, hi):
        def step(i, _):
            for u_ in range(2):
                h = i * 2 + u_
                oall[mb, :, pl.ds(pl.multiple_of(h * 128, 128), 128)] = head(mb, h)
            return 0
        lax.fori_loop(lo // 2, hi // 2, step, 0)

    def o_copy(mb, half, core):
        cs = pl.ds(half * 1024, 1024)
        return pltpu.make_async_remote_copy(
            src_ref=oall.at[mb, pl.ds(pl.multiple_of(core * BLK, BLK), BLK), cs],
            dst_ref=oin.at[pl.ds(mb * BLK, BLK), cs],
            send_sem=os_.at[mb, half], recv_sem=or_.at[mb, half], device_id=partner, device_id_type=MESH)

    with jax.named_scope("pass1"):
        pass_on((0, 1))
    with jax.named_scope("take1"):
        take(0, (0, 1))
    with jax.named_scope("heads1a"):
        heads(0, 0, 8)
    with jax.named_scope("pass2"):
        pass_on((2,))
    o_copy(0, 0, pk).start()
    with jax.named_scope("heads1b"):
        heads(0, 8, 16)
    o_copy(0, 1, pk).start()
    with jax.named_scope("take2"):
        take(1, (2,))
    with jax.named_scope("heads2a"):
        heads(1, 0, 8)
    o_copy(1, 0, pk).start()
    with jax.named_scope("heads2b"):
        heads(1, 8, 16)
    o_copy(1, 1, pk).start()

    with jax.named_scope("wait_wo"):
        for cp in l_wo:
            cp.wait()
    orow = pl.ds(pl.multiple_of(k * BLK, BLK), BLK)
    mine = jnp.concatenate([oall[0, orow], oall[1, orow]], axis=0)
    w_mine = pl.ds(pl.multiple_of(k * 2048, 2048), 2048)
    w_other = pl.ds(pl.multiple_of(pk * 2048, 2048), 2048)
    with jax.named_scope("out_mine"):
        acc = jnp.dot(mine, wo_v[w_mine], preferred_element_type=F32)
    for mb in range(2):
        for half in range(2):
            o_copy(mb, half, pk).wait_recv()
    with jax.named_scope("out_other"):
        acc = acc + jnp.dot(oin[...], wo_v[w_other], preferred_element_type=F32)
    y[...] = acc.astype(BF16)

    for item in range(3):
        for j in (3, 2, 1):
            @pl.when(c + j < NCHIP)
            def _():
                direct(item, j).wait_send()

        def drain(j, _):
            forward(item, c - j).wait_send()
            return 0
        lax.fori_loop(0, c + 1, drain, 0)
    for i in range(2):
        q_copy(i, k).wait_send()
    for mb in range(2):
        for half in range(2):
            o_copy(mb, half, pk).wait_send()


def store_body(y, y1, y2, sem):
    for i, out in enumerate((y1, y2)):
        pltpu.make_async_copy(y.at[pl.ds(i * BLK, BLK)], out, sem.at[i]).start()
    for i, out in enumerate((y1, y2)):
        pltpu.make_async_copy(y.at[pl.ds(i * BLK, BLK)], out, sem.at[i]).wait()


def store(y):
    any_spec = pl.BlockSpec(memory_space=pl.ANY)
    return pl.pallas_call(
        store_body,
        out_shape=(jax.ShapeDtypeStruct((BLK, D_MODEL), BF16),) * 2,
        in_specs=[any_spec],
        out_specs=(any_spec,) * 2,
        scratch_shapes=[pltpu.SemaphoreType.DMA((2,))],
        compiler_params=pltpu.CompilerParams(vmem_limit_bytes=2**20),
    )(y)


def solution(mesh):
    tok_spec = P(('dp', 'sp'), None)
    idx_spec = P(('dp', 'sp'))
    any_spec = pl.BlockSpec(memory_space=pl.ANY)
    vmem_spec = pl.BlockSpec(memory_space=pltpu.VMEM)

    def local_body(x_one, seg_one, pos_one, x_two, seg_two, pos_two, w_qdown, gain_q, w_qup, w_kvdown, gain_kv, w_kvup, w_out):
        dma = pltpu.SemaphoreType.DMA
        call = pl.pallas_call(
            body,
            out_shape=jax.ShapeDtypeStruct((CHIP, D_MODEL), BF16),
            in_specs=[pl.BlockSpec(memory_space=pltpu.HBM)] * 11,
            out_specs=vmem_spec,
            scratch_shapes=[
                pltpu.VMEM((CHIP, D_MODEL), BF16),
                pltpu.VMEM((2, 1, BLK), jnp.int32),
                pltpu.VMEM((D_MODEL, Q_LAT), BF16),
                pltpu.VMEM((Q_LAT,), BF16),
                pltpu.VMEM((4, Q_LAT, 768), BF16),
                pltpu.VMEM((KV_LAT + ROPE, D_MODEL), BF16),
                pltpu.VMEM((KV_LAT,), BF16),
                pltpu.VMEM((4, KV_LAT, 1024), BF16),
                pltpu.VMEM((4096, D_MODEL), BF16),
                pltpu.VMEM((2, TOK, KV_LAT), BF16),
                pltpu.VMEM((TOK, 128), BF16),
                pltpu.VMEM((2 * CHIP, Q_LAT), BF16),
                pltpu.VMEM((3, 2 * CHIP, 128), F32),
                pltpu.VMEM((2, HEADS, CHIP, 256), BF16),
                pltpu.VMEM((2, HEADS, TOK, 256), BF16),
                pltpu.VMEM((2, CHIP, TOK), F32),
                pltpu.VMEM((2, CHIP, 2048), BF16),
                pltpu.VMEM((CHIP, 2048), BF16),
                dma((20,)), dma((3, 3)), dma((3, 4)), dma((3, 4)), dma((3, 4)),
                dma((2,)), dma((2,)), dma((2, 2)), dma((2, 2)),
            ],
            compiler_params=pltpu.CompilerParams(collective_id=0, has_side_effects=True, vmem_limit_bytes=48 * 2**20),
        )
        args = (x_one, pos_one.reshape(1, BLK), x_two, pos_two.reshape(1, BLK), w_qdown, gain_q, w_qup,
                w_kvdown.T, gain_kv, w_kvup, w_out)
        y = call(*(pltpu.with_memory_space_constraint(a, pltpu.HBM) for a in args))
        return store(y)

    return jax.shard_map(local_body, mesh=mesh,
                         in_specs=(tok_spec, idx_spec, idx_spec, tok_spec, idx_spec, idx_spec, P(), P(), P(), P(), P(), P(), P()),
                         out_specs=(tok_spec, tok_spec), check_vma=False)
```

```python
import jax
import jax.numpy as jnp
from jax import lax
from jax.experimental import pallas as pl
from jax.experimental.pallas import tpu as pltpu
from jax.sharding import PartitionSpec as P

MESH = pl.DeviceIdType.MESH
F32 = jnp.float32
BF16 = jnp.bfloat16

D_MODEL = 1792
Q_LAT = 384
KV_LAT = 512
ROPE = 64
NOPE = 128
HEADS = 16
BLK = 64
CHIP = 2 * BLK
TOK = 512
NCHIP = 4
LN_BASE = 9.210340371976184
EPS = 1e-6
SCALE2 = 192 ** -0.5 * 1.4426950408889634
NEG = -1e30
BIG = 3.0e38


def norm_rows(z, gain):
    ms = jnp.mean(z * z, axis=-1, keepdims=True)
    return (z * lax.rsqrt(ms + EPS) * gain.astype(F32)[None, :]).astype(BF16)


def body(x1, p1, x2, p2, wqd, gq, wqu, wkvd, gkv, wkvu, wo, y,
         xv, posv, wqd_v, gq_v, wqu_v, wkvd_v, gkv_v, wkvu_v, wo_v,
         kvlat0, kvlat1, qlat, tabs, qbuf, kvb, krope, bias, oall, oin, acc,
         lsem, ds, dr, fs, fr, qs, qr, os_, or_):
    kvlat = (kvlat0, kvlat1)
    sp = lax.axis_index("sp")
    dp = lax.axis_index("dp")
    k = lax.rem(sp, 2)
    c = lax.div(sp, 2)
    pk = 1 - k

    def dev(chip, core):
        return (dp, chip * 2 + core)

    partner = dev(c, pk)

    def local(src, dst, i):
        cp = pltpu.make_async_copy(src, dst, lsem.at[i])
        cp.start()
        return cp

    l_x1 = local(x1, xv.at[pl.ds(0, BLK)], 0)
    l_x2 = local(x2, xv.at[pl.ds(BLK, BLK)], 1)
    l_p1 = local(p1, posv.at[0], 2)
    l_p2 = local(p2, posv.at[1], 3)
    l_gkv = local(gkv, gkv_v, 4)
    l_wkvd = [local(wkvd.at[pl.ds(a, n)], wkvd_v.at[pl.ds(a, n)], i) for a, n, i in ((256, 320, 5), (0, 256, 20))]
    l_gq = local(gq, gq_v, 6)
    l_wqd = local(wqd, wqd_v, 7)
    l_wkvu = [local(wkvu.at[:, pl.ds(pl.multiple_of(k * 4096 + i * 1024, 1024), 1024)], wkvu_v.at[i], 8 + i) for i in range(4)]
    l_wqu = [local(wqu.at[:, pl.ds(pl.multiple_of(k * 3072 + i * 768, 256), 768)], wqu_v.at[i], 12 + i) for i in range(4)]
    l_wo = [local(wo.at[pl.ds(pl.multiple_of(lax.rem(k * 2048 + i * 1024, 4096), 1024), 1024)], wo_v.at[pl.ds(i * 1024, 1024)], 16 + i) for i in range(4)]

    barrier = pltpu.get_barrier_semaphore()
    pl.semaphore_signal(barrier, inc=1, device_id=partner, device_id_type=MESH)
    for j in range(1, NCHIP):
        pl.semaphore_signal(barrier, inc=1, device_id=dev(lax.rem(c + j, NCHIP), k), device_id_type=MESH)

    for b in range(1, NCHIP):
        @pl.when(c < b)
        def _():
            kvlat0[pl.ds(b * CHIP, CHIP), KV_LAT:] = jnp.zeros((CHIP, 128), BF16)
            kvlat1[pl.ds(b * CHIP, CHIP)] = jnp.zeros((CHIP, KV_LAT), BF16)

            def zero(h, _):
                for mb in range(2):
                    kvb[mb, h, pl.ds(b * CHIP, CHIP)] = jnp.zeros((CHIP, 256), BF16)
                return 0
            lax.fori_loop(0, HEADS, zero, 0)

    lane = lax.broadcasted_iota(jnp.int32, (1, 128), 1)
    lo64 = lane < 64
    lo32 = lax.rem(lane, 64) < 32

    l_p1.wait()
    l_p2.wait()
    own = pl.ds(pl.multiple_of(k * CHIP, CHIP), CHIP)
    eye = lax.broadcasted_iota(jnp.int32, (BLK, BLK), 0) == lax.broadcasted_iota(jnp.int32, (BLK, BLK), 1)
    cols = [jnp.sum(jnp.where(eye, posv[mb].astype(F32), 0.0), axis=1, keepdims=True) for mb in range(2)]
    pos_col = jnp.concatenate(cols, axis=0)
    freq = jnp.exp(lax.rem(lane, 32).astype(F32) * (-LN_BASE / 32))
    ang = pos_col * freq
    cos_t = jnp.cos(ang)
    sin_t = jnp.sin(ang)
    sin_t = jnp.where(lo32, -sin_t, sin_t)
    tabs[0, own] = cos_t
    tabs[1, own] = sin_t
    tabs[2, own] = pos_col + jnp.zeros((CHIP, 128), F32)

    def rot(z, cs, sn):
        sw = jnp.where(lo32, pltpu.roll(z, 96, 1), pltpu.roll(z, 32, 1))
        return z * cs + sw * sn

    with jax.named_scope("wait_x"):
        l_x1.wait()
        l_x2.wait()
        l_gkv.wait()
        l_wkvd[0].wait()

    def kv_down(a, n):
        return lax.dot_general(xv[...], wkvd_v[a:a + n], (((1,), (1,)), ((), ())), preferred_element_type=F32)

    u_b = kv_down(256, 320)
    l_wkvd[1].wait()
    u_a = kv_down(0, 256)
    ur = u_b[:, 256:]
    kr = rot(jnp.concatenate([ur, ur], axis=1), cos_t, sin_t)
    kr = jnp.where(lo64, kr[:BLK], kr[BLK:]).astype(BF16)

    ckv = norm_rows(jnp.concatenate([u_a, u_b[:, :256]], axis=1), gkv_v[...])

    def rows(chip, core):
        return pl.ds(pl.multiple_of(chip * CHIP + core * BLK, BLK), BLK)

    def part(item, chip, core):
        return kvlat[item].at[rows(chip, core)]

    kvlat[0][rows(c, k), KV_LAT:] = kr
    kvlat[0][rows(c, k), :KV_LAT] = ckv[:BLK]
    kvlat[1][rows(c, k)] = ckv[BLK:]

    with jax.named_scope("barrier"):
        pl.semaphore_wait(barrier, 4)

    def direct(item, j):
        p = part(item, c, k)
        return pltpu.make_async_remote_copy(src_ref=p, dst_ref=p, send_sem=ds.at[item, j - 1], recv_sem=dr.at[item, c],
                                            device_id=dev(c + j, k), device_id_type=MESH)

    def direct_recv(item, chip):
        p = part(item, chip, k)
        return pltpu.make_async_remote_copy(src_ref=p, dst_ref=p, send_sem=ds.at[item, 0], recv_sem=dr.at[item, chip],
                                            device_id=partner, device_id_type=MESH)

    def forward(item, chip):
        p = part(item, chip, k)
        return pltpu.make_async_remote_copy(src_ref=p, dst_ref=p, send_sem=fs.at[item, chip], recv_sem=fr.at[item, chip],
                                            device_id=partner, device_id_type=MESH)

    def forward_recv(item, chip):
        p = part(item, chip, pk)
        return pltpu.make_async_remote_copy(src_ref=p, dst_ref=p, send_sem=fs.at[item, chip], recv_sem=fr.at[item, chip],
                                            device_id=partner, device_id_type=MESH)

    def send(item):
        for j in (3, 2, 1):
            @pl.when(c + j < NCHIP)
            def _():
                direct(item, j).start()

    send(0)
    for item in range(2):
        forward(item, c).start()

    l_gq.wait()
    l_wqd.wait()
    with jax.named_scope("q_down"):
        qlat[own] = norm_rows(jnp.dot(xv[...], wqd_v[...], preferred_element_type=F32), gq_v[...])

    def q_copy(i, core):
        r = pl.ds(pl.multiple_of(core * CHIP, CHIP), CHIP)
        p = qlat.at[r] if i == 0 else tabs.at[:, r]
        return pltpu.make_async_remote_copy(src_ref=p, dst_ref=p, send_sem=qs.at[i], recv_sem=qr.at[i],
                                            device_id=partner, device_id_type=MESH)

    for i in range(2):
        q_copy(i, k).start()

    def kv_up(lhs, store):
        for i in range(4):
            kv = jnp.dot(lhs, wkvu_v[i], preferred_element_type=F32).astype(BF16)
            for h in range(4):
                store(i * 4 + h, kv[:, h * 256:(h + 1) * 256])

    def chip_rows(chip):
        return pl.ds(pl.multiple_of(chip * CHIP, CHIP), CHIP)

    def kv_up_own():
        r = chip_rows(c)

        def store(h, val):
            kvb[0, h, r] = val[:CHIP]
            kvb[1, h, r] = val[CHIP:]
        kv_up(jnp.concatenate([kvlat0[r, :KV_LAT], kvlat1[r]], axis=0), store)

    def kv_up_rows(mb, r):
        def store(h, val):
            kvb[mb, h, r] = val
        kv_up(kvlat[mb][r, :KV_LAT], store)

    with jax.named_scope("wait_wkvu"):
        for cp in l_wkvu:
            cp.wait()
    with jax.named_scope("wait_partner"):
        for item in range(2):
            forward_recv(item, c).wait_recv()
    with jax.named_scope("kv_own"):
        kv_up_own()
    send(1)

    for i in range(2):
        q_copy(i, pk).wait_recv()
    for mb in range(2):
        for core in range(2):
            pos = tabs[2, pl.ds(core * CHIP + mb * BLK, BLK), 0:1].astype(jnp.int32)
            qi = c * CHIP + core * BLK + lax.broadcasted_iota(jnp.int32, (BLK, TOK), 0)
            ki = lax.broadcasted_iota(jnp.int32, (BLK, TOK), 1)
            keep = jnp.logical_and(ki <= qi, ki >= qi - pos)
            bias[mb, pl.ds(core * BLK, BLK)] = jnp.where(keep, BIG, NEG)
    for cp in l_wqu:
        cp.wait()

    def q_up(i):
        return jnp.dot(qlat[...], wqu_v[i], preferred_element_type=F32)

    def q_store(i, f):
        for pair in range(2):
            t0, t1, t2 = (f[:, pair * 384 + n * 128: pair * 384 + (n + 1) * 128] for n in range(3))
            n1 = pltpu.roll(jnp.where(lo64, t2, t1), 64, 1)
            r = rot(jnp.where(lo64, t1, t2), tabs[0], tabs[1])
            zero = jnp.zeros_like(r)
            q = ((t0.astype(BF16), jnp.where(lo64, r, zero).astype(BF16)),
                 (n1.astype(BF16), jnp.where(lo64, zero, r).astype(BF16)))
            for odd in range(2):
                h = i * 4 + pair * 2 + odd
                for mb in range(2):
                    for core in range(2):
                        s = slice(core * CHIP + mb * BLK, core * CHIP + (mb + 1) * BLK)
                        for n in range(2):
                            qbuf[mb, h, pl.ds(core * BLK, BLK), n * 128:(n + 1) * 128] = q[odd][n][s]

    with jax.named_scope("q_up"):
        prev = q_up(0)
        for i in range(4):
            nxt = q_up(i + 1) if i < 3 else None
            q_store(i, prev)
            prev = nxt

    def each_earlier_chip(step):
        lax.fori_loop(1, c + 1, lambda j, _: (step(c - j), 0)[1], 0)

    def pass_on(item):
        def step(chip):
            direct_recv(item, chip).wait_recv()
            forward(item, chip).start()
        each_earlier_chip(step)

    def spread_rope():
        r = kvlat0[:, KV_LAT:]
        krope[0] = jnp.concatenate([r[:, :ROPE], r[:, :ROPE]], axis=1)
        krope[1] = jnp.concatenate([r[:, ROPE:], r[:, ROPE:]], axis=1)

    def heads(mb):
        scores = []
        for h in range(HEADS):
            kcat = jnp.concatenate([kvb[mb, h, :, :NOPE], krope[mb]], axis=1)
            scores.append(lax.dot_general(qbuf[mb, h], kcat, (((1,), (1,)), ((), ())), preferred_element_type=F32))
        probs = []
        for s in scores:
            s = jnp.minimum(s, bias[mb])
            m = jnp.max(s, axis=1, keepdims=True)
            e = jnp.exp2((s - m) * SCALE2)
            probs.append((e * (1.0 / jnp.sum(e, axis=1, keepdims=True))).astype(BF16))
        for h in range(HEADS):
            o = jnp.dot(probs[h], kvb[mb, h, :, NOPE:], preferred_element_type=F32)
            oall[mb, :, h * 128:(h + 1) * 128] = o.astype(BF16)

    def o_copy(mb, half, core):
        cs = pl.ds(half * 1024, 1024)
        return pltpu.make_async_remote_copy(
            src_ref=oall.at[mb, pl.ds(pl.multiple_of(core * BLK, BLK), BLK), cs],
            dst_ref=oin.at[pl.ds(mb * BLK, BLK), cs],
            send_sem=os_.at[mb, half], recv_sem=or_.at[mb, half], device_id=partner, device_id_type=MESH)

    with jax.named_scope("pass1"):
        pass_on(0)

    def take_one(chip):
        with jax.named_scope("take1_wait"):
            forward_recv(0, chip).wait_recv()
        with jax.named_scope("take1"):
            kv_up_rows(0, chip_rows(chip))
    each_earlier_chip(take_one)
    with jax.named_scope("pass2"):
        pass_on(1)
    spread_rope()
    with jax.named_scope("heads1"):
        heads(0)
    for half in range(2):
        o_copy(0, half, pk).start()
    with jax.named_scope("take2_wait"):
        each_earlier_chip(lambda chip: forward_recv(1, chip).wait_recv())
    with jax.named_scope("take2"):
        @pl.when(c > 0)
        def _():
            kv_up_rows(1, pl.ds(0, 3 * CHIP))
    with jax.named_scope("heads2"):
        heads(1)
    for half in range(2):
        o_copy(1, half, pk).start()

    with jax.named_scope("out"):
        for cp in l_wo:
            cp.wait()
        for mb, half in ((0, 0), (0, 1), (1, 0)):
            o_copy(mb, half, pk).wait_recv()
        orow = pl.ds(pl.multiple_of(k * BLK, BLK), BLK)
        mine = jnp.concatenate([oall[0, orow], oall[1, orow]], axis=0)
        acc[...] = jnp.dot(jnp.concatenate([mine, oin[:, :1024]], axis=1), wo_v[0:3072], preferred_element_type=F32)
    with jax.named_scope("out_last"):
        o_copy(1, 1, pk).wait_recv()
        y[...] = (acc[...] + jnp.dot(oin[:, 1024:], wo_v[3072:], preferred_element_type=F32)).astype(BF16)

    for item in range(2):
        for j in (3, 2, 1):
            @pl.when(c + j < NCHIP)
            def _():
                direct(item, j).wait_send()

        def drain(j, _):
            forward(item, c - j).wait_send()
            return 0
        lax.fori_loop(0, c + 1, drain, 0)
    for i in range(2):
        q_copy(i, k).wait_send()
    for mb in range(2):
        for half in range(2):
            o_copy(mb, half, pk).wait_send()


def store_body(y, y1, y2, sem):
    for i, out in enumerate((y1, y2)):
        pltpu.make_async_copy(y.at[pl.ds(i * BLK, BLK)], out, sem.at[i]).start()
    for i, out in enumerate((y1, y2)):
        pltpu.make_async_copy(y.at[pl.ds(i * BLK, BLK)], out, sem.at[i]).wait()


def store(y):
    any_spec = pl.BlockSpec(memory_space=pl.ANY)
    return pl.pallas_call(
        store_body,
        out_shape=(jax.ShapeDtypeStruct((BLK, D_MODEL), BF16),) * 2,
        in_specs=[any_spec],
        out_specs=(any_spec,) * 2,
        scratch_shapes=[pltpu.SemaphoreType.DMA((2,))],
        compiler_params=pltpu.CompilerParams(vmem_limit_bytes=2**20),
    )(y)


def solution(mesh):
    tok_spec = P(('dp', 'sp'), None)
    idx_spec = P(('dp', 'sp'))
    any_spec = pl.BlockSpec(memory_space=pl.ANY)
    vmem_spec = pl.BlockSpec(memory_space=pltpu.VMEM)

    def local_body(x_one, seg_one, pos_one, x_two, seg_two, pos_two, w_qdown, gain_q, w_qup, w_kvdown, gain_kv, w_kvup, w_out):
        dma = pltpu.SemaphoreType.DMA
        call = pl.pallas_call(
            body,
            out_shape=jax.ShapeDtypeStruct((CHIP, D_MODEL), BF16),
            in_specs=[pl.BlockSpec(memory_space=pltpu.HBM)] * 11,
            out_specs=vmem_spec,
            scratch_shapes=[
                pltpu.VMEM((CHIP, D_MODEL), BF16),
                pltpu.VMEM((2, 1, BLK), jnp.int32),
                pltpu.VMEM((D_MODEL, Q_LAT), BF16),
                pltpu.VMEM((Q_LAT,), BF16),
                pltpu.VMEM((4, Q_LAT, 768), BF16),
                pltpu.VMEM((KV_LAT + ROPE, D_MODEL), BF16),
                pltpu.VMEM((KV_LAT,), BF16),
                pltpu.VMEM((4, KV_LAT, 1024), BF16),
                pltpu.VMEM((4096, D_MODEL), BF16),
                pltpu.VMEM((TOK, KV_LAT + 128), BF16),
                pltpu.VMEM((TOK, KV_LAT), BF16),
                pltpu.VMEM((2 * CHIP, Q_LAT), BF16),
                pltpu.VMEM((3, 2 * CHIP, 128), F32),
                pltpu.VMEM((2, HEADS, CHIP, 256), BF16),
                pltpu.VMEM((2, HEADS, TOK, 256), BF16),
                pltpu.VMEM((2, TOK, 128), BF16),
                pltpu.VMEM((2, CHIP, TOK), F32),
                pltpu.VMEM((2, CHIP, 2048), BF16),
                pltpu.VMEM((CHIP, 2048), BF16),
                pltpu.VMEM((CHIP, D_MODEL), F32),
                dma((21,)), dma((2, 3)), dma((2, 4)), dma((2, 4)), dma((2, 4)),
                dma((2,)), dma((2,)), dma((2, 2)), dma((2, 2)),
            ],
            compiler_params=pltpu.CompilerParams(collective_id=0, has_side_effects=True, vmem_limit_bytes=52 * 2**20),
        )
        args = (x_one, pos_one.reshape(1, BLK), x_two, pos_two.reshape(1, BLK), w_qdown, gain_q, w_qup,
                w_kvdown.T, gain_kv, w_kvup, w_out)
        y = call(*(pltpu.with_memory_space_constraint(a, pltpu.HBM) for a in args))
        return store(y)

    return jax.shard_map(local_body, mesh=mesh,
                         in_specs=(tok_spec, idx_spec, idx_spec, tok_spec, idx_spec, idx_spec, P(), P(), P(), P(), P(), P(), P()),
                         out_specs=(tok_spec, tok_spec), check_vma=False)
```

```python
import jax
import jax.numpy as jnp
from jax import lax
from jax.experimental import pallas as pl
from jax.experimental.pallas import tpu as pltpu
from jax.sharding import PartitionSpec as P

MESH = pl.DeviceIdType.MESH
F32 = jnp.float32
BF16 = jnp.bfloat16

D_MODEL = 1792
Q_LAT = 384
KV_LAT = 512
ROPE = 64
NOPE = 128
HEADS = 16
BLK = 64
CHIP = 2 * BLK
TOK = 512
NCHIP = 4
LN_BASE = 9.210340371976184
EPS = 1e-6
LEAD = 4
K_A = 1024
SCALE2 = 192 ** -0.5 * 1.4426950408889634
NEG = -1e30
BIG = 3.0e38


def norm_rows(z, gain):
    ms = jnp.mean(z * z, axis=-1, keepdims=True)
    return (z * lax.rsqrt(ms + EPS) * gain.astype(F32)[None, :]).astype(BF16)


def body(x1, p1, x2, p2, wqd, gq, wqu, wkvd, gkv, wkvu, wo, y,
         xv, posv, wqd_v, gq_v, wqu_v, wkvd_v, gkv_v, wkvu_v, wo_v,
         kvlat0, kvlat1, qlat, tabs, qbuf, kheld, kT, vb, kropeT, bias, oall, oin, acc, usum,
         lsem, ds, dr, fs, fr, qs, qr, os_, or_):
    kvlat = (kvlat0, kvlat1)
    sp = lax.axis_index("sp")
    dp = lax.axis_index("dp")
    k = lax.rem(sp, 2)
    c = lax.div(sp, 2)
    pk = 1 - k

    def dev(chip, core):
        return (dp, chip * 2 + core)

    partner = dev(c, pk)

    def local(src, dst, i):
        cp = pltpu.make_async_copy(src, dst, lsem.at[i])
        cp.start()
        return cp

    local(p1, posv.at[0], 0)
    local(p2, posv.at[1], 0)
    local(x1, xv.at[pl.ds(0, BLK)], 1)
    local(x2, xv.at[pl.ds(BLK, BLK)], 1)
    l_wkvd = [local(wkvd.at[:, pl.ds(a, n)], wkvd_v.at[:, pl.ds(a, n)], i) for a, n, i in ((0, K_A, 2), (K_A, D_MODEL - K_A, 3))]
    l_gkv = local(gkv, gkv_v, 4)
    l_gq = local(gq, gq_v, 5)
    l_wqd = local(wqd, wqd_v, 6)
    l_wkvu = local(wkvu.at[:, pl.ds(pl.multiple_of(k * 4096, 4096), 4096)], wkvu_v, 7)
    l_wqu = local(wqu.at[:, pl.ds(pl.multiple_of(k * 3072, 1024), 3072)], wqu_v, 8)
    for i, core in enumerate((k, pk)):
        local(wo.at[pl.ds(pl.multiple_of(core * 2048, 2048), 2048)], wo_v.at[pl.ds(i * 2048, 2048)], 9)

    def wait_whole(ref, i):
        pltpu.make_async_copy(ref, ref, lsem.at[i]).wait()

    barrier = pltpu.get_barrier_semaphore()
    pl.semaphore_signal(barrier, inc=1, device_id=partner, device_id_type=MESH)
    for j in range(1, NCHIP):
        for core in range(2):
            pl.semaphore_signal(barrier, inc=1, device_id=dev(lax.rem(c + j, NCHIP), core), device_id_type=MESH)

    for b in range(1, NCHIP):
        @pl.when(c < b)
        def _():
            kvlat0[pl.ds(b * CHIP, CHIP), KV_LAT:] = jnp.zeros((CHIP, 128), BF16)

            def zero(h, _):
                for mb in range(2):
                    kT[mb, h, :, pl.ds(b * CHIP, CHIP)] = jnp.zeros((128, CHIP), BF16)
                    vb[mb, h, pl.ds(b * CHIP, CHIP)] = jnp.zeros((CHIP, 128), BF16)
                return 0
            lax.fori_loop(0, HEADS, zero, 0)

    lane = lax.broadcasted_iota(jnp.int32, (1, 128), 1)
    lo64 = lane < 64
    lo32 = lax.rem(lane, 64) < 32

    wait_whole(posv, 0)
    own = pl.ds(pl.multiple_of(k * CHIP, CHIP), CHIP)
    eye = lax.broadcasted_iota(jnp.int32, (BLK, BLK), 0) == lax.broadcasted_iota(jnp.int32, (BLK, BLK), 1)
    cols = [jnp.sum(jnp.where(eye, posv[mb].astype(F32), 0.0), axis=1, keepdims=True) for mb in range(2)]
    pos_col = jnp.concatenate(cols, axis=0)
    freq = jnp.exp(lax.rem(lane, 32).astype(F32) * (-LN_BASE / 32))
    ang = pos_col * freq
    cos_t = jnp.cos(ang)
    sin_t = jnp.sin(ang)
    sin_t = jnp.where(lo32, -sin_t, sin_t)
    tabs[0, own] = cos_t
    tabs[1, own] = sin_t
    tabs[2, own] = pos_col + jnp.zeros((CHIP, 128), F32)

    def rot(z, cs, sn):
        sw = jnp.where(lo32, pltpu.roll(z, 96, 1), pltpu.roll(z, 32, 1))
        return z * cs + sw * sn

    def kv_down(a, n):
        return lax.dot_general(xv[:, a:a + n], wkvd_v[:, a:a + n], (((1,), (1,)), ((), ())), preferred_element_type=F32)

    with jax.named_scope("wait_x"):
        wait_whole(xv, 1)
        l_wkvd[0].wait()
    usum[...] = kv_down(0, K_A)
    with jax.named_scope("wait_wd"):
        l_wkvd[1].wait()
        l_gkv.wait()
    u = usum[...] + kv_down(K_A, D_MODEL - K_A)
    ur = u[:, KV_LAT:]
    kr = rot(jnp.concatenate([ur, ur], axis=1), cos_t, sin_t)
    kr = jnp.where(lo64, kr[:BLK], kr[BLK:]).astype(BF16)

    ckv = norm_rows(u[:, :KV_LAT], gkv_v[...])

    def rows(chip, core):
        return pl.ds(pl.multiple_of(chip * CHIP + core * BLK, BLK), BLK)

    def chip_rows(chip):
        return pl.ds(pl.multiple_of(chip * CHIP, CHIP), CHIP)

    def part(item, chip, core):
        return kvlat[item].at[rows(chip, core)]

    kvlat[0][rows(c, k), KV_LAT:] = kr
    kvlat[0][rows(c, k), :KV_LAT] = ckv[:BLK]
    kvlat[1][rows(c, k)] = ckv[BLK:]

    with jax.named_scope("barrier"):
        pl.semaphore_wait(barrier, 7)

    def direct(item, j):
        p = part(item, c, k)
        return pltpu.make_async_remote_copy(src_ref=p, dst_ref=p, send_sem=ds.at[item, j - 1], recv_sem=dr.at[item, j - 1],
                                            device_id=dev(c + j, 1), device_id_type=MESH)

    def direct_recv(item, j):
        p = kvlat[item].at[chip_rows(c - j)]
        return pltpu.make_async_remote_copy(src_ref=p, dst_ref=p, send_sem=ds.at[item, 0], recv_sem=dr.at[item, j - 1],
                                            device_id=partner, device_id_type=MESH)

    def share(item, core):
        p = part(item, c, core)
        return pltpu.make_async_remote_copy(src_ref=p, dst_ref=p, send_sem=fs.at[item, 0], recv_sem=fr.at[item, 0],
                                            device_id=partner, device_id_type=MESH)

    def forward(item, j):
        p = kvlat[item].at[chip_rows(c - j)]
        return pltpu.make_async_remote_copy(src_ref=p, dst_ref=p, send_sem=fs.at[item, j], recv_sem=fr.at[item, j],
                                            device_id=partner, device_id_type=MESH)

    def send(item):
        for j in (3, 2, 1):
            @pl.when(c + j < NCHIP)
            def _():
                direct(item, j).start()

    send(0)
    for item in range(2):
        share(item, k).start()

    l_gq.wait()
    l_wqd.wait()
    with jax.named_scope("q_down"):
        cq = jnp.dot(xv[...], wqd_v[...], preferred_element_type=F32)
        qlat[own] = norm_rows(cq, gq_v[...])

    def q_copy(i, core):
        r = pl.ds(pl.multiple_of(core * CHIP, CHIP), CHIP)
        p = qlat.at[r] if i == 0 else tabs.at[:, r]
        return pltpu.make_async_remote_copy(src_ref=p, dst_ref=p, send_sem=qs.at[i], recv_sem=qr.at[i],
                                            device_id=partner, device_id_type=MESH)

    for i in range(2):
        q_copy(i, k).start()

    def kv_up(lhs, store, turn=True):
        for i in range(4):
            kv = jnp.dot(lhs, wkvu_v[:, i * 1024:(i + 1) * 1024], preferred_element_type=F32).astype(BF16)
            for n in range(4):
                key = kv[:, n * 256:n * 256 + NOPE]
                store(i * 4 + n, key.T if turn else key, kv[:, n * 256 + NOPE:(n + 1) * 256])

    def kv_up_own():
        r = chip_rows(c)

        def store(h, key, val):
            for mb in range(2):
                kT[mb, h, :, r] = key[:, mb * CHIP:(mb + 1) * CHIP]
                vb[mb, h, r] = val[mb * CHIP:(mb + 1) * CHIP]
        kv_up(jnp.concatenate([kvlat0[r, :KV_LAT], kvlat1[r]], axis=0), store)

    def kv_up_device(core, store_key):
        r = rows(c, core)

        def store(h, key, val):
            store_key(h, key)
            for mb in range(2):
                vb[mb, h, r] = val[mb * BLK:(mb + 1) * BLK]
        kv_up(jnp.concatenate([kvlat0[r, :KV_LAT], kvlat1[r]], axis=0), store, False)

    def hold_key(h, key):
        kheld[h] = key

    def join_key(h, key):
        for mb in range(2):
            s = slice(mb * BLK, (mb + 1) * BLK)
            kT[mb, h, :, chip_rows(c)] = jnp.concatenate([key[s], kheld[h, s]], axis=0).T

    def kv_up_first(r):
        def store(h, key, val):
            kT[0, h, :, r] = key
            vb[0, h, r] = val
        kv_up(kvlat0[r, :KV_LAT], store)

    with jax.named_scope("wait_wkvu"):
        l_wkvu.wait()
    def wait_share():
        with jax.named_scope("wait_partner"):
            for item in range(2):
                share(item, pk).wait_recv()

    with jax.named_scope("kv_own"):
        @pl.when(k == 0)
        def _():
            wait_share()
            kv_up_own()

        @pl.when(k == 1)
        def _():
            kv_up_device(k, hold_key)
            wait_share()
            kv_up_device(pk, join_key)

    for i in range(2):
        q_copy(i, pk).wait_recv()
    for mb in range(2):
        for core in range(2):
            pos = tabs[2, pl.ds(core * CHIP + mb * BLK, BLK), 0:1].astype(jnp.int32)
            qi = c * CHIP + core * BLK + lax.broadcasted_iota(jnp.int32, (BLK, TOK), 0)
            ki = lax.broadcasted_iota(jnp.int32, (BLK, TOK), 1)
            keep = jnp.logical_and(ki <= qi, ki >= qi - pos)
            bias[mb, pl.ds(core * BLK, BLK)] = jnp.where(keep, BIG, NEG)
    l_wqu.wait()

    def q_up(i):
        return jnp.dot(qlat[...], wqu_v[:, i * 768:(i + 1) * 768], preferred_element_type=F32)

    def q_store(i, f):
        for pair in range(2):
            t0, t1, t2 = (f[:, pair * 384 + n * 128: pair * 384 + (n + 1) * 128] for n in range(3))
            n1 = pltpu.roll(jnp.where(lo64, t2, t1), 64, 1)
            r = rot(jnp.where(lo64, t1, t2), tabs[0], tabs[1])
            zero = jnp.zeros_like(r)
            q = ((t0.astype(BF16), jnp.where(lo64, r, zero).astype(BF16)),
                 (n1.astype(BF16), jnp.where(lo64, zero, r).astype(BF16)))
            for odd in range(2):
                h = i * 4 + pair * 2 + odd
                for mb in range(2):
                    for core in range(2):
                        s = slice(core * CHIP + mb * BLK, core * CHIP + (mb + 1) * BLK)
                        for n in range(2):
                            qbuf[mb, h, pl.ds(core * BLK, BLK), n * 128:(n + 1) * 128] = q[odd][n][s]

    def nth(i):
        return jnp.where(jnp.logical_and(c == 3, i > 1), 5 - i, i)

    def each_earlier_chip(step):
        lax.fori_loop(1, c + 1, lambda i, _: (step(i, nth(i)), 0)[1], 0)

    def pass_on(item, j):
        direct_recv(item, j).wait_recv()
        forward(item, j).start()

    with jax.named_scope("q_up"):
        prev = q_up(0)
        for i in range(4):
            nxt = q_up(i + 1) if i < 3 else None
            q_store(i, prev)
            prev = nxt

    with jax.named_scope("pass_on"):
        for j, at in ((1, c > 0), (3, c == 3)):
            @pl.when(jnp.logical_and(k == 1, at))
            def _():
                pass_on(0, j)

    send(1)

    def o_copy(mb, half):
        cs = pl.ds(half * 1024, 1024)
        return pltpu.make_async_remote_copy(
            src_ref=oall.at[mb, pl.ds(pl.multiple_of(pk * BLK, BLK), BLK), cs], dst_ref=oin.at[pl.ds(mb * BLK, BLK), cs],
            send_sem=os_.at[0], recv_sem=or_.at[mb * half], device_id=partner, device_id_type=MESH)

    def o_bytes(n, i):
        p = oin.at[pl.ds(0, n)]
        return pltpu.make_async_remote_copy(src_ref=p, dst_ref=p, send_sem=os_.at[0], recv_sem=or_.at[i],
                                            device_id=partner, device_id_type=MESH)

    def spread_rope():
        r = kvlat0[:, KV_LAT:].T
        for mb in range(2):
            half = r[mb * ROPE:(mb + 1) * ROPE]
            kropeT[mb] = jnp.concatenate([half, half], axis=0)

    def heads(mb, lo, hi, beside=lambda h: None):
        scores = []
        for h in range(lo, hi):
            kcat = jnp.concatenate([kT[mb, h], kropeT[mb]], axis=0)
            scores.append(jnp.dot(qbuf[mb, h], kcat, preferred_element_type=F32))
            beside(h)
        probs = []
        for s in scores:
            s = jnp.minimum(s, bias[mb])
            m = jnp.max(s, axis=1, keepdims=True)
            e = jnp.exp2((s - m) * SCALE2)
            probs.append((e * (1.0 / jnp.sum(e, axis=1, keepdims=True))).astype(BF16))
        for h in range(lo, hi):
            o = jnp.dot(probs[h - lo], vb[mb, h], preferred_element_type=F32)
            oall[mb, :, h * 128:(h + 1) * 128] = o.astype(BF16)
            if h % 8 == 7:
                o_copy(mb, h // 8).start()

    def kv_up_second(n):
        def two(i):
            kv = jnp.dot(kvlat1[0:n], wkvu_v[:, i * 512:(i + 1) * 512], preferred_element_type=F32).astype(BF16)
            for h in range(2):
                kT[1, 2 * i + h, :, 0:n] = kv[:, h * 256:h * 256 + NOPE].T
                vb[1, 2 * i + h, 0:n] = kv[:, h * 256 + NOPE:(h + 1) * 256]
        return two

    def take(item, j):
        with jax.named_scope("take_wait"):
            @pl.when(k == 0)
            def _():
                forward(item, j).wait_recv()

    def pass_if(at, item, j):
        @pl.when(jnp.logical_and(k == 1, at))
        def _():
            pass_on(item, j)

    @pl.when(c > 0)
    def _():
        take(0, 1)
        with jax.named_scope("take1"):
            kv_up_first(chip_rows(c - 1))

    @pl.when(c == 2)
    def _():
        pass_if(True, 0, 2)
        take(0, 2)
        with jax.named_scope("take1"):
            kv_up_first(pl.ds(0, CHIP))

    @pl.when(c == 3)
    def _():
        pass_if(True, 0, 2)
        take(0, 3)
        take(0, 2)
        with jax.named_scope("take1"):
            kv_up_first(pl.ds(0, 2 * CHIP))
    spread_rope()
    with jax.named_scope("heads1a"):
        heads(0, 0, 8)

    def take_later(i, j):
        pass_if(True, 1, j)
        take(1, j)

    @pl.when(c == 3)
    def _():
        with jax.named_scope("take2_wait"):
            each_earlier_chip(take_later)
        with jax.named_scope("heads1b"):
            two = kv_up_second(3 * CHIP)
            heads(0, 8, 16, lambda h: two(h - 8))

    @pl.when(c < 3)
    def _():
        with jax.named_scope("heads1c"):
            heads(0, 8, 16)
        with jax.named_scope("take2_wait"):
            each_earlier_chip(take_later)
        for n in (1, 2):
            @pl.when(c == n)
            def _():
                with jax.named_scope("take2"):
                    two = kv_up_second(n * CHIP)
                    for i in range(8):
                        two(i)
    with jax.named_scope("heads2"):
        heads(1, 0, 16)

    with jax.named_scope("out"):
        wait_whole(wo_v, 9)
        orow = pl.ds(pl.multiple_of(k * BLK, BLK), BLK)
        mine = jnp.concatenate([oall[0, orow], oall[1, orow]], axis=0)
        acc[...] = jnp.dot(mine, wo_v[0:2048], preferred_element_type=F32)
    with jax.named_scope("out_b"):
        o_bytes(96, 0).wait_recv()
        acc[...] += jnp.dot(oin[:, :1024], wo_v[2048:3072], preferred_element_type=F32)
    with jax.named_scope("out_last"):
        o_bytes(32, 1).wait_recv()
        y[...] = (acc[...] + jnp.dot(oin[:, 1024:], wo_v[3072:], preferred_element_type=F32)).astype(BF16)

    for item in range(2):
        for j in (3, 2, 1):
            @pl.when(c + j < NCHIP)
            def _():
                direct(item, j).wait_send()

        share(item, k).wait_send()

        @pl.when(k == 1)
        def _():
            each_earlier_chip(lambda i, j: forward(item, j).wait_send())
    for i in range(2):
        q_copy(i, k).wait_send()
    o_bytes(CHIP, 0).wait_send()


def store_body(y, y1, y2, sem):
    for i, out in enumerate((y1, y2)):
        pltpu.make_async_copy(y.at[pl.ds(i * BLK, BLK)], out, sem.at[i]).start()
    for i, out in enumerate((y1, y2)):
        pltpu.make_async_copy(y.at[pl.ds(i * BLK, BLK)], out, sem.at[i]).wait()


def store(y):
    any_spec = pl.BlockSpec(memory_space=pl.ANY)
    return pl.pallas_call(
        store_body,
        out_shape=(jax.ShapeDtypeStruct((BLK, D_MODEL), BF16),) * 2,
        in_specs=[any_spec],
        out_specs=(any_spec,) * 2,
        scratch_shapes=[pltpu.SemaphoreType.DMA((2,))],
        compiler_params=pltpu.CompilerParams(vmem_limit_bytes=2**20),
    )(y)


def solution(mesh):
    tok_spec = P(('dp', 'sp'), None)
    idx_spec = P(('dp', 'sp'))
    any_spec = pl.BlockSpec(memory_space=pl.ANY)
    vmem_spec = pl.BlockSpec(memory_space=pltpu.VMEM)

    def local_body(x_one, seg_one, pos_one, x_two, seg_two, pos_two, w_qdown, gain_q, w_qup, w_kvdown, gain_kv, w_kvup, w_out):
        dma = pltpu.SemaphoreType.DMA
        call = pl.pallas_call(
            body,
            out_shape=jax.ShapeDtypeStruct((CHIP, D_MODEL), BF16),
            in_specs=[pl.BlockSpec(memory_space=pltpu.HBM)] * 11,
            out_specs=vmem_spec,
            scratch_shapes=[
                pltpu.VMEM((CHIP, D_MODEL), BF16),
                pltpu.VMEM((2, 1, BLK), jnp.int32),
                pltpu.VMEM((D_MODEL, Q_LAT), BF16),
                pltpu.VMEM((Q_LAT,), BF16),
                pltpu.VMEM((Q_LAT, 3072), BF16),
                pltpu.VMEM((KV_LAT + ROPE, D_MODEL), BF16),
                pltpu.VMEM((KV_LAT,), BF16),
                pltpu.VMEM((KV_LAT, 4096), BF16),
                pltpu.VMEM((4096, D_MODEL), BF16),
                pltpu.VMEM((TOK, KV_LAT + 128), BF16),
                pltpu.VMEM((TOK, KV_LAT), BF16),
                pltpu.VMEM((2 * CHIP, Q_LAT), BF16),
                pltpu.VMEM((3, 2 * CHIP, 128), F32),
                pltpu.VMEM((2, HEADS, CHIP, 256), BF16),
                pltpu.VMEM((HEADS, CHIP, 128), BF16),
                pltpu.VMEM((2, HEADS, 128, TOK), BF16),
                pltpu.VMEM((2, HEADS, TOK, 128), BF16),
                pltpu.VMEM((2, 128, TOK), BF16),
                pltpu.VMEM((2, CHIP, TOK), F32),
                pltpu.VMEM((2, CHIP, 2048), BF16),
                pltpu.VMEM((CHIP, 2048), BF16),
                pltpu.VMEM((CHIP, D_MODEL), F32),
                pltpu.VMEM((CHIP, KV_LAT + ROPE), F32),
                dma((10,)), dma((2, 3)), dma((2, 3)), dma((2, 4)), dma((2, 4)),
                dma((2,)), dma((2,)), dma((1,)), dma((2,)),
            ],
            compiler_params=pltpu.CompilerParams(collective_id=0, has_side_effects=True, vmem_limit_bytes=52 * 2**20),
        )
        args = (x_one, pos_one.reshape(1, BLK), x_two, pos_two.reshape(1, BLK), w_qdown, gain_q, w_qup,
                w_kvdown.T, gain_kv, w_kvup, w_out)
        y = call(*(pltpu.with_memory_space_constraint(a, pltpu.HBM) for a in args))
        return store(y)

    return jax.shard_map(local_body, mesh=mesh,
                         in_specs=(tok_spec, idx_spec, idx_spec, tok_spec, idx_spec, idx_spec, P(), P(), P(), P(), P(), P(), P()),
                         out_specs=(tok_spec, tok_spec), check_vma=False)
```

```python
import jax
import jax.numpy as jnp
from jax import lax
from jax.experimental import pallas as pl
from jax.experimental.pallas import tpu as pltpu
from jax.sharding import PartitionSpec as P

MESH = pl.DeviceIdType.MESH
F32 = jnp.float32
BF16 = jnp.bfloat16

D_MODEL = 1792
Q_LAT = 384
KV_LAT = 512
ROPE = 64
NOPE = 128
HEADS = 16
BLK = 64
CHIP = 2 * BLK
TOK = 512
NCHIP = 4
LN_BASE = 9.210340371976184
EPS = 1e-6
LEAD = 4
K_A = 1024
SCALE2 = 192 ** -0.5 * 1.4426950408889634
NEG = -1e30
BIG = 3.0e38


def norm_rows(z, gain):
    ms = jnp.mean(z * z, axis=-1, keepdims=True)
    return (z * lax.rsqrt(ms + EPS) * gain.astype(F32)[None, :]).astype(BF16)


def body(x1, p1, x2, p2, wqd, gq, wqu, wkvd, gkv, wkvu, wo, y,
         xv, posv, wqd_v, gq_v, wqu_v, wkvd_v, gkv_v, wkvu_v, wo_v,
         kvlat0, kvlat1, qlat, tabs, qbuf, kheld, kT, vb, kropeT, bias, oall, oin, acc, usum,
         lsem, sent, dr, fr, qr, or_):
    kvlat = (kvlat0, kvlat1)
    sp = lax.axis_index("sp")
    dp = lax.axis_index("dp")
    k = lax.rem(sp, 2)
    c = lax.div(sp, 2)
    pk = 1 - k

    def dev(chip, core):
        return (dp, chip * 2 + core)

    partner = dev(c, pk)

    def local(src, dst, i):
        cp = pltpu.make_async_copy(src, dst, lsem.at[i])
        cp.start()
        return cp

    local(p1, posv.at[0], 0)
    local(p2, posv.at[1], 0)
    local(x1, xv.at[pl.ds(0, BLK)], 1)
    local(x2, xv.at[pl.ds(BLK, BLK)], 1)
    l_wkvd = [local(wkvd.at[:, pl.ds(a, n)], wkvd_v.at[:, pl.ds(a, n)], i) for a, n, i in ((0, K_A, 2), (K_A, D_MODEL - K_A, 3))]
    l_gkv = local(gkv, gkv_v, 6)
    l_gq = local(gq, gq_v, 7)
    l_wqd = local(wqd, wqd_v, 4)
    l_wkvu = local(wkvu.at[:, pl.ds(pl.multiple_of(k * 4096, 4096), 4096)], wkvu_v, 5)

    def wait_whole(ref, i):
        pltpu.make_async_copy(ref, ref, lsem.at[i]).wait()

    def wait_bytes(ref, n, sem):
        p = ref.at[pl.ds(0, n)]
        pltpu.make_async_copy(p, p, sem).wait()

    barrier = pltpu.get_barrier_semaphore()
    pl.semaphore_signal(barrier, inc=1, device_id=partner, device_id_type=MESH)
    for j in range(1, NCHIP):
        for core in range(2):
            pl.semaphore_signal(barrier, inc=1, device_id=dev(lax.rem(c + j, NCHIP), core), device_id_type=MESH)

    for b in range(1, NCHIP):
        @pl.when(c < b)
        def _():
            kvlat0[pl.ds(b * CHIP, CHIP), KV_LAT:] = jnp.zeros((CHIP, 128), BF16)

            def zero(h, _):
                for mb in range(2):
                    kT[mb, h, :, pl.ds(b * CHIP, CHIP)] = jnp.zeros((128, CHIP), BF16)
                    vb[mb, h, pl.ds(b * CHIP, CHIP)] = jnp.zeros((CHIP, 128), BF16)
                return 0
            lax.fori_loop(0, HEADS, zero, 0)

    lane = lax.broadcasted_iota(jnp.int32, (1, 128), 1)
    lo64 = lane < 64
    lo32 = lax.rem(lane, 64) < 32

    wait_whole(posv, 0)
    own = pl.ds(pl.multiple_of(k * CHIP, CHIP), CHIP)
    eye = lax.broadcasted_iota(jnp.int32, (BLK, BLK), 0) == lax.broadcasted_iota(jnp.int32, (BLK, BLK), 1)
    cols = [jnp.sum(jnp.where(eye, posv[mb].astype(F32), 0.0), axis=1, keepdims=True) for mb in range(2)]
    pos_col = jnp.concatenate(cols, axis=0)
    freq = jnp.exp(lax.rem(lane, 32).astype(F32) * (-LN_BASE / 32))
    ang = pos_col * freq
    cos_t = jnp.cos(ang)
    sin_t = jnp.sin(ang)
    sin_t = jnp.where(lo32, -sin_t, sin_t)
    tabs[0, own] = cos_t
    tabs[1, own] = sin_t
    tabs[2, own] = pos_col + jnp.zeros((CHIP, 128), F32)

    def rot(z, cs, sn):
        sw = jnp.where(lo32, pltpu.roll(z, 96, 1), pltpu.roll(z, 32, 1))
        return z * cs + sw * sn

    def kv_down(a, n):
        return lax.dot_general(xv[:, a:a + n], wkvd_v[:, a:a + n], (((1,), (1,)), ((), ())), preferred_element_type=F32)

    with jax.named_scope("wait_x"):
        wait_whole(xv, 1)
        l_wkvd[0].wait()
    l_wqu = local(wqu.at[:, pl.ds(pl.multiple_of(k * 3072, 1024), 3072)], wqu_v, 1)
    usum[...] = kv_down(0, K_A)
    with jax.named_scope("wait_wd"):
        l_wkvd[1].wait()
        l_gkv.wait()
    u = usum[...] + kv_down(K_A, D_MODEL - K_A)
    ur = u[:, KV_LAT:]
    kr = rot(jnp.concatenate([ur, ur], axis=1), cos_t, sin_t)
    kr = jnp.where(lo64, kr[:BLK], kr[BLK:]).astype(BF16)

    ckv = norm_rows(u[:, :KV_LAT], gkv_v[...])

    def rows(chip, core):
        return pl.ds(pl.multiple_of(chip * CHIP + core * BLK, BLK), BLK)

    def chip_rows(chip):
        return pl.ds(pl.multiple_of(chip * CHIP, CHIP), CHIP)

    def part(item, chip, core):
        return kvlat[item].at[rows(chip, core)]

    kvlat[0][rows(c, k), KV_LAT:] = kr
    kvlat[0][rows(c, k), :KV_LAT] = ckv[:BLK]
    kvlat[1][rows(c, k)] = ckv[BLK:]

    with jax.named_scope("barrier"):
        pl.semaphore_wait(barrier, 7)

    def direct(item, j):
        p = part(item, c, k)
        return pltpu.make_async_remote_copy(src_ref=p, dst_ref=p, send_sem=sent.at[0], recv_sem=dr.at[item, j - 1],
                                            device_id=dev(c + j, 1), device_id_type=MESH)

    def direct_recv(item, j):
        p = kvlat[item].at[chip_rows(c - j)]
        return pltpu.make_async_remote_copy(src_ref=p, dst_ref=p, send_sem=sent.at[0], recv_sem=dr.at[item, j - 1],
                                            device_id=partner, device_id_type=MESH)

    def share(item, core):
        p = part(item, c, core)
        return pltpu.make_async_remote_copy(src_ref=p, dst_ref=p, send_sem=sent.at[0], recv_sem=fr.at[0],
                                            device_id=partner, device_id_type=MESH)

    def forward(item, j):
        p = kvlat[item].at[chip_rows(c - j)]
        return pltpu.make_async_remote_copy(src_ref=p, dst_ref=p, send_sem=sent.at[0], recv_sem=fr.at[3 if item else 1 if j == 1 else 2],
                                            device_id=partner, device_id_type=MESH)

    def send(item, pairs):
        for chip, j in pairs:
            @pl.when(c == chip)
            def _():
                direct(item, j).start()

    send(0, ((0, 3), (0, 2), (0, 1), (1, 2), (1, 1), (2, 1)))
    for item in range(2):
        share(item, k).start()

    l_gq.wait()
    l_wqd.wait()
    with jax.named_scope("q_down"):
        cq = jnp.dot(xv[...], wqd_v[...], preferred_element_type=F32)
        qlat[own] = norm_rows(cq, gq_v[...])

    def q_copy(i, core):
        r = pl.ds(pl.multiple_of(core * CHIP, CHIP), CHIP)
        p = qlat.at[r] if i == 0 else tabs.at[:, r]
        return pltpu.make_async_remote_copy(src_ref=p, dst_ref=p, send_sem=sent.at[0], recv_sem=qr.at[0],
                                            device_id=partner, device_id_type=MESH)

    for i in range(2):
        q_copy(i, k).start()

    def kv_up(lhs, store, turn=True):
        for i in range(4):
            kv = jnp.dot(lhs, wkvu_v[:, i * 1024:(i + 1) * 1024], preferred_element_type=F32).astype(BF16)
            for n in range(4):
                key = kv[:, n * 256:n * 256 + NOPE]
                store(i * 4 + n, key.T if turn else key, kv[:, n * 256 + NOPE:(n + 1) * 256])

    def kv_up_own():
        r = chip_rows(c)

        def store(h, key, val):
            for mb in range(2):
                kT[mb, h, :, r] = key[:, mb * CHIP:(mb + 1) * CHIP]
                vb[mb, h, r] = val[mb * CHIP:(mb + 1) * CHIP]
        kv_up(jnp.concatenate([kvlat0[r, :KV_LAT], kvlat1[r]], axis=0), store)

    def kv_up_device(core, store_key):
        r = rows(c, core)

        def store(h, key, val):
            store_key(h, key)
            for mb in range(2):
                vb[mb, h, r] = val[mb * BLK:(mb + 1) * BLK]
        kv_up(jnp.concatenate([kvlat0[r, :KV_LAT], kvlat1[r]], axis=0), store, False)

    def hold_key(h, key):
        kheld[h] = key

    def join_key(h, key):
        for mb in range(2):
            s = slice(mb * BLK, (mb + 1) * BLK)
            kT[mb, h, :, chip_rows(c)] = jnp.concatenate([key[s], kheld[h, s]], axis=0).T

    def kv_up_first(r):
        def store(h, key, val):
            kT[0, h, :, r] = key
            vb[0, h, r] = val
        kv_up(kvlat0[r, :KV_LAT], store)

    send(1, ((2, 1),))
    with jax.named_scope("wait_wkvu"):
        l_wkvu.wait()
    for i, core in enumerate((k, pk)):
        local(wo.at[pl.ds(pl.multiple_of(core * 2048, 2048), 2048)], wo_v.at[pl.ds(i * 2048, 2048)], 0)
    def wait_share():
        with jax.named_scope("wait_partner"):
            wait_bytes(wqd_v, 192, fr.at[0])

    def q_up(i):
        return jnp.dot(qlat[...], wqu_v[:, i * 768:(i + 1) * 768], preferred_element_type=F32)

    def q_store(i, f):
        for pair in range(2):
            t0, t1, t2 = (f[:, pair * 384 + n * 128: pair * 384 + (n + 1) * 128] for n in range(3))
            n1 = pltpu.roll(jnp.where(lo64, t2, t1), 64, 1)
            r = rot(jnp.where(lo64, t1, t2), tabs[0], tabs[1])
            zero = jnp.zeros_like(r)
            q = ((t0.astype(BF16), jnp.where(lo64, r, zero).astype(BF16)),
                 (n1.astype(BF16), jnp.where(lo64, zero, r).astype(BF16)))
            for odd in range(2):
                h = i * 4 + pair * 2 + odd
                for mb in range(2):
                    for core in range(2):
                        s = slice(core * CHIP + mb * BLK, core * CHIP + (mb + 1) * BLK)
                        for n in range(2):
                            qbuf[mb, h, pl.ds(core * BLK, BLK), n * 128:(n + 1) * 128] = q[odd][n][s]

    def queries():
        wait_bytes(wqd_v, 384, qr.at[0])
        for mb in range(2):
            for core in range(2):
                pos = tabs[2, pl.ds(core * CHIP + mb * BLK, BLK), 0:1].astype(jnp.int32)
                qi = c * CHIP + core * BLK + lax.broadcasted_iota(jnp.int32, (BLK, TOK), 0)
                ki = lax.broadcasted_iota(jnp.int32, (BLK, TOK), 1)
                keep = jnp.logical_and(ki <= qi, ki >= qi - pos)
                bias[mb, pl.ds(core * BLK, BLK)] = jnp.where(keep, BIG, NEG)
        l_wqu.wait()
        prev = q_up(0)
        for i in range(4):
            nxt = q_up(i + 1) if i < 3 else None
            q_store(i, prev)
            prev = nxt

    with jax.named_scope("kv_own"):
        @pl.when(k == 0)
        def _():
            wait_share()
            kv_up_own()
            queries()

        @pl.when(k == 1)
        def _():
            kv_up_device(k, hold_key)
            wait_share()
            kv_up_device(pk, join_key)
            queries()

    def pass_on(item, j):
        direct_recv(item, j).wait_recv()
        forward(item, j).start()

    with jax.named_scope("pass_on"):
        for j, at in ((1, c > 0), (3, c == 3)):
            @pl.when(jnp.logical_and(k == 1, at))
            def _():
                pass_on(0, j)

    send(1, ((0, 3), (0, 2), (0, 1), (1, 2), (1, 1)))

    def o_copy(mb, half):
        cs = pl.ds(half * 1024, 1024)
        return pltpu.make_async_remote_copy(
            src_ref=oall.at[mb, pl.ds(pl.multiple_of(pk * BLK, BLK), BLK), cs], dst_ref=oin.at[pl.ds(mb * BLK, BLK), cs],
            send_sem=sent.at[1], recv_sem=or_.at[mb * half], device_id=partner, device_id_type=MESH)

    def spread_rope():
        r = kvlat0[:, KV_LAT:].T
        for mb in range(2):
            half = r[mb * ROPE:(mb + 1) * ROPE]
            kropeT[mb] = jnp.concatenate([half, half], axis=0)

    def heads(mb):
        scores = []
        for h in range(HEADS):
            kcat = jnp.concatenate([kT[mb, h], kropeT[mb]], axis=0)
            scores.append(jnp.dot(qbuf[mb, h], kcat, preferred_element_type=F32))
        probs = []
        for s in scores:
            s = jnp.minimum(s, bias[mb])
            m = jnp.max(s, axis=1, keepdims=True)
            e = jnp.exp2((s - m) * SCALE2)
            probs.append((e * (1.0 / jnp.sum(e, axis=1, keepdims=True))).astype(BF16))
        for h in range(HEADS):
            o = jnp.dot(probs[h], vb[mb, h], preferred_element_type=F32)
            oall[mb, :, h * 128:(h + 1) * 128] = o.astype(BF16)
            if h % 8 == 7:
                o_copy(mb, h // 8).start()

    def kv_up_second(n):
        def store(h, key, val):
            kT[1, h, :, 0:n] = key
            vb[1, h, 0:n] = val
        kv_up(kvlat1[0:n], store)

    def take(ref, n, i):
        with jax.named_scope("take_wait"):
            @pl.when(k == 0)
            def _():
                wait_bytes(ref, n, fr.at[i])

    def pass_if(at, item, j):
        @pl.when(jnp.logical_and(k == 1, at))
        def _():
            pass_on(item, j)

    @pl.when(c > 0)
    def _():
        take(kvlat0, CHIP, 1)
        with jax.named_scope("take1"):
            kv_up_first(chip_rows(c - 1))

    for n in (2, 3):
        @pl.when(c == n)
        def _():
            pass_if(True, 0, 2)
            take(kvlat0, (n - 1) * CHIP, 2)
            with jax.named_scope("take1"):
                kv_up_first(pl.ds(0, (n - 1) * CHIP))
    spread_rope()
    pass_if(c == 3, 1, 1)
    with jax.named_scope("heads1"):
        heads(0)

    for n in range(NCHIP):
        @pl.when(c == n)
        def _():
            if n > 0:
                for j in ((1,), (1, 2), (3, 2))[n - 1]:
                    pass_if(True, 1, j)
                take(kvlat1, n * CHIP, 3)
            with jax.named_scope("heads2"):
                if n > 0:
                    kv_up_second(n * CHIP)
                heads(1)

    with jax.named_scope("out"):
        wait_whole(wo_v, 0)
        orow = pl.ds(pl.multiple_of(k * BLK, BLK), BLK)
        mine = jnp.concatenate([oall[0, orow], oall[1, orow]], axis=0)

        @pl.when(k == 0)
        def _():
            wait_bytes(oin, 96, or_.at[0])
            wait_bytes(oin, 32, or_.at[1])
            y[...] = jnp.dot(jnp.concatenate([mine, oin[...]], axis=1), wo_v[...], preferred_element_type=F32).astype(BF16)

        @pl.when(k == 1)
        def _():
            acc[...] = jnp.dot(mine, wo_v[0:2048], preferred_element_type=F32)
            wait_bytes(oin, 96, or_.at[0])
            acc[...] += jnp.dot(oin[:, :1024], wo_v[2048:3072], preferred_element_type=F32)
            wait_bytes(oin, 32, or_.at[1])
            y[...] = (acc[...] + jnp.dot(oin[:, 1024:], wo_v[3072:], preferred_element_type=F32)).astype(BF16)

    for n in range(NCHIP):
        @pl.when(c == n)
        def _():
            wait_bytes(wqd_v, 192 * (NCHIP - 1 - n) + 192 + 384, sent.at[0])

            if n > 0:
                @pl.when(k == 1)
                def _():
                    wait_bytes(wqd_v, 384 * n, sent.at[0])
    wait_bytes(oin, CHIP, sent.at[1])


def store_body(y, y1, y2, sem):
    for i, out in enumerate((y1, y2)):
        pltpu.make_async_copy(y.at[pl.ds(i * BLK, BLK)], out, sem.at[i]).start()
    for i, out in enumerate((y1, y2)):
        pltpu.make_async_copy(y.at[pl.ds(i * BLK, BLK)], out, sem.at[i]).wait()


def store(y):
    any_spec = pl.BlockSpec(memory_space=pl.ANY)
    return pl.pallas_call(
        store_body,
        out_shape=(jax.ShapeDtypeStruct((BLK, D_MODEL), BF16),) * 2,
        in_specs=[any_spec],
        out_specs=(any_spec,) * 2,
        scratch_shapes=[pltpu.SemaphoreType.DMA((2,))],
        compiler_params=pltpu.CompilerParams(vmem_limit_bytes=2**20),
    )(y)


def solution(mesh):
    tok_spec = P(('dp', 'sp'), None)
    idx_spec = P(('dp', 'sp'))
    any_spec = pl.BlockSpec(memory_space=pl.ANY)
    vmem_spec = pl.BlockSpec(memory_space=pltpu.VMEM)

    def local_body(x_one, seg_one, pos_one, x_two, seg_two, pos_two, w_qdown, gain_q, w_qup, w_kvdown, gain_kv, w_kvup, w_out):
        dma = pltpu.SemaphoreType.DMA
        call = pl.pallas_call(
            body,
            out_shape=jax.ShapeDtypeStruct((CHIP, D_MODEL), BF16),
            in_specs=[pl.BlockSpec(memory_space=pltpu.HBM)] * 11,
            out_specs=vmem_spec,
            scratch_shapes=[
                pltpu.VMEM((CHIP, D_MODEL), BF16),
                pltpu.VMEM((2, 1, BLK), jnp.int32),
                pltpu.VMEM((D_MODEL, Q_LAT), BF16),
                pltpu.VMEM((Q_LAT,), BF16),
                pltpu.VMEM((Q_LAT, 3072), BF16),
                pltpu.VMEM((KV_LAT + ROPE, D_MODEL), BF16),
                pltpu.VMEM((KV_LAT,), BF16),
                pltpu.VMEM((KV_LAT, 4096), BF16),
                pltpu.VMEM((4096, D_MODEL), BF16),
                pltpu.VMEM((TOK, KV_LAT + 128), BF16),
                pltpu.VMEM((TOK, KV_LAT), BF16),
                pltpu.VMEM((2 * CHIP, Q_LAT), BF16),
                pltpu.VMEM((3, 2 * CHIP, 128), F32),
                pltpu.VMEM((2, HEADS, CHIP, 256), BF16),
                pltpu.VMEM((HEADS, CHIP, 128), BF16),
                pltpu.VMEM((2, HEADS, 128, TOK), BF16),
                pltpu.VMEM((2, HEADS, TOK, 128), BF16),
                pltpu.VMEM((2, 128, TOK), BF16),
                pltpu.VMEM((2, CHIP, TOK), F32),
                pltpu.VMEM((2, CHIP, 2048), BF16),
                pltpu.VMEM((CHIP, 2048), BF16),
                pltpu.VMEM((CHIP, D_MODEL), F32),
                pltpu.VMEM((CHIP, KV_LAT + ROPE), F32),
                dma((8,)), dma((2,)), dma((2, 3)), dma((4,)), dma((1,)), dma((2,)),
            ],
            compiler_params=pltpu.CompilerParams(collective_id=0, has_side_effects=True, vmem_limit_bytes=52 * 2**20),
        )
        args = (x_one, pos_one.reshape(1, BLK), x_two, pos_two.reshape(1, BLK), w_qdown, gain_q, w_qup,
                w_kvdown.T, gain_kv, w_kvup, w_out)
        y = call(*(pltpu.with_memory_space_constraint(a, pltpu.HBM) for a in args))
        return store(y)

    return jax.shard_map(local_body, mesh=mesh,
                         in_specs=(tok_spec, idx_spec, idx_spec, tok_spec, idx_spec, idx_spec, P(), P(), P(), P(), P(), P(), P()),
                         out_specs=(tok_spec, tok_spec), check_vma=False)
```

```python
import jax
import jax.numpy as jnp
from jax import lax
from jax.experimental import pallas as pl
from jax.experimental.pallas import tpu as pltpu
from jax.sharding import PartitionSpec as P

MESH = pl.DeviceIdType.MESH
F32 = jnp.float32
BF16 = jnp.bfloat16

D_MODEL = 1792
Q_LAT = 384
KV_LAT = 512
ROPE = 64
NOPE = 128
HEADS = 16
BLK = 64
CHIP = 2 * BLK
TOK = 512
NCHIP = 4
LN_BASE = 9.210340371976184
EPS = 1e-6
LEAD = 4
K_A = 1024
SCALE2 = 192 ** -0.5 * 1.4426950408889634
NEG = -1e30
BIG = 3.0e38


def norm_rows(z, gain):
    ms = jnp.mean(z * z, axis=-1, keepdims=True)
    return (z * lax.rsqrt(ms + EPS) * gain.astype(F32)[None, :]).astype(BF16)


def body(x1, p1, x2, p2, wqd, gq, wqu, wkvd, gkv, wkvu, wo, y,
         xv, posv, wqd_v, gq_v, wqu_v, wkvd_v, gkv_v, wkvu_v, wo_v,
         kvlat0, kvlat1, qlat, tabs, qbuf, kheld, kT, vb, kropeT, bias, oall, oin, acc, usum,
         lsem, sent, dr, fr, qr, or_):
    kvlat = (kvlat0, kvlat1)
    sp = lax.axis_index("sp")
    dp = lax.axis_index("dp")
    k = lax.rem(sp, 2)
    c = lax.div(sp, 2)
    pk = 1 - k

    def dev(chip, core):
        return (dp, chip * 2 + core)

    partner = dev(c, pk)

    def local(src, dst, i):
        cp = pltpu.make_async_copy(src, dst, lsem.at[i])
        cp.start()
        return cp

    local(p1, posv.at[0], 0)
    local(p2, posv.at[1], 0)
    local(x1, xv.at[pl.ds(0, BLK)], 1)
    local(x2, xv.at[pl.ds(BLK, BLK)], 1)
    l_wkvd = [local(wkvd.at[:, pl.ds(a, n)], wkvd_v.at[:, pl.ds(a, n)], i) for a, n, i in ((0, K_A, 2), (K_A, D_MODEL - K_A, 3))]
    l_gkv = local(gkv, gkv_v, 6)
    l_gq = local(gq, gq_v, 7)
    l_wqd = local(wqd, wqd_v, 4)
    l_wkvu = local(wkvu.at[:, pl.ds(pl.multiple_of(k * 4096, 4096), 4096)], wkvu_v, 5)

    def wait_whole(ref, i):
        pltpu.make_async_copy(ref, ref, lsem.at[i]).wait()

    def wait_bytes(ref, n, sem):
        p = ref.at[pl.ds(0, n)]
        pltpu.make_async_copy(p, p, sem).wait()

    barrier = pltpu.get_barrier_semaphore()
    pl.semaphore_signal(barrier, inc=1, device_id=partner, device_id_type=MESH)
    for j in range(1, NCHIP):
        for core in range(2):
            pl.semaphore_signal(barrier, inc=1, device_id=dev(lax.rem(c + j, NCHIP), core), device_id_type=MESH)

    for b in range(1, NCHIP):
        @pl.when(c < b)
        def _():
            kvlat0[pl.ds(b * CHIP, CHIP), KV_LAT:] = jnp.zeros((CHIP, 128), BF16)
            kvlat1[pl.ds(b * CHIP, CHIP)] = jnp.zeros((CHIP, KV_LAT), BF16)

            def zero(h, _):
                for mb in range(2):
                    kT[mb, h, :, pl.ds(b * CHIP, CHIP)] = jnp.zeros((128, CHIP), BF16)
                    vb[mb, h, pl.ds(b * CHIP, CHIP)] = jnp.zeros((CHIP, 128), BF16)
                return 0
            lax.fori_loop(0, HEADS, zero, 0)

    lane = lax.broadcasted_iota(jnp.int32, (1, 128), 1)
    lo64 = lane < 64
    lo32 = lax.rem(lane, 64) < 32

    wait_whole(posv, 0)
    own = pl.ds(pl.multiple_of(k * CHIP, CHIP), CHIP)
    eye = lax.broadcasted_iota(jnp.int32, (BLK, BLK), 0) == lax.broadcasted_iota(jnp.int32, (BLK, BLK), 1)
    cols = [jnp.sum(jnp.where(eye, posv[mb].astype(F32), 0.0), axis=1, keepdims=True) for mb in range(2)]
    pos_col = jnp.concatenate(cols, axis=0)
    freq = jnp.exp(lax.rem(lane, 32).astype(F32) * (-LN_BASE / 32))
    ang = pos_col * freq
    cos_t = jnp.cos(ang)
    sin_t = jnp.sin(ang)
    sin_t = jnp.where(lo32, -sin_t, sin_t)
    tabs[0, own] = cos_t
    tabs[1, own] = sin_t
    tabs[2, own] = pos_col + jnp.zeros((CHIP, 128), F32)

    def rot(z, cs, sn):
        sw = jnp.where(lo32, pltpu.roll(z, 96, 1), pltpu.roll(z, 32, 1))
        return z * cs + sw * sn

    def kv_down(a, n):
        return lax.dot_general(xv[:, a:a + n], wkvd_v[:, a:a + n], (((1,), (1,)), ((), ())), preferred_element_type=F32)

    with jax.named_scope("wait_x"):
        wait_whole(xv, 1)
        l_wkvd[0].wait()
    l_wqu = local(wqu.at[:, pl.ds(pl.multiple_of(k * 3072, 1024), 3072)], wqu_v, 1)
    usum[...] = kv_down(0, K_A)
    with jax.named_scope("wait_wd"):
        l_wkvd[1].wait()
        l_gkv.wait()
    u = usum[...] + kv_down(K_A, D_MODEL - K_A)
    ur = u[:, KV_LAT:]
    kr = rot(jnp.concatenate([ur, ur], axis=1), cos_t, sin_t)
    kr = jnp.where(lo64, kr[:BLK], kr[BLK:]).astype(BF16)

    ckv = norm_rows(u[:, :KV_LAT], gkv_v[...])

    def rows(chip, core):
        return pl.ds(pl.multiple_of(chip * CHIP + core * BLK, BLK), BLK)

    def chip_rows(chip):
        return pl.ds(pl.multiple_of(chip * CHIP, CHIP), CHIP)

    def part(item, chip, core):
        return kvlat[item].at[rows(chip, core)]

    kvlat[0][rows(c, k), KV_LAT:] = kr
    kvlat[0][rows(c, k), :KV_LAT] = ckv[:BLK]
    kvlat[1][rows(c, k)] = ckv[BLK:]

    with jax.named_scope("barrier"):
        pl.semaphore_wait(barrier, 7)

    def direct(item, j):
        p = part(item, c, k)
        return pltpu.make_async_remote_copy(src_ref=p, dst_ref=p, send_sem=sent.at[0], recv_sem=dr.at[item, j - 1],
                                            device_id=dev(c + j, 1), device_id_type=MESH)

    def direct_recv(item, j):
        p = kvlat[item].at[chip_rows(c - j)]
        return pltpu.make_async_remote_copy(src_ref=p, dst_ref=p, send_sem=sent.at[0], recv_sem=dr.at[item, j - 1],
                                            device_id=partner, device_id_type=MESH)

    def share(item, core):
        p = part(item, c, core)
        return pltpu.make_async_remote_copy(src_ref=p, dst_ref=p, send_sem=sent.at[0], recv_sem=fr.at[0],
                                            device_id=partner, device_id_type=MESH)

    def forward(item, j):
        p = kvlat[item].at[chip_rows(c - j)]
        return pltpu.make_async_remote_copy(src_ref=p, dst_ref=p, send_sem=sent.at[0], recv_sem=fr.at[2 * item + (1 if j == 1 else 2)],
                                            device_id=partner, device_id_type=MESH)

    def send(item, pairs):
        for chip, j in pairs:
            @pl.when(c == chip)
            def _():
                direct(item, j).start()

    send(0, ((0, 3), (0, 2), (0, 1), (1, 2), (1, 1), (2, 1)))
    for item in range(2):
        share(item, k).start()

    l_gq.wait()
    l_wqd.wait()
    with jax.named_scope("q_down"):
        cq = jnp.dot(xv[...], wqd_v[...], preferred_element_type=F32)
        qlat[own] = norm_rows(cq, gq_v[...])

    def q_copy(i, core):
        r = pl.ds(pl.multiple_of(core * CHIP, CHIP), CHIP)
        p = qlat.at[r] if i == 0 else tabs.at[:, r]
        return pltpu.make_async_remote_copy(src_ref=p, dst_ref=p, send_sem=sent.at[0], recv_sem=qr.at[0],
                                            device_id=partner, device_id_type=MESH)

    for i in range(2):
        q_copy(i, k).start()

    def kv_up(lhs, store, turn=True):
        for i in range(4):
            kv = jnp.dot(lhs, wkvu_v[:, i * 1024:(i + 1) * 1024], preferred_element_type=F32).astype(BF16)
            for n in range(4):
                key = kv[:, n * 256:n * 256 + NOPE]
                store(i * 4 + n, key.T if turn else key, kv[:, n * 256 + NOPE:(n + 1) * 256])

    def kv_up_own():
        r = chip_rows(c)

        def store(h, key, val):
            for mb in range(2):
                kT[mb, h, :, r] = key[:, mb * CHIP:(mb + 1) * CHIP]
                vb[mb, h, r] = val[mb * CHIP:(mb + 1) * CHIP]
        kv_up(jnp.concatenate([kvlat0[r, :KV_LAT], kvlat1[r]], axis=0), store)

    def kv_up_device(core, store_key):
        r = rows(c, core)

        def store(h, key, val):
            store_key(h, key)
            for mb in range(2):
                vb[mb, h, r] = val[mb * BLK:(mb + 1) * BLK]
        kv_up(jnp.concatenate([kvlat0[r, :KV_LAT], kvlat1[r]], axis=0), store, False)

    def hold_key(h, key):
        kheld[h] = key

    def join_key(h, key):
        for mb in range(2):
            s = slice(mb * BLK, (mb + 1) * BLK)
            kT[mb, h, :, chip_rows(c)] = jnp.concatenate([key[s], kheld[h, s]], axis=0).T

    def kv_up_rows(mb, r):
        def store(h, key, val):
            kT[mb, h, :, r] = key
            vb[mb, h, r] = val
        kv_up(kvlat[mb][r, :KV_LAT], store)

    send(1, ((2, 1),))
    with jax.named_scope("wait_wkvu"):
        l_wkvu.wait()
    for i, core in enumerate((k, pk)):
        local(wo.at[pl.ds(pl.multiple_of(core * 2048, 2048), 2048)], wo_v.at[pl.ds(i * 2048, 2048)], 0)
    def wait_share():
        with jax.named_scope("wait_partner"):
            wait_bytes(wqd_v, 192, fr.at[0])

    def q_up(i):
        return jnp.dot(qlat[...], wqu_v[:, i * 768:(i + 1) * 768], preferred_element_type=F32)

    def q_store(i, f):
        for pair in range(2):
            t0, t1, t2 = (f[:, pair * 384 + n * 128: pair * 384 + (n + 1) * 128] for n in range(3))
            n1 = pltpu.roll(jnp.where(lo64, t2, t1), 64, 1)
            r = rot(jnp.where(lo64, t1, t2), tabs[0], tabs[1])
            zero = jnp.zeros_like(r)
            q = ((t0.astype(BF16), jnp.where(lo64, r, zero).astype(BF16)),
                 (n1.astype(BF16), jnp.where(lo64, zero, r).astype(BF16)))
            for odd in range(2):
                h = i * 4 + pair * 2 + odd
                for mb in range(2):
                    for core in range(2):
                        s = slice(core * CHIP + mb * BLK, core * CHIP + (mb + 1) * BLK)
                        for n in range(2):
                            qbuf[mb, h, pl.ds(core * BLK, BLK), n * 128:(n + 1) * 128] = q[odd][n][s]

    def queries():
        wait_bytes(wqd_v, 384, qr.at[0])
        for mb in range(2):
            for core in range(2):
                pos = tabs[2, pl.ds(core * CHIP + mb * BLK, BLK), 0:1].astype(jnp.int32)
                qi = c * CHIP + core * BLK + lax.broadcasted_iota(jnp.int32, (BLK, TOK), 0)
                ki = lax.broadcasted_iota(jnp.int32, (BLK, TOK), 1)
                keep = jnp.logical_and(ki <= qi, ki >= qi - pos)
                bias[mb, pl.ds(core * BLK, BLK)] = jnp.where(keep, BIG, NEG)
        l_wqu.wait()
        prev = q_up(0)
        for i in range(4):
            nxt = q_up(i + 1) if i < 3 else None
            q_store(i, prev)
            prev = nxt

    with jax.named_scope("kv_own"):
        @pl.when(k == 0)
        def _():
            wait_share()
            kv_up_own()

        @pl.when(k == 1)
        def _():
            kv_up_device(k, hold_key)
            wait_share()
            kv_up_device(pk, join_key)

    with jax.named_scope("queries"):
        queries()

    def pass_on(item, j):
        direct_recv(item, j).wait_recv()
        forward(item, j).start()

    with jax.named_scope("pass_on"):
        for j, at in ((1, c > 0), (3, c == 3)):
            @pl.when(jnp.logical_and(k == 1, at))
            def _():
                pass_on(0, j)

    send(1, ((0, 3), (0, 2), (0, 1), (1, 2), (1, 1)))

    def o_copy(mb, half):
        cs = pl.ds(half * 1024, 1024)
        return pltpu.make_async_remote_copy(
            src_ref=oall.at[mb, pl.ds(pl.multiple_of(pk * BLK, BLK), BLK), cs], dst_ref=oin.at[pl.ds(mb * BLK, BLK), cs],
            send_sem=sent.at[1], recv_sem=or_.at[mb * half], device_id=partner, device_id_type=MESH)

    def spread_rope():
        r = kvlat0[:, KV_LAT:].T
        for mb in range(2):
            half = r[mb * ROPE:(mb + 1) * ROPE]
            kropeT[mb] = jnp.concatenate([half, half], axis=0)

    def heads(mb, kv_up_first, then={}):
        scores = []
        if mb == 1:
            kv_up_first()
        for h in range(HEADS):
            kcat = jnp.concatenate([kT[mb, h], kropeT[mb]], axis=0)
            scores.append(jnp.dot(qbuf[mb, h], kcat, preferred_element_type=F32))
        if mb == 0:
            kv_up_first()
        probs = []
        for h, s in enumerate(scores):
            s = jnp.minimum(s, bias[mb])
            m = jnp.max(s, axis=1, keepdims=True)
            e = jnp.exp2((s - m) * SCALE2)
            probs.append((e * (1.0 / jnp.sum(e, axis=1, keepdims=True))).astype(BF16))
            if h in then:
                then[h]()
        for h in range(HEADS):
            o = jnp.dot(probs[h], vb[mb, h], preferred_element_type=F32)
            oall[mb, :, h * 128:(h + 1) * 128] = o.astype(BF16)
            if mb == 1 and h == 7:
                o_copy(1, 0).start()
        for half in ((0, 1), (1,))[mb]:
            o_copy(mb, half).start()

    def take(ref, n, i):
        with jax.named_scope("take_wait"):
            @pl.when(k == 0)
            def _():
                wait_bytes(ref, n, fr.at[i])

    def pass_if(at, item, j):
        @pl.when(jnp.logical_and(k == 1, at))
        def _():
            pass_on(item, j)

    @pl.when(c > 0)
    def _():
        take(kvlat0, CHIP, 1)
        with jax.named_scope("take1"):
            kv_up_rows(0, chip_rows(c - 1))

    for n in (2, 3):
        @pl.when(c == n)
        def _():
            pass_if(True, 0, 2)
            take(kvlat0, (n - 1) * CHIP, 2)
            with jax.named_scope("take1"):
                kv_up_rows(0, pl.ds(0, (n - 1) * CHIP))
    spread_rope()
    @pl.when(c == 3)
    def _():
        pass_if(True, 1, 1)
        take(kvlat1, CHIP, 3)

    def third_rows():
        kv_up_rows(1, pl.ds(2 * CHIP, CHIP))

    late = jnp.logical_and(k == 1, c == 3)

    @pl.when(late)
    def _():
        with jax.named_scope("heads1"):
            heads(0, third_rows, {3: lambda: pass_on(1, 3), 8: lambda: pass_on(1, 2)})

    @pl.when(jnp.logical_not(late))
    def _():
        with jax.named_scope("heads1"):
            heads(0, third_rows)

    @pl.when(c == 1)
    def _():
        pass_if(True, 1, 1)
        take(kvlat1, CHIP, 3)

    @pl.when(c == 2)
    def _():
        for j in (1, 2):
            pass_if(True, 1, j)
        for i in (3, 4):
            take(kvlat1, CHIP, i)

    @pl.when(c == 3)
    def _():
        take(kvlat1, 2 * CHIP, 4)

    with jax.named_scope("heads2"):
        heads(1, lambda: kv_up_rows(1, pl.ds(0, 2 * CHIP)))

    with jax.named_scope("out"):
        wait_whole(wo_v, 0)
        orow = pl.ds(pl.multiple_of(k * BLK, BLK), BLK)
        mine = jnp.concatenate([oall[0, orow], oall[1, orow]], axis=0)

        @pl.when(k == 0)
        def _():
            wait_bytes(oin, 96, or_.at[0])
            wait_bytes(oin, 32, or_.at[1])
            y[...] = jnp.dot(jnp.concatenate([mine, oin[...]], axis=1), wo_v[...], preferred_element_type=F32).astype(BF16)

        @pl.when(k == 1)
        def _():
            acc[...] = jnp.dot(mine, wo_v[0:2048], preferred_element_type=F32)
            wait_bytes(oin, 96, or_.at[0])
            acc[...] += jnp.dot(oin[:, :1024], wo_v[2048:3072], preferred_element_type=F32)
            wait_bytes(oin, 32, or_.at[1])
            y[...] = (acc[...] + jnp.dot(oin[:, 1024:], wo_v[3072:], preferred_element_type=F32)).astype(BF16)

    for n in range(NCHIP):
        @pl.when(c == n)
        def _():
            wait_bytes(wqd_v, 192 * (NCHIP - 1 - n) + 192 + 384, sent.at[0])

            if n > 0:
                @pl.when(k == 1)
                def _():
                    wait_bytes(wqd_v, 384 * n, sent.at[0])
    wait_bytes(oin, CHIP, sent.at[1])


def store_body(y, y1, y2, sem):
    for i, out in enumerate((y1, y2)):
        pltpu.make_async_copy(y.at[pl.ds(i * BLK, BLK)], out, sem.at[i]).start()
    for i, out in enumerate((y1, y2)):
        pltpu.make_async_copy(y.at[pl.ds(i * BLK, BLK)], out, sem.at[i]).wait()


def store(y):
    any_spec = pl.BlockSpec(memory_space=pl.ANY)
    return pl.pallas_call(
        store_body,
        out_shape=(jax.ShapeDtypeStruct((BLK, D_MODEL), BF16),) * 2,
        in_specs=[any_spec],
        out_specs=(any_spec,) * 2,
        scratch_shapes=[pltpu.SemaphoreType.DMA((2,))],
        compiler_params=pltpu.CompilerParams(vmem_limit_bytes=2**20),
    )(y)


def solution(mesh):
    tok_spec = P(('dp', 'sp'), None)
    idx_spec = P(('dp', 'sp'))
    any_spec = pl.BlockSpec(memory_space=pl.ANY)
    vmem_spec = pl.BlockSpec(memory_space=pltpu.VMEM)

    def local_body(x_one, seg_one, pos_one, x_two, seg_two, pos_two, w_qdown, gain_q, w_qup, w_kvdown, gain_kv, w_kvup, w_out):
        dma = pltpu.SemaphoreType.DMA
        call = pl.pallas_call(
            body,
            out_shape=jax.ShapeDtypeStruct((CHIP, D_MODEL), BF16),
            in_specs=[pl.BlockSpec(memory_space=pltpu.HBM)] * 11,
            out_specs=vmem_spec,
            scratch_shapes=[
                pltpu.VMEM((CHIP, D_MODEL), BF16),
                pltpu.VMEM((2, 1, BLK), jnp.int32),
                pltpu.VMEM((D_MODEL, Q_LAT), BF16),
                pltpu.VMEM((Q_LAT,), BF16),
                pltpu.VMEM((Q_LAT, 3072), BF16),
                pltpu.VMEM((KV_LAT + ROPE, D_MODEL), BF16),
                pltpu.VMEM((KV_LAT,), BF16),
                pltpu.VMEM((KV_LAT, 4096), BF16),
                pltpu.VMEM((4096, D_MODEL), BF16),
                pltpu.VMEM((TOK, KV_LAT + 128), BF16),
                pltpu.VMEM((TOK, KV_LAT), BF16),
                pltpu.VMEM((2 * CHIP, Q_LAT), BF16),
                pltpu.VMEM((3, 2 * CHIP, 128), F32),
                pltpu.VMEM((2, HEADS, CHIP, 256), BF16),
                pltpu.VMEM((HEADS, CHIP, 128), BF16),
                pltpu.VMEM((2, HEADS, 128, TOK), BF16),
                pltpu.VMEM((2, HEADS, TOK, 128), BF16),
                pltpu.VMEM((2, 128, TOK), BF16),
                pltpu.VMEM((2, CHIP, TOK), F32),
                pltpu.VMEM((2, CHIP, 2048), BF16),
                pltpu.VMEM((CHIP, 2048), BF16),
                pltpu.VMEM((CHIP, D_MODEL), F32),
                pltpu.VMEM((CHIP, KV_LAT + ROPE), F32),
                dma((8,)), dma((2,)), dma((2, 3)), dma((5,)), dma((1,)), dma((2,)),
            ],
            compiler_params=pltpu.CompilerParams(collective_id=0, has_side_effects=True, vmem_limit_bytes=52 * 2**20),
        )
        args = (x_one, pos_one.reshape(1, BLK), x_two, pos_two.reshape(1, BLK), w_qdown, gain_q, w_qup,
                w_kvdown.T, gain_kv, w_kvup, w_out)
        y = call(*(pltpu.with_memory_space_constraint(a, pltpu.HBM) for a in args))
        return store(y)

    return jax.shard_map(local_body, mesh=mesh,
                         in_specs=(tok_spec, idx_spec, idx_spec, tok_spec, idx_spec, idx_spec, P(), P(), P(), P(), P(), P(), P()),
                         out_specs=(tok_spec, tok_spec), check_vma=False)
```

```python
import jax
import jax.numpy as jnp
from jax import lax
from jax.experimental import pallas as pl
from jax.experimental.pallas import tpu as pltpu
from jax.sharding import PartitionSpec as P

MESH = pl.DeviceIdType.MESH
F32 = jnp.float32
BF16 = jnp.bfloat16

D_MODEL = 1792
Q_LAT = 384
KV_LAT = 512
ROPE = 64
NOPE = 128
HEADS = 16
BLK = 64
CHIP = 2 * BLK
TOK = 512
NCHIP = 4
LN_BASE = 9.210340371976184
EPS = 1e-6
K_A = 1024
SCALE2 = 192 ** -0.5 * 1.4426950408889634
NEG = -1e30
BIG = 3.0e38
OFF = -1.5e38
OWN = 3 * CHIP


def norm_rows(z, gain):
    ms = jnp.mean(z * z, axis=-1, keepdims=True)
    return (z * lax.rsqrt(ms + EPS) * gain.astype(F32)[None, :]).astype(BF16)


def body(x1, p1, x2, p2, wqd, gq, wqu, wkvd, gkv, wkvu, wo, y,
         xv, posv, wqd_v, gq_v, wqu_v, wkvd_v, gkv_v, wkvu_v, wo_v,
         kvlat0, kvlat1, qlat, tabs, qbuf, kheld, kT, vb, kropeT, start, flags, causal, oall, oin, acc, usum,
         lsem, sent, dr, fr, qr, or_):
    kvlat = (kvlat0, kvlat1)
    sp = lax.axis_index("sp")
    dp = lax.axis_index("dp")
    k = lax.rem(sp, 2)
    c = lax.div(sp, 2)
    pk = 1 - k

    def dev(chip, core):
        return (dp, chip * 2 + core)

    partner = dev(c, pk)

    def local(src, dst, i):
        cp = pltpu.make_async_copy(src, dst, lsem.at[i])
        cp.start()
        return cp

    local(p1, posv.at[0], 0)
    local(p2, posv.at[1], 0)
    local(x1, xv.at[pl.ds(0, BLK)], 1)
    local(x2, xv.at[pl.ds(BLK, BLK)], 1)
    l_wkvd = [local(wkvd.at[:, pl.ds(a, n)], wkvd_v.at[:, pl.ds(a, n)], i) for a, n, i in ((0, K_A, 2), (K_A, D_MODEL - K_A, 3))]
    l_gkv = local(gkv, gkv_v, 6)
    l_gq = local(gq, gq_v, 7)
    l_wqd = local(wqd, wqd_v, 4)
    l_wkvu = local(wkvu.at[:, pl.ds(pl.multiple_of(k * 4096, 4096), 4096)], wkvu_v, 5)

    def wait_whole(ref, i):
        pltpu.make_async_copy(ref, ref, lsem.at[i]).wait()

    def wait_bytes(ref, n, sem):
        p = ref.at[pl.ds(0, n)]
        pltpu.make_async_copy(p, p, sem).wait()

    barrier = pltpu.get_barrier_semaphore()
    pl.semaphore_signal(barrier, inc=1, device_id=partner, device_id_type=MESH)
    for j in range(1, NCHIP):
        for core in range(2):
            pl.semaphore_signal(barrier, inc=1, device_id=dev(lax.rem(c + j, NCHIP), core), device_id_type=MESH)

    for b in range(NCHIP - 1):
        @pl.when(c <= b)
        def _():
            def zero(h, _):
                kT[0, h, :, pl.ds(b * CHIP, CHIP)] = jnp.zeros((128, CHIP), BF16)
                vb[0, h, pl.ds(b * CHIP, CHIP)] = jnp.zeros((CHIP, 128), BF16)
                return 0
            lax.fori_loop(0, HEADS, zero, 0)

        @pl.when(c < b)
        def _():
            kvlat0[pl.ds(b * CHIP, CHIP), KV_LAT:] = jnp.zeros((CHIP, 128), BF16)
            kvlat1[pl.ds(b * CHIP, CHIP)] = jnp.zeros((CHIP, KV_LAT), BF16)

    tri = lax.broadcasted_iota(jnp.int32, (CHIP, CHIP), 1) <= lax.broadcasted_iota(jnp.int32, (CHIP, CHIP), 0)
    causal[...] = jnp.where(tri, BIG, NEG)

    lane = lax.broadcasted_iota(jnp.int32, (1, 128), 1)
    lo64 = lane < 64
    lane64 = lax.rem(lane, 64)
    lo32 = lax.rem(lane, 64) < 32

    wait_whole(posv, 0)
    own = pl.ds(pl.multiple_of(k * CHIP, CHIP), CHIP)
    eye = lax.broadcasted_iota(jnp.int32, (BLK, BLK), 0) == lax.broadcasted_iota(jnp.int32, (BLK, BLK), 1)
    cols = [jnp.sum(jnp.where(eye, posv[mb].astype(F32), 0.0), axis=1, keepdims=True) for mb in range(2)]
    pos_col = jnp.concatenate(cols, axis=0)
    freq = jnp.exp(lax.rem(lane, 32).astype(F32) * (-LN_BASE / 32))
    ang = pos_col * freq
    cos_t = jnp.cos(ang)
    sin_t = jnp.sin(ang)
    sin_t = jnp.where(lo32, -sin_t, sin_t)
    tabs[0, own] = cos_t
    tabs[1, own] = sin_t
    tabs[2, own] = pos_col + jnp.zeros((CHIP, 128), F32)

    def rot(z, cs, sn):
        sw = jnp.where(lo32, pltpu.roll(z, 96, 1), pltpu.roll(z, 32, 1))
        return z * cs + sw * sn

    def kv_down(a, n):
        return lax.dot_general(xv[:, a:a + n], wkvd_v[:, a:a + n], (((1,), (1,)), ((), ())), preferred_element_type=F32)

    with jax.named_scope("wait_x"):
        wait_whole(xv, 1)
        l_wkvd[0].wait()
    l_wqu = local(wqu.at[:, pl.ds(pl.multiple_of(k * 3072, 1024), 3072)], wqu_v, 1)
    usum[...] = kv_down(0, K_A)
    with jax.named_scope("wait_wd"):
        l_wkvd[1].wait()
        l_gkv.wait()
    u = usum[...] + kv_down(K_A, D_MODEL - K_A)
    ur = u[:, KV_LAT:]
    kr = rot(jnp.concatenate([ur, ur], axis=1), cos_t, sin_t)
    kr = jnp.where(lo64, kr[:BLK], kr[BLK:]).astype(BF16)

    ckv = norm_rows(u[:, :KV_LAT], gkv_v[...])

    def rows(chip, core):
        return pl.ds(pl.multiple_of(chip * CHIP + core * BLK, BLK), BLK)

    def chip_rows(chip):
        return pl.ds(pl.multiple_of(chip * CHIP, CHIP), CHIP)

    def part(item, chip, core):
        return kvlat[item].at[rows(chip, core)]

    kvlat[0][rows(c, k), KV_LAT:] = kr
    kvlat[0][rows(c, k), :KV_LAT] = ckv[:BLK]
    kvlat[1][rows(c, k)] = ckv[BLK:]

    with jax.named_scope("barrier"):
        pl.semaphore_wait(barrier, 7)

    def direct(item, j):
        p = part(item, c, k)
        return pltpu.make_async_remote_copy(src_ref=p, dst_ref=p, send_sem=sent.at[0], recv_sem=dr.at[item, j - 1],
                                            device_id=dev(c + j, 1), device_id_type=MESH)

    def direct_recv(item, j):
        p = kvlat[item].at[chip_rows(c - j)]
        return pltpu.make_async_remote_copy(src_ref=p, dst_ref=p, send_sem=sent.at[0], recv_sem=dr.at[item, j - 1],
                                            device_id=partner, device_id_type=MESH)

    def share(item, core):
        p = part(item, c, core)
        return pltpu.make_async_remote_copy(src_ref=p, dst_ref=p, send_sem=sent.at[0], recv_sem=fr.at[0],
                                            device_id=partner, device_id_type=MESH)

    def forward(item, j):
        p = kvlat[item].at[chip_rows(c - j)]
        return pltpu.make_async_remote_copy(src_ref=p, dst_ref=p, send_sem=sent.at[0], recv_sem=fr.at[2 * item + (1 if j == 1 else 2)],
                                            device_id=partner, device_id_type=MESH)

    def send(item, pairs):
        for chip, j in pairs:
            @pl.when(c == chip)
            def _():
                direct(item, j).start()

    send(0, ((0, 3), (0, 2), (0, 1), (1, 2), (1, 1), (2, 1)))
    for item in range(2):
        share(item, k).start()

    l_gq.wait()
    l_wqd.wait()
    with jax.named_scope("q_down"):
        cq = jnp.dot(xv[...], wqd_v[...], preferred_element_type=F32)
        qlat[own] = norm_rows(cq, gq_v[...])

    def q_copy(i, core):
        r = pl.ds(pl.multiple_of(core * CHIP, CHIP), CHIP)
        p = qlat.at[r] if i == 0 else tabs.at[:, r]
        return pltpu.make_async_remote_copy(src_ref=p, dst_ref=p, send_sem=sent.at[0], recv_sem=qr.at[0],
                                            device_id=partner, device_id_type=MESH)

    for i in range(2):
        q_copy(i, k).start()

    def kv_up(lhs, store, turn=True):
        for i in range(4):
            kv = jnp.dot(lhs, wkvu_v[:, i * 1024:(i + 1) * 1024], preferred_element_type=F32).astype(BF16)
            for n in range(4):
                key = kv[:, n * 256:n * 256 + NOPE]
                store(i * 4 + n, key.T if turn else key, kv[:, n * 256 + NOPE:(n + 1) * 256])

    def kv_up_own():
        r = chip_rows(c)

        def store(h, key, val):
            for mb in range(2):
                kT[mb, h, :, OWN:] = key[:, mb * CHIP:(mb + 1) * CHIP]
                vb[mb, h, OWN:] = val[mb * CHIP:(mb + 1) * CHIP]
        kv_up(jnp.concatenate([kvlat0[r, :KV_LAT], kvlat1[r]], axis=0), store)

    def kv_up_device(core, store_key):
        r = rows(c, core)

        def store(h, key, val):
            store_key(h, key)
            for mb in range(2):
                vb[mb, h, pl.ds(pl.multiple_of(OWN + core * BLK, BLK), BLK)] = val[mb * BLK:(mb + 1) * BLK]
        kv_up(jnp.concatenate([kvlat0[r, :KV_LAT], kvlat1[r]], axis=0), store, False)

    def hold_key(h, key):
        kheld[h] = key

    def join_key(h, key):
        for mb in range(2):
            s = slice(mb * BLK, (mb + 1) * BLK)
            kT[mb, h, :, OWN:] = jnp.concatenate([key[s], kheld[h, s]], axis=0).T

    def kv_up_rows(mb, r):
        def store(h, key, val):
            kT[mb, h, :, r] = key
            vb[mb, h, r] = val
        kv_up(kvlat[mb][r, :KV_LAT], store)

    send(1, ((2, 1),))
    with jax.named_scope("wait_wkvu"):
        l_wkvu.wait()
    for i, core in enumerate((k, pk)):
        local(wo.at[pl.ds(pl.multiple_of(core * 2048, 2048), 2048)], wo_v.at[pl.ds(i * 2048, 2048)], 0)
    def wait_share():
        with jax.named_scope("wait_partner"):
            wait_bytes(wqd_v, 192, fr.at[0])

    def q_up(i):
        return jnp.dot(qlat[...], wqu_v[:, i * 768:(i + 1) * 768], preferred_element_type=F32)

    def q_store(i, f):
        for pair in range(2):
            t0, t1, t2 = (f[:, pair * 384 + n * 128: pair * 384 + (n + 1) * 128] for n in range(3))
            n1 = pltpu.roll(jnp.where(lo64, t2, t1), 64, 1)
            r = rot(jnp.where(lo64, t1, t2), tabs[0], tabs[1])
            q = ((t0.astype(BF16), jnp.where(lo64, r, flags[...]).astype(BF16)),
                 (n1.astype(BF16), jnp.where(lo64, flags[...], r).astype(BF16)))
            for odd in range(2):
                h = i * 4 + pair * 2 + odd
                for mb in range(2):
                    for core in range(2):
                        s = slice(core * CHIP + mb * BLK, core * CHIP + (mb + 1) * BLK)
                        for n in range(2):
                            qbuf[mb, h, pl.ds(core * BLK, BLK), n * 128:(n + 1) * 128] = q[odd][n][s]

    def queries():
        wait_bytes(wqd_v, 384, qr.at[0])
        row = lax.broadcasted_iota(jnp.int32, (2 * CHIP, 1), 0)
        index = c * CHIP + lax.div(row, CHIP) * BLK + lax.rem(row, BLK)
        start[...] = index.astype(F32) - tabs[2]
        flags[...] = jnp.where(lane64 == 0, (start[...] > 0.5).astype(F32), (lane64 == 1).astype(F32))
        col = lax.broadcasted_iota(jnp.int32, (ROPE, TOK), 1)
        kind = lax.broadcasted_iota(jnp.int32, (ROPE, TOK), 0)
        place = jnp.where(col < OWN, col, c * CHIP + col - OWN).astype(F32)
        empty = jnp.logical_and(col >= c * CHIP, col < OWN)
        for mb in range(2):
            firsts = [jnp.max(start[pl.ds(core * CHIP + mb * BLK, BLK)], axis=0, keepdims=True) for core in range(2)]
            first = jnp.maximum(firsts[0], firsts[1])
            before = place < jnp.concatenate([first] * 4, axis=1)
            off = jnp.logical_or(jnp.logical_and(kind == 0, before), jnp.logical_and(kind == 1, empty))
            masks = jnp.where(off, OFF, 0.0).astype(BF16)
            kropeT[mb, 0, ROPE:] = masks
            kropeT[mb, 1, :ROPE] = masks
        l_wqu.wait()
        prev = q_up(0)
        for i in range(4):
            nxt = q_up(i + 1) if i < 3 else None
            q_store(i, prev)
            prev = nxt

    with jax.named_scope("kv_own"):
        @pl.when(k == 0)
        def _():
            wait_share()
            kv_up_own()

        @pl.when(k == 1)
        def _():
            kv_up_device(k, hold_key)
            wait_share()
            kv_up_device(pk, join_key)

    with jax.named_scope("queries"):
        queries()

    def pass_on(item, j):
        direct_recv(item, j).wait_recv()
        forward(item, j).start()

    with jax.named_scope("pass_on"):
        for j, at in ((1, c > 0), (3, c == 3)):
            @pl.when(jnp.logical_and(k == 1, at))
            def _():
                pass_on(0, j)

    send(1, ((0, 3), (0, 2), (0, 1), (1, 2), (1, 1)))

    def o_copy(mb, half):
        cs = pl.ds(half * 1024, 1024)
        return pltpu.make_async_remote_copy(
            src_ref=oall.at[mb, pl.ds(pl.multiple_of(pk * BLK, BLK), BLK), cs], dst_ref=oin.at[pl.ds(mb * BLK, BLK), cs],
            send_sem=sent.at[1], recv_sem=or_.at[mb * half], device_id=partner, device_id_type=MESH)

    def shared_keys():
        r = jnp.concatenate([kvlat0[0:OWN, KV_LAT:], kvlat0[chip_rows(c), KV_LAT:]], axis=0).T
        for mb in range(2):
            kropeT[mb, 0, :ROPE] = r[mb * ROPE:(mb + 1) * ROPE]
            kropeT[mb, 1, ROPE:] = r[mb * ROPE:(mb + 1) * ROPE]

    def heads(mb, kv_up_first, then={}):
        scores = []
        if mb == 1:
            kv_up_first()
        for h in range(HEADS):
            kcat = jnp.concatenate([kT[mb, h], kropeT[mb, h % 2]], axis=0)
            scores.append(jnp.dot(qbuf[mb, h], kcat, preferred_element_type=F32))
        if mb == 0:
            kv_up_first()
        probs = []
        for h, s in enumerate(scores):
            s = jnp.concatenate([s[:, :OWN], jnp.minimum(s[:, OWN:], causal[...])], axis=1)
            m = jnp.max(s, axis=1, keepdims=True)
            e = jnp.exp2((s - m) * SCALE2)
            probs.append((e * (1.0 / jnp.sum(e, axis=1, keepdims=True))).astype(BF16))
            if h in then:
                then[h]()
        for h in range(HEADS):
            o = jnp.dot(probs[h], vb[mb, h], preferred_element_type=F32)
            oall[mb, :, h * 128:(h + 1) * 128] = o.astype(BF16)
            if mb == 1 and h == 7:
                o_copy(1, 0).start()
        for half in ((0, 1), (1,))[mb]:
            o_copy(mb, half).start()

    def take(ref, n, i):
        with jax.named_scope("take_wait"):
            @pl.when(k == 0)
            def _():
                wait_bytes(ref, n, fr.at[i])

    def pass_if(at, item, j):
        @pl.when(jnp.logical_and(k == 1, at))
        def _():
            pass_on(item, j)

    @pl.when(c > 0)
    def _():
        take(kvlat0, CHIP, 1)
        with jax.named_scope("take1"):
            kv_up_rows(0, chip_rows(c - 1))

    for n in (2, 3):
        @pl.when(c == n)
        def _():
            pass_if(True, 0, 2)
            take(kvlat0, (n - 1) * CHIP, 2)
            with jax.named_scope("take1"):
                kv_up_rows(0, pl.ds(0, (n - 1) * CHIP))
    shared_keys()
    @pl.when(c == 3)
    def _():
        pass_if(True, 1, 1)
        take(kvlat1, CHIP, 3)

    def third_rows():
        kv_up_rows(1, pl.ds(2 * CHIP, CHIP))

    late = jnp.logical_and(k == 1, c == 3)

    @pl.when(late)
    def _():
        with jax.named_scope("heads1"):
            heads(0, third_rows, {3: lambda: pass_on(1, 3), 8: lambda: pass_on(1, 2)})

    @pl.when(jnp.logical_not(late))
    def _():
        with jax.named_scope("heads1"):
            heads(0, third_rows)

    @pl.when(c == 1)
    def _():
        pass_if(True, 1, 1)
        take(kvlat1, CHIP, 3)

    @pl.when(c == 2)
    def _():
        for j in (1, 2):
            pass_if(True, 1, j)
        for i in (3, 4):
            take(kvlat1, CHIP, i)

    @pl.when(c == 3)
    def _():
        take(kvlat1, 2 * CHIP, 4)

    with jax.named_scope("heads2"):
        heads(1, lambda: kv_up_rows(1, pl.ds(0, 2 * CHIP)))

    with jax.named_scope("out"):
        wait_whole(wo_v, 0)
        orow = pl.ds(pl.multiple_of(k * BLK, BLK), BLK)
        mine = jnp.concatenate([oall[0, orow], oall[1, orow]], axis=0)

        @pl.when(k == 0)
        def _():
            wait_bytes(oin, 96, or_.at[0])
            wait_bytes(oin, 32, or_.at[1])
            y[...] = jnp.dot(jnp.concatenate([mine, oin[...]], axis=1), wo_v[...], preferred_element_type=F32).astype(BF16)

        @pl.when(k == 1)
        def _():
            acc[...] = jnp.dot(mine, wo_v[0:2048], preferred_element_type=F32)
            wait_bytes(oin, 96, or_.at[0])
            acc[...] += jnp.dot(oin[:, :1024], wo_v[2048:3072], preferred_element_type=F32)
            wait_bytes(oin, 32, or_.at[1])
            y[...] = (acc[...] + jnp.dot(oin[:, 1024:], wo_v[3072:], preferred_element_type=F32)).astype(BF16)

    for n in range(NCHIP):
        @pl.when(c == n)
        def _():
            wait_bytes(wqd_v, 192 * (NCHIP - 1 - n) + 192 + 384, sent.at[0])

            if n > 0:
                @pl.when(k == 1)
                def _():
                    wait_bytes(wqd_v, 384 * n, sent.at[0])
    wait_bytes(oin, CHIP, sent.at[1])


def store_body(y, y1, y2, sem):
    for i, out in enumerate((y1, y2)):
        pltpu.make_async_copy(y.at[pl.ds(i * BLK, BLK)], out, sem.at[i]).start()
    for i, out in enumerate((y1, y2)):
        pltpu.make_async_copy(y.at[pl.ds(i * BLK, BLK)], out, sem.at[i]).wait()


def store(y):
    any_spec = pl.BlockSpec(memory_space=pl.ANY)
    return pl.pallas_call(
        store_body,
        out_shape=(jax.ShapeDtypeStruct((BLK, D_MODEL), BF16),) * 2,
        in_specs=[any_spec],
        out_specs=(any_spec,) * 2,
        scratch_shapes=[pltpu.SemaphoreType.DMA((2,))],
        compiler_params=pltpu.CompilerParams(vmem_limit_bytes=2**20),
    )(y)


def solution(mesh):
    tok_spec = P(('dp', 'sp'), None)
    idx_spec = P(('dp', 'sp'))
    any_spec = pl.BlockSpec(memory_space=pl.ANY)
    vmem_spec = pl.BlockSpec(memory_space=pltpu.VMEM)

    def local_body(x_one, seg_one, pos_one, x_two, seg_two, pos_two, w_qdown, gain_q, w_qup, w_kvdown, gain_kv, w_kvup, w_out):
        dma = pltpu.SemaphoreType.DMA
        call = pl.pallas_call(
            body,
            out_shape=jax.ShapeDtypeStruct((CHIP, D_MODEL), BF16),
            in_specs=[pl.BlockSpec(memory_space=pltpu.HBM)] * 11,
            out_specs=vmem_spec,
            scratch_shapes=[
                pltpu.VMEM((CHIP, D_MODEL), BF16),
                pltpu.VMEM((2, 1, BLK), jnp.int32),
                pltpu.VMEM((D_MODEL, Q_LAT), BF16),
                pltpu.VMEM((Q_LAT,), BF16),
                pltpu.VMEM((Q_LAT, 3072), BF16),
                pltpu.VMEM((KV_LAT + ROPE, D_MODEL), BF16),
                pltpu.VMEM((KV_LAT,), BF16),
                pltpu.VMEM((KV_LAT, 4096), BF16),
                pltpu.VMEM((4096, D_MODEL), BF16),
                pltpu.VMEM((TOK, KV_LAT + 128), BF16),
                pltpu.VMEM((TOK, KV_LAT), BF16),
                pltpu.VMEM((2 * CHIP, Q_LAT), BF16),
                pltpu.VMEM((3, 2 * CHIP, 128), F32),
                pltpu.VMEM((2, HEADS, CHIP, 256), BF16),
                pltpu.VMEM((HEADS, CHIP, 128), BF16),
                pltpu.VMEM((2, HEADS, 128, TOK), BF16),
                pltpu.VMEM((2, HEADS, TOK, 128), BF16),
                pltpu.VMEM((2, 2, 128, TOK), BF16),
                pltpu.VMEM((2 * CHIP, 128), F32),
                pltpu.VMEM((2 * CHIP, 128), F32),
                pltpu.VMEM((CHIP, CHIP), F32),
                pltpu.VMEM((2, CHIP, 2048), BF16),
                pltpu.VMEM((CHIP, 2048), BF16),
                pltpu.VMEM((CHIP, D_MODEL), F32),
                pltpu.VMEM((CHIP, KV_LAT + ROPE), F32),
                dma((8,)), dma((2,)), dma((2, 3)), dma((5,)), dma((1,)), dma((2,)),
            ],
            compiler_params=pltpu.CompilerParams(collective_id=0, has_side_effects=True, vmem_limit_bytes=52 * 2**20),
        )
        args = (x_one, pos_one.reshape(1, BLK), x_two, pos_two.reshape(1, BLK), w_qdown, gain_q, w_qup,
                w_kvdown.T, gain_kv, w_kvup, w_out)
        y = call(*(pltpu.with_memory_space_constraint(a, pltpu.HBM) for a in args))
        return store(y)

    return jax.shard_map(local_body, mesh=mesh,
                         in_specs=(tok_spec, idx_spec, idx_spec, tok_spec, idx_spec, idx_spec, P(), P(), P(), P(), P(), P(), P()),
                         out_specs=(tok_spec, tok_spec), check_vma=False)
```

```python
import jax
import jax.numpy as jnp
from jax import lax
from jax.experimental import pallas as pl
from jax.experimental.pallas import tpu as pltpu
from jax.sharding import PartitionSpec as P

MESH = pl.DeviceIdType.MESH
F32 = jnp.float32
BF16 = jnp.bfloat16

D_MODEL = 1792
Q_LAT = 384
KV_LAT = 512
ROPE = 64
NOPE = 128
HEADS = 16
BLK = 64
CHIP = 2 * BLK
TOK = 512
NCHIP = 4
LN_BASE = 9.210340371976184
EPS = 1e-6
K_A = 768
SCALE2 = 192 ** -0.5 * 1.4426950408889634
NEG = -1e30
BIG = 3.0e38
OFF = -1.5e38
OWN = 3 * CHIP


def norm_rows(z, gain):
    ms = jnp.mean(z * z, axis=-1, keepdims=True)
    return (z * lax.rsqrt(ms + EPS) * gain.astype(F32)[None, :]).astype(BF16)


def body(x1, p1, x2, p2, wqd, gq, wqu, wkvd, gkv, wkvu, wo, y,
         xv, posv, wqd_v, gq_v, wqu_v, wkvd_v, gkv_v, wkvu_v, wo_v,
         kvlat0, kvlat1, qlat, tabs, qbuf, kheld, kT, vb, kropeT, start, flags, causal, oall, oin, acc, usum,
         lsem, sent, dr, fr, qr, or_):
    kvlat = (kvlat0, kvlat1)
    sp = lax.axis_index("sp")
    dp = lax.axis_index("dp")
    k = lax.rem(sp, 2)
    c = lax.div(sp, 2)
    pk = 1 - k

    def dev(chip, core):
        return (dp, chip * 2 + core)

    partner = dev(c, pk)

    def local(src, dst, i):
        cp = pltpu.make_async_copy(src, dst, lsem.at[i])
        cp.start()
        return cp

    local(p1, posv.at[0], 0)
    local(p2, posv.at[1], 0)
    local(x1, xv.at[pl.ds(0, BLK)], 1)
    local(x2, xv.at[pl.ds(BLK, BLK)], 1)
    l_wkvd = [local(wkvd.at[:, pl.ds(a, n)], wkvd_v.at[:, pl.ds(a, n)], i) for a, n, i in ((0, K_A, 2), (K_A, D_MODEL - K_A, 3))]
    l_gkv = local(gkv, gkv_v, 6)
    l_gq = local(gq, gq_v, 7)
    l_wqd = local(wqd, wqd_v, 4)
    l_wkvu = local(wkvu.at[:, pl.ds(pl.multiple_of(k * 4096, 4096), 4096)], wkvu_v, 5)

    def wait_whole(ref, i):
        pltpu.make_async_copy(ref, ref, lsem.at[i]).wait()

    def wait_bytes(ref, n, sem):
        p = ref.at[pl.ds(0, n)]
        pltpu.make_async_copy(p, p, sem).wait()

    barrier = pltpu.get_barrier_semaphore()
    pl.semaphore_signal(barrier, inc=1, device_id=partner, device_id_type=MESH)
    for j in range(1, NCHIP):
        for core in range(2):
            pl.semaphore_signal(barrier, inc=1, device_id=dev(lax.rem(c + j, NCHIP), core), device_id_type=MESH)

    for b in range(NCHIP - 1):
        @pl.when(c <= b)
        def _():
            def zero(h, _):
                kT[0, h, :, pl.ds(b * CHIP, CHIP)] = jnp.zeros((128, CHIP), BF16)
                vb[0, h, pl.ds(b * CHIP, CHIP)] = jnp.zeros((CHIP, 128), BF16)
                return 0
            lax.fori_loop(0, HEADS, zero, 0)

        @pl.when(c < b)
        def _():
            kvlat0[pl.ds(b * CHIP, CHIP), KV_LAT:] = jnp.zeros((CHIP, 128), BF16)
            kvlat1[pl.ds(b * CHIP, CHIP)] = jnp.zeros((CHIP, KV_LAT), BF16)

    tri = lax.broadcasted_iota(jnp.int32, (CHIP, CHIP), 1) <= lax.broadcasted_iota(jnp.int32, (CHIP, CHIP), 0)
    causal[...] = jnp.where(tri, BIG, NEG)

    lane = lax.broadcasted_iota(jnp.int32, (1, 128), 1)
    lo64 = lane < 64
    lane64 = lax.rem(lane, 64)
    lo32 = lax.rem(lane, 64) < 32

    wait_whole(posv, 0)
    own = pl.ds(pl.multiple_of(k * CHIP, CHIP), CHIP)
    eye = lax.broadcasted_iota(jnp.int32, (BLK, BLK), 0) == lax.broadcasted_iota(jnp.int32, (BLK, BLK), 1)
    cols = [jnp.sum(jnp.where(eye, posv[mb].astype(F32), 0.0), axis=1, keepdims=True) for mb in range(2)]
    pos_col = jnp.concatenate(cols, axis=0)
    freq = jnp.exp(lax.rem(lane, 32).astype(F32) * (-LN_BASE / 32))
    ang = pos_col * freq
    cos_t = jnp.cos(ang)
    sin_t = jnp.sin(ang)
    sin_t = jnp.where(lo32, -sin_t, sin_t)
    tabs[0, own] = cos_t
    tabs[1, own] = sin_t
    tabs[2, own] = pos_col + jnp.zeros((CHIP, 128), F32)

    def rot(z, cs, sn):
        sw = jnp.where(lo32, pltpu.roll(z, 96, 1), pltpu.roll(z, 32, 1))
        return z * cs + sw * sn

    def kv_down(a, n):
        return lax.dot_general(xv[:, a:a + n], wkvd_v[:, a:a + n], (((1,), (1,)), ((), ())), preferred_element_type=F32)

    with jax.named_scope("wait_x"):
        wait_whole(xv, 1)
        l_wkvd[0].wait()
    l_wqu = local(wqu.at[:, pl.ds(pl.multiple_of(k * 3072, 1024), 3072)], wqu_v, 1)
    usum[...] = kv_down(0, K_A)
    with jax.named_scope("wait_wd"):
        l_wkvd[1].wait()
        l_gkv.wait()
    u = usum[...] + kv_down(K_A, D_MODEL - K_A)
    ur = u[:, KV_LAT:]
    kr = rot(jnp.concatenate([ur, ur], axis=1), cos_t, sin_t)
    kr = jnp.where(lo64, kr[:BLK], kr[BLK:]).astype(BF16)

    ckv = norm_rows(u[:, :KV_LAT], gkv_v[...])

    def rows(chip, core):
        return pl.ds(pl.multiple_of(chip * CHIP + core * BLK, BLK), BLK)

    def chip_rows(chip):
        return pl.ds(pl.multiple_of(chip * CHIP, CHIP), CHIP)

    def part(item, chip, core):
        return kvlat[item].at[rows(chip, core)]

    kvlat[0][rows(c, k), KV_LAT:] = kr
    kvlat[0][rows(c, k), :KV_LAT] = ckv[:BLK]
    kvlat[1][rows(c, k)] = ckv[BLK:]

    with jax.named_scope("barrier"):
        pl.semaphore_wait(barrier, 7)

    def direct(item, j):
        p = part(item, c, k)
        return pltpu.make_async_remote_copy(src_ref=p, dst_ref=p, send_sem=sent.at[0], recv_sem=dr.at[item, j - 1],
                                            device_id=dev(c + j, 1), device_id_type=MESH)

    def direct_recv(item, j):
        p = kvlat[item].at[chip_rows(c - j)]
        return pltpu.make_async_remote_copy(src_ref=p, dst_ref=p, send_sem=sent.at[0], recv_sem=dr.at[item, j - 1],
                                            device_id=partner, device_id_type=MESH)

    def share(item, core):
        p = part(item, c, core)
        return pltpu.make_async_remote_copy(src_ref=p, dst_ref=p, send_sem=sent.at[0], recv_sem=fr.at[0],
                                            device_id=partner, device_id_type=MESH)

    def forward(item, j):
        p = kvlat[item].at[chip_rows(c - j)]
        return pltpu.make_async_remote_copy(src_ref=p, dst_ref=p, send_sem=sent.at[0], recv_sem=fr.at[2 * item + (1 if j == 1 else 2)],
                                            device_id=partner, device_id_type=MESH)

    def send(item, pairs):
        for chip, j in pairs:
            @pl.when(c == chip)
            def _():
                direct(item, j).start()

    send(0, ((0, 3), (0, 2), (0, 1), (1, 2), (1, 1), (2, 1)))
    for item in range(2):
        share(item, k).start()

    l_gq.wait()
    l_wqd.wait()
    with jax.named_scope("q_down"):
        cq = jnp.dot(xv[...], wqd_v[...], preferred_element_type=F32)
        qlat[own] = norm_rows(cq, gq_v[...])

    def q_copy(i, core):
        r = pl.ds(pl.multiple_of(core * CHIP, CHIP), CHIP)
        p = qlat.at[r] if i == 0 else tabs.at[:, r]
        return pltpu.make_async_remote_copy(src_ref=p, dst_ref=p, send_sem=sent.at[0], recv_sem=qr.at[0],
                                            device_id=partner, device_id_type=MESH)

    for i in range(2):
        q_copy(i, k).start()

    def turned(h, key):
        t = key.T
        return jnp.concatenate([t[64:], t[:64]], axis=0) if h % 2 else t

    def kv_up(lhs, store, turn=True):
        for i in range(4):
            kv = jnp.dot(lhs, wkvu_v[:, i * 1024:(i + 1) * 1024], preferred_element_type=F32).astype(BF16)
            for n in range(4):
                key = kv[:, n * 256:n * 256 + NOPE]
                store(i * 4 + n, turned(i * 4 + n, key) if turn else key, kv[:, n * 256 + NOPE:(n + 1) * 256])

    def kv_up_own():
        r = chip_rows(c)

        def store(h, key, val):
            for mb in range(2):
                kT[mb, h, :, OWN:] = key[:, mb * CHIP:(mb + 1) * CHIP]
                vb[mb, h, OWN:] = val[mb * CHIP:(mb + 1) * CHIP]
        kv_up(jnp.concatenate([kvlat0[r, :KV_LAT], kvlat1[r]], axis=0), store)

    def kv_up_device(core, store_key):
        r = rows(c, core)

        def store(h, key, val):
            store_key(h, key)
            for mb in range(2):
                vb[mb, h, pl.ds(pl.multiple_of(OWN + core * BLK, BLK), BLK)] = val[mb * BLK:(mb + 1) * BLK]
        kv_up(jnp.concatenate([kvlat0[r, :KV_LAT], kvlat1[r]], axis=0), store, False)

    def hold_key(h, key):
        kheld[h] = key

    def join_key(h, key):
        for mb in range(2):
            s = slice(mb * BLK, (mb + 1) * BLK)
            kT[mb, h, :, OWN:] = turned(h, jnp.concatenate([key[s], kheld[h, s]], axis=0))

    def kv_up_rows(mb, r):
        def store(h, key, val):
            kT[mb, h, :, r] = key
            vb[mb, h, r] = val
        kv_up(kvlat[mb][r, :KV_LAT], store)

    send(1, ((2, 1),))
    with jax.named_scope("wait_wkvu"):
        l_wkvu.wait()
    for i, core in enumerate((k, pk)):
        local(wo.at[pl.ds(pl.multiple_of(core * 2048, 2048), 2048)], wo_v.at[pl.ds(i * 2048, 2048)], 0)
    def wait_share():
        with jax.named_scope("wait_partner"):
            wait_bytes(wqd_v, 192, fr.at[0])

    def q_up(i):
        return jnp.dot(qlat[...], wqu_v[:, i * 768:(i + 1) * 768], preferred_element_type=F32)

    def q_store(i, f):
        for pair in range(2):
            t0, t1, t2 = (f[:, pair * 384 + n * 128: pair * 384 + (n + 1) * 128] for n in range(3))
            n1 = jnp.where(lo64, t2, t1)
            r = rot(jnp.where(lo64, t1, t2), tabs[0], tabs[1])
            q = ((t0.astype(BF16), jnp.where(lo64, r, flags[...]).astype(BF16)),
                 (n1.astype(BF16), jnp.where(lo64, flags[...], r).astype(BF16)))
            for odd in range(2):
                h = i * 4 + pair * 2 + odd
                for mb in range(2):
                    for core in range(2):
                        s = slice(core * CHIP + mb * BLK, core * CHIP + (mb + 1) * BLK)
                        for n in range(2):
                            qbuf[mb, h, pl.ds(core * BLK, BLK), n * 128:(n + 1) * 128] = q[odd][n][s]

    def queries():
        wait_bytes(wqd_v, 384, qr.at[0])
        row = lax.broadcasted_iota(jnp.int32, (2 * CHIP, 1), 0)
        index = c * CHIP + lax.div(row, CHIP) * BLK + lax.rem(row, BLK)
        start[...] = index.astype(F32) - tabs[2]
        flags[...] = jnp.where(lane64 == 0, (start[...] > 0.5).astype(F32), (lane64 == 1).astype(F32))
        col = lax.broadcasted_iota(jnp.int32, (ROPE, TOK), 1)
        kind = lax.broadcasted_iota(jnp.int32, (ROPE, TOK), 0)
        place = jnp.where(col < OWN, col, c * CHIP + col - OWN).astype(F32)
        empty = jnp.logical_and(col >= c * CHIP, col < OWN)
        for mb in range(2):
            firsts = [jnp.max(start[pl.ds(core * CHIP + mb * BLK, BLK)], axis=0, keepdims=True) for core in range(2)]
            first = jnp.maximum(firsts[0], firsts[1])
            before = place < jnp.concatenate([first] * 4, axis=1)
            off = jnp.logical_or(jnp.logical_and(kind == 0, before), jnp.logical_and(kind == 1, empty))
            masks = jnp.where(off, OFF, 0.0).astype(BF16)
            kropeT[mb, 0, ROPE:] = masks
            kropeT[mb, 1, :ROPE] = masks
        l_wqu.wait()
        prev = q_up(0)
        for i in range(4):
            nxt = q_up(i + 1) if i < 3 else None
            q_store(i, prev)
            prev = nxt

    with jax.named_scope("kv_own"):
        @pl.when(k == 0)
        def _():
            wait_share()
            kv_up_own()

        @pl.when(k == 1)
        def _():
            kv_up_device(k, hold_key)
            wait_share()
            kv_up_device(pk, join_key)

    with jax.named_scope("queries"):
        queries()

    def pass_on(item, j):
        direct_recv(item, j).wait_recv()
        forward(item, j).start()

    with jax.named_scope("pass_on"):
        for j, at in ((1, c > 0), (3, c == 3)):
            @pl.when(jnp.logical_and(k == 1, at))
            def _():
                pass_on(0, j)

    send(1, ((0, 3), (0, 2), (0, 1), (1, 2), (1, 1)))

    def o_copy(mb, half):
        cs = pl.ds(half * 1024, 1024)
        return pltpu.make_async_remote_copy(
            src_ref=oall.at[mb, pl.ds(pl.multiple_of(pk * BLK, BLK), BLK), cs], dst_ref=oin.at[pl.ds(mb * BLK, BLK), cs],
            send_sem=sent.at[1], recv_sem=or_.at[mb * half], device_id=partner, device_id_type=MESH)

    def shared_keys():
        r = jnp.concatenate([kvlat0[0:OWN, KV_LAT:], kvlat0[chip_rows(c), KV_LAT:]], axis=0).T
        for mb in range(2):
            kropeT[mb, 0, :ROPE] = r[mb * ROPE:(mb + 1) * ROPE]
            kropeT[mb, 1, ROPE:] = r[mb * ROPE:(mb + 1) * ROPE]

    def heads(mb, kv_up_first, then={}):
        scores = []
        if mb == 1:
            kv_up_first()
        for h in range(HEADS):
            kcat = jnp.concatenate([kT[mb, h], kropeT[mb, h % 2]], axis=0)
            scores.append(jnp.dot(qbuf[mb, h], kcat, preferred_element_type=F32))
        if mb == 0:
            kv_up_first()
        probs = []
        for h, s in enumerate(scores):
            s = jnp.concatenate([s[:, :OWN], jnp.minimum(s[:, OWN:], causal[...])], axis=1)
            m = jnp.max(s, axis=1, keepdims=True)
            e = jnp.exp2((s - m) * SCALE2)
            probs.append((e * (1.0 / jnp.sum(e, axis=1, keepdims=True))).astype(BF16))
            if h in then:
                then[h]()
        for h in range(HEADS):
            o = jnp.dot(probs[h], vb[mb, h], preferred_element_type=F32)
            oall[mb, :, h * 128:(h + 1) * 128] = o.astype(BF16)
            if mb == 1 and h == 7:
                o_copy(1, 0).start()
        for half in ((0, 1), (1,))[mb]:
            o_copy(mb, half).start()

    def take(ref, n, i):
        with jax.named_scope("take_wait"):
            @pl.when(k == 0)
            def _():
                wait_bytes(ref, n, fr.at[i])

    def pass_if(at, item, j):
        @pl.when(jnp.logical_and(k == 1, at))
        def _():
            pass_on(item, j)

    @pl.when(c > 0)
    def _():
        take(kvlat0, CHIP, 1)
        with jax.named_scope("take1"):
            kv_up_rows(0, chip_rows(c - 1))

    for n in (2, 3):
        @pl.when(c == n)
        def _():
            pass_if(True, 0, 2)
            take(kvlat0, (n - 1) * CHIP, 2)
            with jax.named_scope("take1"):
                kv_up_rows(0, pl.ds(0, (n - 1) * CHIP))
    shared_keys()
    @pl.when(c == 3)
    def _():
        pass_if(True, 1, 1)
        take(kvlat1, CHIP, 3)

    def third_rows():
        kv_up_rows(1, pl.ds(2 * CHIP, CHIP))

    late = jnp.logical_and(k == 1, c == 3)

    @pl.when(late)
    def _():
        with jax.named_scope("heads1"):
            heads(0, third_rows, {3: lambda: pass_on(1, 3), 8: lambda: pass_on(1, 2)})

    @pl.when(jnp.logical_not(late))
    def _():
        with jax.named_scope("heads1"):
            heads(0, third_rows)

    @pl.when(c == 1)
    def _():
        pass_if(True, 1, 1)
        take(kvlat1, CHIP, 3)

    @pl.when(c == 2)
    def _():
        for j in (1, 2):
            pass_if(True, 1, j)
        for i in (3, 4):
            take(kvlat1, CHIP, i)

    @pl.when(c == 3)
    def _():
        take(kvlat1, 2 * CHIP, 4)

    with jax.named_scope("heads2"):
        heads(1, lambda: kv_up_rows(1, pl.ds(0, 2 * CHIP)))

    with jax.named_scope("out"):
        wait_whole(wo_v, 0)
        orow = pl.ds(pl.multiple_of(k * BLK, BLK), BLK)
        mine = jnp.concatenate([oall[0, orow], oall[1, orow]], axis=0)

        @pl.when(k == 0)
        def _():
            wait_bytes(oin, 96, or_.at[0])
            wait_bytes(oin, 32, or_.at[1])
            y[...] = jnp.dot(jnp.concatenate([mine, oin[...]], axis=1), wo_v[...], preferred_element_type=F32).astype(BF16)

        @pl.when(k == 1)
        def _():
            acc[...] = jnp.dot(mine, wo_v[0:2048], preferred_element_type=F32)
            wait_bytes(oin, 96, or_.at[0])
            acc[...] += jnp.dot(oin[:, :1024], wo_v[2048:3072], preferred_element_type=F32)
            wait_bytes(oin, 32, or_.at[1])
            y[...] = (acc[...] + jnp.dot(oin[:, 1024:], wo_v[3072:], preferred_element_type=F32)).astype(BF16)

    for n in range(NCHIP):
        @pl.when(c == n)
        def _():
            wait_bytes(wqd_v, 192 * (NCHIP - 1 - n) + 192 + 384, sent.at[0])

            if n > 0:
                @pl.when(k == 1)
                def _():
                    wait_bytes(wqd_v, 384 * n, sent.at[0])
    wait_bytes(oin, CHIP, sent.at[1])


def store_body(y, y1, y2, sem):
    for i, out in enumerate((y1, y2)):
        pltpu.make_async_copy(y.at[pl.ds(i * BLK, BLK)], out, sem.at[i]).start()
    for i, out in enumerate((y1, y2)):
        pltpu.make_async_copy(y.at[pl.ds(i * BLK, BLK)], out, sem.at[i]).wait()


def store(y):
    any_spec = pl.BlockSpec(memory_space=pl.ANY)
    return pl.pallas_call(
        store_body,
        out_shape=(jax.ShapeDtypeStruct((BLK, D_MODEL), BF16),) * 2,
        in_specs=[any_spec],
        out_specs=(any_spec,) * 2,
        scratch_shapes=[pltpu.SemaphoreType.DMA((2,))],
        compiler_params=pltpu.CompilerParams(vmem_limit_bytes=2**20),
    )(y)


def solution(mesh):
    tok_spec = P(('dp', 'sp'), None)
    idx_spec = P(('dp', 'sp'))
    any_spec = pl.BlockSpec(memory_space=pl.ANY)
    vmem_spec = pl.BlockSpec(memory_space=pltpu.VMEM)

    def local_body(x_one, seg_one, pos_one, x_two, seg_two, pos_two, w_qdown, gain_q, w_qup, w_kvdown, gain_kv, w_kvup, w_out):
        dma = pltpu.SemaphoreType.DMA
        call = pl.pallas_call(
            body,
            out_shape=jax.ShapeDtypeStruct((CHIP, D_MODEL), BF16),
            in_specs=[pl.BlockSpec(memory_space=pltpu.HBM)] * 11,
            out_specs=vmem_spec,
            scratch_shapes=[
                pltpu.VMEM((CHIP, D_MODEL), BF16),
                pltpu.VMEM((2, 1, BLK), jnp.int32),
                pltpu.VMEM((D_MODEL, Q_LAT), BF16),
                pltpu.VMEM((Q_LAT,), BF16),
                pltpu.VMEM((Q_LAT, 3072), BF16),
                pltpu.VMEM((KV_LAT + ROPE, D_MODEL), BF16),
                pltpu.VMEM((KV_LAT,), BF16),
                pltpu.VMEM((KV_LAT, 4096), BF16),
                pltpu.VMEM((4096, D_MODEL), BF16),
                pltpu.VMEM((TOK, KV_LAT + 128), BF16),
                pltpu.VMEM((TOK, KV_LAT), BF16),
                pltpu.VMEM((2 * CHIP, Q_LAT), BF16),
                pltpu.VMEM((3, 2 * CHIP, 128), F32),
                pltpu.VMEM((2, HEADS, CHIP, 256), BF16),
                pltpu.VMEM((HEADS, CHIP, 128), BF16),
                pltpu.VMEM((2, HEADS, 128, TOK), BF16),
                pltpu.VMEM((2, HEADS, TOK, 128), BF16),
                pltpu.VMEM((2, 2, 128, TOK), BF16),
                pltpu.VMEM((2 * CHIP, 128), F32),
                pltpu.VMEM((2 * CHIP, 128), F32),
                pltpu.VMEM((CHIP, CHIP), F32),
                pltpu.VMEM((2, CHIP, 2048), BF16),
                pltpu.VMEM((CHIP, 2048), BF16),
                pltpu.VMEM((CHIP, D_MODEL), F32),
                pltpu.VMEM((CHIP, KV_LAT + ROPE), F32),
                dma((8,)), dma((2,)), dma((2, 3)), dma((5,)), dma((1,)), dma((2,)),
            ],
            compiler_params=pltpu.CompilerParams(collective_id=0, has_side_effects=True, vmem_limit_bytes=52 * 2**20),
        )
        args = (x_one, pos_one.reshape(1, BLK), x_two, pos_two.reshape(1, BLK), w_qdown, gain_q, w_qup,
                w_kvdown.T, gain_kv, w_kvup, w_out)
        y = call(*(pltpu.with_memory_space_constraint(a, pltpu.HBM) for a in args))
        return store(y)

    return jax.shard_map(local_body, mesh=mesh,
                         in_specs=(tok_spec, idx_spec, idx_spec, tok_spec, idx_spec, idx_spec, P(), P(), P(), P(), P(), P(), P()),
                         out_specs=(tok_spec, tok_spec), check_vma=False)
```

```python
import jax
import jax.numpy as jnp
from jax import lax
from jax.experimental import pallas as pl
from jax.experimental.pallas import tpu as pltpu
from jax.sharding import PartitionSpec as P

MESH = pl.DeviceIdType.MESH
F32 = jnp.float32
BF16 = jnp.bfloat16

D_MODEL = 1792
Q_LAT = 384
KV_LAT = 512
ROPE = 64
NOPE = 128
HEADS = 16
BLK = 64
CHIP = 2 * BLK
TOK = 512
NCHIP = 4
LN_BASE = 9.210340371976184
EPS = 1e-6
K_A = 768
SCALE2 = 192 ** -0.5 * 1.4426950408889634
NEG = -1e30
BIG = 3.0e38
OFF = -1.5e38
OWN = 3 * CHIP


def norm_rows(z, gain):
    ms = jnp.mean(z * z, axis=-1, keepdims=True)
    return (z * lax.rsqrt(ms + EPS) * gain.astype(F32)[None, :]).astype(BF16)


def body(x1, p1, x2, p2, wqd, gq, wqu, wkvd, gkv, wkvu, wo, y,
         xv, posv, wqd_v, gq_v, wqu_v, wkvd_v, gkv_v, wkvu_v, wo_v,
         kvlat0, kvlat1, qlat, tabs, qbuf, kheld, kT, vb, kropeT, start, flags, causal, oall, oin, acc, usum,
         lsem, sent, dr, fr, qr, or_):
    kvlat = (kvlat0, kvlat1)
    sp = lax.axis_index("sp")
    dp = lax.axis_index("dp")
    k = lax.rem(sp, 2)
    c = lax.div(sp, 2)
    pk = 1 - k

    def dev(chip, core):
        return (dp, chip * 2 + core)

    partner = dev(c, pk)

    def local(src, dst, i):
        cp = pltpu.make_async_copy(src, dst, lsem.at[i])
        cp.start()
        return cp

    local(p1, posv.at[0], 0)
    local(p2, posv.at[1], 0)
    local(x1, xv.at[pl.ds(0, BLK)], 1)
    local(x2, xv.at[pl.ds(BLK, BLK)], 1)
    l_wkvd = [local(wkvd.at[:, pl.ds(a, n)], wkvd_v.at[:, pl.ds(a, n)], i) for a, n, i in ((0, K_A, 2), (K_A, D_MODEL - K_A, 3))]
    l_gkv = local(gkv, gkv_v, 6)
    l_gq = local(gq, gq_v, 7)
    l_wqd = local(wqd, wqd_v, 4)
    l_wkvu = local(wkvu.at[:, pl.ds(pl.multiple_of(k * 4096, 4096), 4096)], wkvu_v, 5)

    def wait_whole(ref, i):
        pltpu.make_async_copy(ref, ref, lsem.at[i]).wait()

    def wait_bytes(ref, n, sem):
        p = ref.at[pl.ds(0, n)]
        pltpu.make_async_copy(p, p, sem).wait()

    barrier = pltpu.get_barrier_semaphore()
    pl.semaphore_signal(barrier, inc=1, device_id=partner, device_id_type=MESH)
    for j in range(1, NCHIP):
        for core in range(2):
            pl.semaphore_signal(barrier, inc=1, device_id=dev(lax.rem(c + j, NCHIP), core), device_id_type=MESH)

    for b in range(NCHIP - 1):
        @pl.when(c <= b)
        def _():
            def zero(h, _):
                kT[0, h, :, pl.ds(b * CHIP, CHIP)] = jnp.zeros((128, CHIP), BF16)
                vb[0, h, pl.ds(b * CHIP, CHIP)] = jnp.zeros((CHIP, 128), BF16)
                return 0
            lax.fori_loop(0, HEADS, zero, 0)

        @pl.when(c < b)
        def _():
            kvlat0[pl.ds(b * CHIP, CHIP), KV_LAT:] = jnp.zeros((CHIP, 128), BF16)
            kvlat1[pl.ds(b * CHIP, CHIP)] = jnp.zeros((CHIP, KV_LAT), BF16)

    tri = lax.broadcasted_iota(jnp.int32, (CHIP, CHIP), 1) <= lax.broadcasted_iota(jnp.int32, (CHIP, CHIP), 0)
    causal[...] = jnp.where(tri, BIG, NEG)

    lane = lax.broadcasted_iota(jnp.int32, (1, 128), 1)
    lo64 = lane < 64
    lane64 = lax.rem(lane, 64)
    lo32 = lax.rem(lane, 64) < 32

    wait_whole(posv, 0)
    own = pl.ds(pl.multiple_of(k * CHIP, CHIP), CHIP)
    eye = lax.broadcasted_iota(jnp.int32, (BLK, BLK), 0) == lax.broadcasted_iota(jnp.int32, (BLK, BLK), 1)
    cols = [jnp.sum(jnp.where(eye, posv[mb].astype(F32), 0.0), axis=1, keepdims=True) for mb in range(2)]
    pos_col = jnp.concatenate(cols, axis=0)
    freq = jnp.exp(lax.rem(lane, 32).astype(F32) * (-LN_BASE / 32))
    ang = pos_col * freq
    cos_t = jnp.cos(ang)
    sin_t = jnp.sin(ang)
    sin_t = jnp.where(lo32, -sin_t, sin_t)
    tabs[0, own] = cos_t
    tabs[1, own] = sin_t
    tabs[2, own] = pos_col + jnp.zeros((CHIP, 128), F32)

    def rot(z, cs, sn):
        sw = jnp.where(lo32, pltpu.roll(z, 96, 1), pltpu.roll(z, 32, 1))
        return z * cs + sw * sn

    def kv_down(a, n):
        return lax.dot_general(xv[:, a:a + n], wkvd_v[:, a:a + n], (((1,), (1,)), ((), ())), preferred_element_type=F32)

    with jax.named_scope("wait_x"):
        wait_whole(xv, 1)
        l_wkvd[0].wait()
    l_wqu = local(wqu.at[:, pl.ds(pl.multiple_of(k * 3072, 1024), 3072)], wqu_v, 1)
    usum[...] = kv_down(0, K_A)
    with jax.named_scope("wait_wd"):
        l_wkvd[1].wait()
        l_gkv.wait()
    u = usum[...] + kv_down(K_A, D_MODEL - K_A)
    ur = u[:, KV_LAT:]
    kr = rot(jnp.concatenate([ur, ur], axis=1), cos_t, sin_t)
    kr = jnp.where(lo64, kr[:BLK], kr[BLK:]).astype(BF16)

    ckv = norm_rows(u[:, :KV_LAT], gkv_v[...])

    def rows(chip, core):
        return pl.ds(pl.multiple_of(chip * CHIP + core * BLK, BLK), BLK)

    def chip_rows(chip):
        return pl.ds(pl.multiple_of(chip * CHIP, CHIP), CHIP)

    def part(item, chip, core):
        return kvlat[item].at[rows(chip, core)]

    kvlat[0][rows(c, k), KV_LAT:] = kr
    kvlat[0][rows(c, k), :KV_LAT] = ckv[:BLK]
    kvlat[1][rows(c, k)] = ckv[BLK:]

    with jax.named_scope("barrier"):
        pl.semaphore_wait(barrier, 7)

    def direct(item, j):
        p = part(item, c, k)
        return pltpu.make_async_remote_copy(src_ref=p, dst_ref=p, send_sem=sent.at[0], recv_sem=dr.at[item, j - 1],
                                            device_id=dev(c + j, 1), device_id_type=MESH)

    def direct_recv(item, j):
        p = kvlat[item].at[chip_rows(c - j)]
        return pltpu.make_async_remote_copy(src_ref=p, dst_ref=p, send_sem=sent.at[0], recv_sem=dr.at[item, j - 1],
                                            device_id=partner, device_id_type=MESH)

    def share(item, core):
        p = part(item, c, core)
        return pltpu.make_async_remote_copy(src_ref=p, dst_ref=p, send_sem=sent.at[0], recv_sem=fr.at[0],
                                            device_id=partner, device_id_type=MESH)

    def forward(item, j):
        p = kvlat[item].at[chip_rows(c - j)]
        return pltpu.make_async_remote_copy(src_ref=p, dst_ref=p, send_sem=sent.at[0], recv_sem=fr.at[2 * item + (1 if j == 1 else 2)],
                                            device_id=partner, device_id_type=MESH)

    def send(item, pairs):
        for chip, j in pairs:
            @pl.when(c == chip)
            def _():
                direct(item, j).start()

    send(0, ((0, 3), (0, 2), (0, 1), (1, 2), (1, 1), (2, 1)))
    for item in range(2):
        share(item, k).start()

    l_gq.wait()
    l_wqd.wait()
    with jax.named_scope("q_down"):
        cq = jnp.dot(xv[...], wqd_v[...], preferred_element_type=F32)
        qlat[own] = norm_rows(cq, gq_v[...])

    def q_copy(i, core):
        r = pl.ds(pl.multiple_of(core * CHIP, CHIP), CHIP)
        p = qlat.at[r] if i == 0 else tabs.at[:, r]
        return pltpu.make_async_remote_copy(src_ref=p, dst_ref=p, send_sem=sent.at[0], recv_sem=qr.at[0],
                                            device_id=partner, device_id_type=MESH)

    for i in range(2):
        q_copy(i, k).start()

    def turned(h, key):
        t = key.T
        return jnp.concatenate([t[64:], t[:64]], axis=0) if h % 2 else t

    def kv_up(lhs, store, turn=True):
        for i in range(4):
            kv = jnp.dot(lhs, wkvu_v[:, i * 1024:(i + 1) * 1024], preferred_element_type=F32).astype(BF16)
            for n in range(4):
                key = kv[:, n * 256:n * 256 + NOPE]
                store(i * 4 + n, turned(i * 4 + n, key) if turn else key, kv[:, n * 256 + NOPE:(n + 1) * 256])

    def kv_up_own():
        r = chip_rows(c)

        def store(h, key, val):
            for mb in range(2):
                kT[mb, h, :, OWN:] = key[:, mb * CHIP:(mb + 1) * CHIP]
                vb[mb, h, OWN:] = val[mb * CHIP:(mb + 1) * CHIP]
        kv_up(jnp.concatenate([kvlat0[r, :KV_LAT], kvlat1[r]], axis=0), store)

    def kv_up_device(core, store_key):
        r = rows(c, core)

        def store(h, key, val):
            store_key(h, key)
            for mb in range(2):
                vb[mb, h, pl.ds(pl.multiple_of(OWN + core * BLK, BLK), BLK)] = val[mb * BLK:(mb + 1) * BLK]
        kv_up(jnp.concatenate([kvlat0[r, :KV_LAT], kvlat1[r]], axis=0), store, False)

    def hold_key(h, key):
        kheld[h] = key

    def join_key(h, key):
        for mb in range(2):
            s = slice(mb * BLK, (mb + 1) * BLK)
            kT[mb, h, :, OWN:] = turned(h, jnp.concatenate([key[s], kheld[h, s]], axis=0))

    def kv_up_rows(mb, r):
        def store(h, key, val):
            kT[mb, h, :, r] = key
            vb[mb, h, r] = val
        kv_up(kvlat[mb][r, :KV_LAT], store)

    send(1, ((2, 1),))
    with jax.named_scope("wait_wkvu"):
        l_wkvu.wait()
    for i, core in enumerate((k, pk)):
        local(wo.at[pl.ds(pl.multiple_of(core * 2048, 2048), 2048)], wo_v.at[pl.ds(i * 2048, 2048)], 0)
    def wait_share():
        with jax.named_scope("wait_partner"):
            wait_bytes(wqd_v, 192, fr.at[0])

    def q_up(i):
        return jnp.dot(qlat[...], wqu_v[:, i * 768:(i + 1) * 768], preferred_element_type=F32)

    def q_store(i, f):
        for pair in range(2):
            t0, t1, t2 = (f[:, pair * 384 + n * 128: pair * 384 + (n + 1) * 128] for n in range(3))
            n1 = jnp.where(lo64, t2, t1)
            r = rot(jnp.where(lo64, t1, t2), tabs[0], tabs[1])
            q = ((t0.astype(BF16), jnp.where(lo64, r, flags[...]).astype(BF16)),
                 (n1.astype(BF16), jnp.where(lo64, flags[...], r).astype(BF16)))
            for odd in range(2):
                h = i * 4 + pair * 2 + odd
                for mb in range(2):
                    for core in range(2):
                        s = slice(core * CHIP + mb * BLK, core * CHIP + (mb + 1) * BLK)
                        for n in range(2):
                            qbuf[mb, h, pl.ds(core * BLK, BLK), n * 128:(n + 1) * 128] = q[odd][n][s]

    def queries():
        wait_bytes(wqd_v, 384, qr.at[0])
        row = lax.broadcasted_iota(jnp.int32, (2 * CHIP, 1), 0)
        index = c * CHIP + lax.div(row, CHIP) * BLK + lax.rem(row, BLK)
        start[...] = index.astype(F32) - tabs[2]
        flags[...] = jnp.where(lane64 == 0, (start[...] > 0.5).astype(F32), (lane64 == 1).astype(F32))
        col = lax.broadcasted_iota(jnp.int32, (ROPE, TOK), 1)
        kind = lax.broadcasted_iota(jnp.int32, (ROPE, TOK), 0)
        place = jnp.where(col < OWN, col, c * CHIP + col - OWN).astype(F32)
        empty = jnp.logical_and(col >= c * CHIP, col < OWN)
        for mb in range(2):
            firsts = [jnp.max(start[pl.ds(core * CHIP + mb * BLK, BLK)], axis=0, keepdims=True) for core in range(2)]
            first = jnp.maximum(firsts[0], firsts[1])
            before = place < jnp.concatenate([first] * 4, axis=1)
            off = jnp.logical_or(jnp.logical_and(kind == 0, before), jnp.logical_and(kind == 1, empty))
            masks = jnp.where(off, OFF, 0.0).astype(BF16)
            kropeT[mb, 0, ROPE:] = masks
            kropeT[mb, 1, :ROPE] = masks
        l_wqu.wait()
        prev = q_up(0)
        for i in range(4):
            nxt = q_up(i + 1) if i < 3 else None
            q_store(i, prev)
            prev = nxt

    with jax.named_scope("kv_own"):
        @pl.when(k == 0)
        def _():
            wait_share()
            kv_up_own()

        @pl.when(k == 1)
        def _():
            kv_up_device(k, hold_key)
            wait_share()
            kv_up_device(pk, join_key)

    with jax.named_scope("queries"):
        queries()

    def pass_on(item, j):
        direct_recv(item, j).wait_recv()
        forward(item, j).start()

    with jax.named_scope("pass_on"):
        for j, at in ((1, c > 0), (3, c == 3)):
            @pl.when(jnp.logical_and(k == 1, at))
            def _():
                pass_on(0, j)

    send(1, ((0, 3), (0, 2), (0, 1), (1, 2), (1, 1)))

    def o_copy(mb, half):
        cs = pl.ds(half * 1024, 1024)
        return pltpu.make_async_remote_copy(
            src_ref=oall.at[mb, pl.ds(pl.multiple_of(pk * BLK, BLK), BLK), cs], dst_ref=oin.at[pl.ds(mb * BLK, BLK), cs],
            send_sem=sent.at[1], recv_sem=or_.at[mb * half], device_id=partner, device_id_type=MESH)

    def shared_keys():
        r = jnp.concatenate([kvlat0[0:OWN, KV_LAT:], kvlat0[chip_rows(c), KV_LAT:]], axis=0).T
        for mb in range(2):
            kropeT[mb, 0, :ROPE] = r[mb * ROPE:(mb + 1) * ROPE]
            kropeT[mb, 1, ROPE:] = r[mb * ROPE:(mb + 1) * ROPE]

    def heads(mb, kv_up_first, then={}):
        scores = []
        if mb == 1:
            kv_up_first()
        for h in range(HEADS):
            kcat = jnp.concatenate([kT[mb, h], kropeT[mb, h % 2]], axis=0)
            scores.append(jnp.dot(qbuf[mb, h], kcat, preferred_element_type=F32))
        if mb == 0:
            kv_up_first()
        probs = []
        for h, s in enumerate(scores):
            s = jnp.concatenate([s[:, :OWN], jnp.minimum(s[:, OWN:], causal[...])], axis=1)
            m = jnp.max(s, axis=1, keepdims=True)
            e = jnp.exp2((s - m) * SCALE2)
            probs.append((e * (1.0 / jnp.sum(e, axis=1, keepdims=True))).astype(BF16))
            if h in then:
                then[h]()
        for h in range(HEADS):
            o = jnp.dot(probs[h], vb[mb, h], preferred_element_type=F32)
            oall[mb, :, h * 128:(h + 1) * 128] = o.astype(BF16)
            if mb == 1 and h == 7:
                o_copy(1, 0).start()
        for half in ((0, 1), (1,))[mb]:
            o_copy(mb, half).start()

    def take(ref, n, i):
        with jax.named_scope("take_wait"):
            @pl.when(k == 0)
            def _():
                wait_bytes(ref, n, fr.at[i])

    def pass_if(at, item, j):
        @pl.when(jnp.logical_and(k == 1, at))
        def _():
            pass_on(item, j)

    @pl.when(c > 0)
    def _():
        take(kvlat0, CHIP, 1)
        with jax.named_scope("take1"):
            kv_up_rows(0, chip_rows(c - 1))

    for n in (2, 3):
        @pl.when(c == n)
        def _():
            pass_if(True, 0, 2)
            take(kvlat0, (n - 1) * CHIP, 2)
            with jax.named_scope("take1"):
                kv_up_rows(0, pl.ds(0, (n - 1) * CHIP))
    shared_keys()
    @pl.when(c == 3)
    def _():
        pass_if(True, 1, 1)
        take(kvlat1, CHIP, 3)

    def third_rows():
        kv_up_rows(1, pl.ds(2 * CHIP, CHIP))

    late = jnp.logical_and(k == 1, c == 3)

    @pl.when(late)
    def _():
        with jax.named_scope("heads1"):
            heads(0, third_rows, {5: lambda: pass_on(1, 3), 9: lambda: pass_on(1, 2)})

    @pl.when(jnp.logical_not(late))
    def _():
        with jax.named_scope("heads1"):
            heads(0, third_rows)

    @pl.when(c == 1)
    def _():
        pass_if(True, 1, 1)
        take(kvlat1, CHIP, 3)

    @pl.when(c == 2)
    def _():
        for j in (1, 2):
            pass_if(True, 1, j)
        for i in (3, 4):
            take(kvlat1, CHIP, i)

    @pl.when(c == 3)
    def _():
        take(kvlat1, 2 * CHIP, 4)

    with jax.named_scope("heads2"):
        heads(1, lambda: kv_up_rows(1, pl.ds(0, 2 * CHIP)))

    with jax.named_scope("out"):
        wait_whole(wo_v, 0)
        orow = pl.ds(pl.multiple_of(k * BLK, BLK), BLK)
        mine = jnp.concatenate([oall[0, orow], oall[1, orow]], axis=0)

        @pl.when(k == 0)
        def _():
            wait_bytes(oin, 96, or_.at[0])
            wait_bytes(oin, 32, or_.at[1])
            y[...] = jnp.dot(jnp.concatenate([mine, oin[...]], axis=1), wo_v[...], preferred_element_type=F32).astype(BF16)

        @pl.when(k == 1)
        def _():
            acc[...] = jnp.dot(mine, wo_v[0:2048], preferred_element_type=F32)
            wait_bytes(oin, 96, or_.at[0])
            acc[...] += jnp.dot(oin[:, :1024], wo_v[2048:3072], preferred_element_type=F32)
            wait_bytes(oin, 32, or_.at[1])
            y[...] = (acc[...] + jnp.dot(oin[:, 1024:], wo_v[3072:], preferred_element_type=F32)).astype(BF16)

    for n in range(NCHIP):
        @pl.when(c == n)
        def _():
            wait_bytes(wqd_v, 192 * (NCHIP - 1 - n) + 192 + 384, sent.at[0])

            if n > 0:
                @pl.when(k == 1)
                def _():
                    wait_bytes(wqd_v, 384 * n, sent.at[0])
    wait_bytes(oin, CHIP, sent.at[1])


def store_body(y, y1, y2, sem):
    for i, out in enumerate((y1, y2)):
        pltpu.make_async_copy(y.at[pl.ds(i * BLK, BLK)], out, sem.at[i]).start()
    for i, out in enumerate((y1, y2)):
        pltpu.make_async_copy(y.at[pl.ds(i * BLK, BLK)], out, sem.at[i]).wait()


def store(y):
    any_spec = pl.BlockSpec(memory_space=pl.ANY)
    return pl.pallas_call(
        store_body,
        out_shape=(jax.ShapeDtypeStruct((BLK, D_MODEL), BF16),) * 2,
        in_specs=[any_spec],
        out_specs=(any_spec,) * 2,
        scratch_shapes=[pltpu.SemaphoreType.DMA((2,))],
        compiler_params=pltpu.CompilerParams(vmem_limit_bytes=2**20),
    )(y)


def solution(mesh):
    tok_spec = P(('dp', 'sp'), None)
    idx_spec = P(('dp', 'sp'))
    any_spec = pl.BlockSpec(memory_space=pl.ANY)
    vmem_spec = pl.BlockSpec(memory_space=pltpu.VMEM)

    def local_body(x_one, seg_one, pos_one, x_two, seg_two, pos_two, w_qdown, gain_q, w_qup, w_kvdown, gain_kv, w_kvup, w_out):
        dma = pltpu.SemaphoreType.DMA
        call = pl.pallas_call(
            body,
            out_shape=jax.ShapeDtypeStruct((CHIP, D_MODEL), BF16),
            in_specs=[pl.BlockSpec(memory_space=pltpu.HBM)] * 11,
            out_specs=vmem_spec,
            scratch_shapes=[
                pltpu.VMEM((CHIP, D_MODEL), BF16),
                pltpu.VMEM((2, 1, BLK), jnp.int32),
                pltpu.VMEM((D_MODEL, Q_LAT), BF16),
                pltpu.VMEM((Q_LAT,), BF16),
                pltpu.VMEM((Q_LAT, 3072), BF16),
                pltpu.VMEM((KV_LAT + ROPE, D_MODEL), BF16),
                pltpu.VMEM((KV_LAT,), BF16),
                pltpu.VMEM((KV_LAT, 4096), BF16),
                pltpu.VMEM((4096, D_MODEL), BF16),
                pltpu.VMEM((TOK, KV_LAT + 128), BF16),
                pltpu.VMEM((TOK, KV_LAT), BF16),
                pltpu.VMEM((2 * CHIP, Q_LAT), BF16),
                pltpu.VMEM((3, 2 * CHIP, 128), F32),
                pltpu.VMEM((2, HEADS, CHIP, 256), BF16),
                pltpu.VMEM((HEADS, CHIP, 128), BF16),
                pltpu.VMEM((2, HEADS, 128, TOK), BF16),
                pltpu.VMEM((2, HEADS, TOK, 128), BF16),
                pltpu.VMEM((2, 2, 128, TOK), BF16),
                pltpu.VMEM((2 * CHIP, 128), F32),
                pltpu.VMEM((2 * CHIP, 128), F32),
                pltpu.VMEM((CHIP, CHIP), F32),
                pltpu.VMEM((2, CHIP, 2048), BF16),
                pltpu.VMEM((CHIP, 2048), BF16),
                pltpu.VMEM((CHIP, D_MODEL), F32),
                pltpu.VMEM((CHIP, KV_LAT + ROPE), F32),
                dma((8,)), dma((2,)), dma((2, 3)), dma((5,)), dma((1,)), dma((2,)),
            ],
            compiler_params=pltpu.CompilerParams(collective_id=0, has_side_effects=True, vmem_limit_bytes=52 * 2**20),
        )
        args = (x_one, pos_one.reshape(1, BLK), x_two, pos_two.reshape(1, BLK), w_qdown, gain_q, w_qup,
                w_kvdown.T, gain_kv, w_kvup, w_out)
        y = call(*(pltpu.with_memory_space_constraint(a, pltpu.HBM) for a in args))
        return store(y)

    return jax.shard_map(local_body, mesh=mesh,
                         in_specs=(tok_spec, idx_spec, idx_spec, tok_spec, idx_spec, idx_spec, P(), P(), P(), P(), P(), P(), P()),
                         out_specs=(tok_spec, tok_spec), check_vma=False)
```

```python
import jax
import jax.numpy as jnp
from jax import lax
from jax.experimental import pallas as pl
from jax.experimental.pallas import tpu as pltpu
from jax.sharding import PartitionSpec as P

MESH = pl.DeviceIdType.MESH
F32 = jnp.float32
BF16 = jnp.bfloat16

D_MODEL = 1792
Q_LAT = 384
KV_LAT = 512
ROPE = 64
NOPE = 128
HEADS = 16
BLK = 64
CHIP = 2 * BLK
TOK = 512
NCHIP = 4
LN_BASE = 9.210340371976184
EPS = 1e-6
K_A = 768
SCALE2 = 192 ** -0.5 * 1.4426950408889634
NEG = -1e30
BIG = 3.0e38
OFF = -1.5e38
OWN = 3 * CHIP


def norm_rows(z, gain):
    ms = jnp.mean(z * z, axis=-1, keepdims=True)
    return (z * lax.rsqrt(ms + EPS) * gain.astype(F32)[None, :]).astype(BF16)


def body(x1, p1, x2, p2, wqd, gq, wqu, wkvd, gkv, wkvu, wo, y,
         xv, posv, wqd_v, gq_v, wqu_v, wkvd_v, gkv_v, wkvu_v, wo_v,
         kvlat0, kvlat1, qlat, tabs, qbuf, kheld, kT, vb, kropeT, start, flags, causal, oall, oin, acc, usum,
         lsem, sent, dr, fr, qr, or_):
    kvlat = (kvlat0, kvlat1)
    sp = lax.axis_index("sp")
    dp = lax.axis_index("dp")
    k = lax.rem(sp, 2)
    c = lax.div(sp, 2)
    pk = 1 - k

    def dev(chip, core):
        return (dp, chip * 2 + core)

    partner = dev(c, pk)

    def local(src, dst, i):
        cp = pltpu.make_async_copy(src, dst, lsem.at[i])
        cp.start()
        return cp

    local(p1, posv.at[0], 0)
    local(p2, posv.at[1], 0)
    local(x1, xv.at[pl.ds(0, BLK)], 1)
    local(x2, xv.at[pl.ds(BLK, BLK)], 1)
    l_wkvd = [local(wkvd.at[:, pl.ds(a, n)], wkvd_v.at[:, pl.ds(a, n)], i) for a, n, i in ((0, K_A, 2), (K_A, D_MODEL - K_A, 3))]
    l_gkv = local(gkv, gkv_v, 6)
    l_gq = local(gq, gq_v, 7)
    l_wqd = local(wqd, wqd_v, 4)
    l_wkvu = local(wkvu.at[:, pl.ds(pl.multiple_of(k * 4096, 4096), 4096)], wkvu_v, 5)

    def wait_whole(ref, i):
        pltpu.make_async_copy(ref, ref, lsem.at[i]).wait()

    def wait_bytes(ref, n, sem):
        p = ref.at[pl.ds(0, n)]
        pltpu.make_async_copy(p, p, sem).wait()

    barrier = pltpu.get_barrier_semaphore()
    pl.semaphore_signal(barrier, inc=1, device_id=partner, device_id_type=MESH)
    for j in range(1, NCHIP):
        for core in range(2):
            pl.semaphore_signal(barrier, inc=1, device_id=dev(lax.rem(c + j, NCHIP), core), device_id_type=MESH)

    for b in range(NCHIP - 1):
        @pl.when(c <= b)
        def _():
            def zero(h, _):
                kT[0, h, :, pl.ds(b * CHIP, CHIP)] = jnp.zeros((128, CHIP), BF16)
                vb[0, h, pl.ds(b * CHIP, CHIP)] = jnp.zeros((CHIP, 128), BF16)
                return 0
            lax.fori_loop(0, HEADS, zero, 0)

        @pl.when(c < b)
        def _():
            kvlat0[pl.ds(b * CHIP, CHIP), KV_LAT:] = jnp.zeros((CHIP, 128), BF16)
            kvlat1[pl.ds(b * CHIP, CHIP)] = jnp.zeros((CHIP, KV_LAT), BF16)

    tri = lax.broadcasted_iota(jnp.int32, (CHIP, CHIP), 1) <= lax.broadcasted_iota(jnp.int32, (CHIP, CHIP), 0)
    causal[...] = jnp.where(tri, BIG, NEG)

    lane = lax.broadcasted_iota(jnp.int32, (1, 128), 1)
    lo64 = lane < 64
    lane64 = lax.rem(lane, 64)
    lo32 = lax.rem(lane, 64) < 32

    wait_whole(posv, 0)
    own = pl.ds(pl.multiple_of(k * CHIP, CHIP), CHIP)
    eye = lax.broadcasted_iota(jnp.int32, (BLK, BLK), 0) == lax.broadcasted_iota(jnp.int32, (BLK, BLK), 1)
    cols = [jnp.sum(jnp.where(eye, posv[mb].astype(F32), 0.0), axis=1, keepdims=True) for mb in range(2)]
    pos_col = jnp.concatenate(cols, axis=0)
    freq = jnp.exp(lax.rem(lane, 32).astype(F32) * (-LN_BASE / 32))
    ang = pos_col * freq
    cos_t = jnp.cos(ang)
    sin_t = jnp.sin(ang)
    sin_t = jnp.where(lo32, -sin_t, sin_t)
    tabs[0, own] = cos_t
    tabs[1, own] = sin_t
    tabs[2, own] = pos_col + jnp.zeros((CHIP, 128), F32)

    def rot(z, cs, sn):
        sw = jnp.where(lo32, pltpu.roll(z, 96, 1), pltpu.roll(z, 32, 1))
        return z * cs + sw * sn

    def kv_down(a, n):
        return lax.dot_general(xv[:, a:a + n], wkvd_v[:, a:a + n], (((1,), (1,)), ((), ())), preferred_element_type=F32)

    with jax.named_scope("wait_x"):
        wait_whole(xv, 1)
        l_wkvd[0].wait()
    l_wqu = local(wqu.at[:, pl.ds(pl.multiple_of(k * 3072, 1024), 3072)], wqu_v, 1)
    usum[...] = kv_down(0, K_A)
    with jax.named_scope("wait_wd"):
        l_wkvd[1].wait()
        l_gkv.wait()
    u = usum[...] + kv_down(K_A, D_MODEL - K_A)
    ur = u[:, KV_LAT:]
    kr = rot(jnp.concatenate([ur, ur], axis=1), cos_t, sin_t)
    kr = jnp.where(lo64, kr[:BLK], kr[BLK:]).astype(BF16)

    ckv = norm_rows(u[:, :KV_LAT], gkv_v[...])

    def rows(chip, core):
        return pl.ds(pl.multiple_of(chip * CHIP + core * BLK, BLK), BLK)

    def chip_rows(chip):
        return pl.ds(pl.multiple_of(chip * CHIP, CHIP), CHIP)

    def part(item, chip, core):
        return kvlat[item].at[rows(chip, core)]

    kvlat[0][rows(c, k), KV_LAT:] = kr
    kvlat[0][rows(c, k), :KV_LAT] = ckv[:BLK]
    kvlat[1][rows(c, k)] = ckv[BLK:]

    with jax.named_scope("barrier"):
        pl.semaphore_wait(barrier, 7)

    def direct(item, j):
        p = part(item, c, k)
        return pltpu.make_async_remote_copy(src_ref=p, dst_ref=p, send_sem=sent.at[0], recv_sem=dr.at[item, j - 1],
                                            device_id=dev(c + j, 1), device_id_type=MESH)

    def direct_recv(item, j):
        p = kvlat[item].at[chip_rows(c - j)]
        return pltpu.make_async_remote_copy(src_ref=p, dst_ref=p, send_sem=sent.at[0], recv_sem=dr.at[item, j - 1],
                                            device_id=partner, device_id_type=MESH)

    def share(item, core):
        p = part(item, c, core)
        return pltpu.make_async_remote_copy(src_ref=p, dst_ref=p, send_sem=sent.at[0], recv_sem=fr.at[0],
                                            device_id=partner, device_id_type=MESH)

    def forward(item, j):
        p = kvlat[item].at[chip_rows(c - j)]
        return pltpu.make_async_remote_copy(src_ref=p, dst_ref=p, send_sem=sent.at[0], recv_sem=fr.at[2 * item + (1 if j == 1 else 2)],
                                            device_id=partner, device_id_type=MESH)

    def send(item, pairs):
        for chip, j in pairs:
            @pl.when(c == chip)
            def _():
                direct(item, j).start()

    send(0, ((0, 3), (0, 2), (0, 1), (1, 2), (1, 1), (2, 1)))
    for item in range(2):
        share(item, k).start()

    l_gq.wait()
    l_wqd.wait()
    with jax.named_scope("q_down"):
        cq = jnp.dot(xv[...], wqd_v[...], preferred_element_type=F32)
        qlat[own] = norm_rows(cq, gq_v[...])

    def q_copy(i, core):
        r = pl.ds(pl.multiple_of(core * CHIP, CHIP), CHIP)
        p = qlat.at[r] if i == 0 else tabs.at[:, r]
        return pltpu.make_async_remote_copy(src_ref=p, dst_ref=p, send_sem=sent.at[0], recv_sem=qr.at[0],
                                            device_id=partner, device_id_type=MESH)

    for i in range(2):
        q_copy(i, k).start()

    def turned(h, key):
        t = key.T
        return jnp.concatenate([t[64:], t[:64]], axis=0) if h % 2 else t

    def kv_up(lhs, store, turn=True):
        for i in range(4):
            kv = jnp.dot(lhs, wkvu_v[:, i * 1024:(i + 1) * 1024], preferred_element_type=F32).astype(BF16)
            for n in range(4):
                key = kv[:, n * 256:n * 256 + NOPE]
                store(i * 4 + n, turned(i * 4 + n, key) if turn else key, kv[:, n * 256 + NOPE:(n + 1) * 256])

    def kv_up_own():
        r = chip_rows(c)

        def store(h, key, val):
            for mb in range(2):
                kT[mb, h, :, OWN:] = key[:, mb * CHIP:(mb + 1) * CHIP]
                vb[mb, h, OWN:] = val[mb * CHIP:(mb + 1) * CHIP]
        kv_up(jnp.concatenate([kvlat0[r, :KV_LAT], kvlat1[r]], axis=0), store)

    def kv_up_device(core, store_key):
        r = rows(c, core)

        def store(h, key, val):
            store_key(h, key)
            for mb in range(2):
                vb[mb, h, pl.ds(pl.multiple_of(OWN + core * BLK, BLK), BLK)] = val[mb * BLK:(mb + 1) * BLK]
        kv_up(jnp.concatenate([kvlat0[r, :KV_LAT], kvlat1[r]], axis=0), store, False)

    def hold_key(h, key):
        kheld[h] = key

    def join_key(h, key):
        for mb in range(2):
            s = slice(mb * BLK, (mb + 1) * BLK)
            kT[mb, h, :, OWN:] = turned(h, jnp.concatenate([key[s], kheld[h, s]], axis=0))

    def kv_up_rows(mb, r):
        def store(h, key, val):
            kT[mb, h, :, r] = key
            vb[mb, h, r] = val
        kv_up(kvlat[mb][r, :KV_LAT], store)

    send(1, ((2, 1),))
    with jax.named_scope("wait_wkvu"):
        l_wkvu.wait()
    for i, core in enumerate((k, pk)):
        local(wo.at[pl.ds(pl.multiple_of(core * 2048, 2048), 2048)], wo_v.at[pl.ds(i * 2048, 2048)], 0)
    def wait_share():
        with jax.named_scope("wait_partner"):
            wait_bytes(wqd_v, 192, fr.at[0])

    def q_up(i):
        return jnp.dot(qlat[...], wqu_v[:, i * 768:(i + 1) * 768], preferred_element_type=F32)

    def q_store(i, f):
        for pair in range(2):
            t0, t1, t2 = (f[:, pair * 384 + n * 128: pair * 384 + (n + 1) * 128] for n in range(3))
            n1 = jnp.where(lo64, t2, t1)
            r = rot(jnp.where(lo64, t1, t2), tabs[0], tabs[1])
            q = ((t0.astype(BF16), jnp.where(lo64, r, flags[...]).astype(BF16)),
                 (n1.astype(BF16), jnp.where(lo64, flags[...], r).astype(BF16)))
            for odd in range(2):
                h = i * 4 + pair * 2 + odd
                for mb in range(2):
                    for core in range(2):
                        s = slice(core * CHIP + mb * BLK, core * CHIP + (mb + 1) * BLK)
                        for n in range(2):
                            qbuf[mb, h, pl.ds(core * BLK, BLK), n * 128:(n + 1) * 128] = q[odd][n][s]

    def queries():
        wait_bytes(wqd_v, 384, qr.at[0])
        row = lax.broadcasted_iota(jnp.int32, (2 * CHIP, 1), 0)
        index = c * CHIP + lax.div(row, CHIP) * BLK + lax.rem(row, BLK)
        start[...] = index.astype(F32) - tabs[2]
        flags[...] = jnp.where(lane64 == 0, (start[...] > 0.5).astype(F32), (lane64 == 1).astype(F32))
        col = lax.broadcasted_iota(jnp.int32, (ROPE, TOK), 1)
        kind = lax.broadcasted_iota(jnp.int32, (ROPE, TOK), 0)
        place = jnp.where(col < OWN, col, c * CHIP + col - OWN).astype(F32)
        empty = jnp.logical_and(col >= c * CHIP, col < OWN)
        for mb in range(2):
            firsts = [jnp.max(start[pl.ds(core * CHIP + mb * BLK, BLK)], axis=0, keepdims=True) for core in range(2)]
            first = jnp.maximum(firsts[0], firsts[1])
            before = place < jnp.concatenate([first] * 4, axis=1)
            off = jnp.logical_or(jnp.logical_and(kind == 0, before), jnp.logical_and(kind == 1, empty))
            masks = jnp.where(off, OFF, 0.0).astype(BF16)
            kropeT[mb, 0, ROPE:] = masks
            kropeT[mb, 1, :ROPE] = masks
        l_wqu.wait()
        prev = q_up(0)
        for i in range(4):
            nxt = q_up(i + 1) if i < 3 else None
            q_store(i, prev)
            prev = nxt

    with jax.named_scope("kv_own"):
        @pl.when(k == 0)
        def _():
            wait_share()
            kv_up_own()

        @pl.when(k == 1)
        def _():
            kv_up_device(k, hold_key)
            wait_share()
            kv_up_device(pk, join_key)

    with jax.named_scope("queries"):
        queries()

    def pass_on(item, j):
        direct_recv(item, j).wait_recv()
        forward(item, j).start()

    with jax.named_scope("pass_on"):
        for j, at in ((1, c > 0), (3, c == 3)):
            @pl.when(jnp.logical_and(k == 1, at))
            def _():
                pass_on(0, j)

    send(1, ((0, 3), (0, 2), (0, 1), (1, 2), (1, 1)))

    def o_copy(mb, half):
        cs = pl.ds(half * 1024, 1024)
        return pltpu.make_async_remote_copy(
            src_ref=oall.at[mb, pl.ds(pl.multiple_of(pk * BLK, BLK), BLK), cs], dst_ref=oin.at[pl.ds(mb * BLK, BLK), cs],
            send_sem=sent.at[1], recv_sem=or_.at[mb * half], device_id=partner, device_id_type=MESH)

    def shared_keys():
        r = jnp.concatenate([kvlat0[0:OWN, KV_LAT:], kvlat0[chip_rows(c), KV_LAT:]], axis=0).T
        for mb in range(2):
            kropeT[mb, 0, :ROPE] = r[mb * ROPE:(mb + 1) * ROPE]
            kropeT[mb, 1, ROPE:] = r[mb * ROPE:(mb + 1) * ROPE]

    def heads(mb, kv_up_first, then={}):
        scores = []
        if mb == 1:
            kv_up_first()
        for h in range(HEADS):
            kcat = jnp.concatenate([kT[mb, h], kropeT[mb, h % 2]], axis=0)
            scores.append(jnp.dot(qbuf[mb, h], kcat, preferred_element_type=F32))
        if mb == 0:
            kv_up_first()
        probs = []
        for h, s in enumerate(scores):
            s = jnp.concatenate([s[:, :OWN], jnp.minimum(s[:, OWN:], causal[...])], axis=1)
            m = jnp.max(s, axis=1, keepdims=True)
            e = jnp.exp2((s - m) * SCALE2)
            probs.append((e * (1.0 / jnp.sum(e, axis=1, keepdims=True))).astype(BF16))
            if h in then:
                then[h]()
        for h in range(HEADS):
            o = jnp.dot(probs[h], vb[mb, h], preferred_element_type=F32)
            oall[mb, :, h * 128:(h + 1) * 128] = o.astype(BF16)
            if mb == 1 and h == 7:
                o_copy(1, 0).start()
        for half in ((0, 1), (1,))[mb]:
            o_copy(mb, half).start()

    def take(ref, n, i):
        with jax.named_scope("take_wait"):
            @pl.when(k == 0)
            def _():
                wait_bytes(ref, n, fr.at[i])

    def pass_if(at, item, j):
        @pl.when(jnp.logical_and(k == 1, at))
        def _():
            pass_on(item, j)

    @pl.when(c > 0)
    def _():
        take(kvlat0, CHIP, 1)
        with jax.named_scope("take1"):
            kv_up_rows(0, chip_rows(c - 1))

    for n in (2, 3):
        @pl.when(c == n)
        def _():
            pass_if(True, 0, 2)
            take(kvlat0, (n - 1) * CHIP, 2)
            with jax.named_scope("take1"):
                kv_up_rows(0, pl.ds(0, (n - 1) * CHIP))
    shared_keys()
    @pl.when(c == 3)
    def _():
        pass_if(True, 1, 1)
        take(kvlat1, CHIP, 3)

    def third_rows():
        kv_up_rows(1, pl.ds(2 * CHIP, CHIP))

    late = jnp.logical_and(k == 1, c == 3)

    @pl.when(late)
    def _():
        with jax.named_scope("heads1"):
            heads(0, third_rows, {6: lambda: pass_on(1, 3), 10: lambda: pass_on(1, 2)})

    @pl.when(jnp.logical_not(late))
    def _():
        with jax.named_scope("heads1"):
            heads(0, third_rows)

    @pl.when(c == 1)
    def _():
        pass_if(True, 1, 1)
        take(kvlat1, CHIP, 3)

    @pl.when(c == 2)
    def _():
        for j in (1, 2):
            pass_if(True, 1, j)
        for i in (3, 4):
            take(kvlat1, CHIP, i)

    @pl.when(c == 3)
    def _():
        take(kvlat1, 2 * CHIP, 4)

    with jax.named_scope("heads2"):
        heads(1, lambda: kv_up_rows(1, pl.ds(0, 2 * CHIP)))

    with jax.named_scope("out"):
        wait_whole(wo_v, 0)
        orow = pl.ds(pl.multiple_of(k * BLK, BLK), BLK)
        mine = jnp.concatenate([oall[0, orow], oall[1, orow]], axis=0)

        @pl.when(k == 0)
        def _():
            wait_bytes(oin, 96, or_.at[0])
            wait_bytes(oin, 32, or_.at[1])
            y[...] = jnp.dot(jnp.concatenate([mine, oin[...]], axis=1), wo_v[...], preferred_element_type=F32).astype(BF16)

        @pl.when(k == 1)
        def _():
            acc[...] = jnp.dot(mine, wo_v[0:2048], preferred_element_type=F32)
            wait_bytes(oin, 96, or_.at[0])
            acc[...] += jnp.dot(oin[:, :1024], wo_v[2048:3072], preferred_element_type=F32)
            wait_bytes(oin, 32, or_.at[1])
            y[...] = (acc[...] + jnp.dot(oin[:, 1024:], wo_v[3072:], preferred_element_type=F32)).astype(BF16)

    for n in range(NCHIP):
        @pl.when(c == n)
        def _():
            wait_bytes(wqd_v, 192 * (NCHIP - 1 - n) + 192 + 384, sent.at[0])

            if n > 0:
                @pl.when(k == 1)
                def _():
                    wait_bytes(wqd_v, 384 * n, sent.at[0])
    wait_bytes(oin, CHIP, sent.at[1])


def store_body(y, y1, y2, sem):
    for i, out in enumerate((y1, y2)):
        pltpu.make_async_copy(y.at[pl.ds(i * BLK, BLK)], out, sem.at[i]).start()
    for i, out in enumerate((y1, y2)):
        pltpu.make_async_copy(y.at[pl.ds(i * BLK, BLK)], out, sem.at[i]).wait()


def store(y):
    any_spec = pl.BlockSpec(memory_space=pl.ANY)
    return pl.pallas_call(
        store_body,
        out_shape=(jax.ShapeDtypeStruct((BLK, D_MODEL), BF16),) * 2,
        in_specs=[any_spec],
        out_specs=(any_spec,) * 2,
        scratch_shapes=[pltpu.SemaphoreType.DMA((2,))],
        compiler_params=pltpu.CompilerParams(vmem_limit_bytes=2**20),
    )(y)


def solution(mesh):
    tok_spec = P(('dp', 'sp'), None)
    idx_spec = P(('dp', 'sp'))
    any_spec = pl.BlockSpec(memory_space=pl.ANY)
    vmem_spec = pl.BlockSpec(memory_space=pltpu.VMEM)

    def local_body(x_one, seg_one, pos_one, x_two, seg_two, pos_two, w_qdown, gain_q, w_qup, w_kvdown, gain_kv, w_kvup, w_out):
        dma = pltpu.SemaphoreType.DMA
        call = pl.pallas_call(
            body,
            out_shape=jax.ShapeDtypeStruct((CHIP, D_MODEL), BF16),
            in_specs=[pl.BlockSpec(memory_space=pltpu.HBM)] * 11,
            out_specs=vmem_spec,
            scratch_shapes=[
                pltpu.VMEM((CHIP, D_MODEL), BF16),
                pltpu.VMEM((2, 1, BLK), jnp.int32),
                pltpu.VMEM((D_MODEL, Q_LAT), BF16),
                pltpu.VMEM((Q_LAT,), BF16),
                pltpu.VMEM((Q_LAT, 3072), BF16),
                pltpu.VMEM((KV_LAT + ROPE, D_MODEL), BF16),
                pltpu.VMEM((KV_LAT,), BF16),
                pltpu.VMEM((KV_LAT, 4096), BF16),
                pltpu.VMEM((4096, D_MODEL), BF16),
                pltpu.VMEM((TOK, KV_LAT + 128), BF16),
                pltpu.VMEM((TOK, KV_LAT), BF16),
                pltpu.VMEM((2 * CHIP, Q_LAT), BF16),
                pltpu.VMEM((3, 2 * CHIP, 128), F32),
                pltpu.VMEM((2, HEADS, CHIP, 256), BF16),
                pltpu.VMEM((HEADS, CHIP, 128), BF16),
                pltpu.VMEM((2, HEADS, 128, TOK), BF16),
                pltpu.VMEM((2, HEADS, TOK, 128), BF16),
                pltpu.VMEM((2, 2, 128, TOK), BF16),
                pltpu.VMEM((2 * CHIP, 128), F32),
                pltpu.VMEM((2 * CHIP, 128), F32),
                pltpu.VMEM((CHIP, CHIP), F32),
                pltpu.VMEM((2, CHIP, 2048), BF16),
                pltpu.VMEM((CHIP, 2048), BF16),
                pltpu.VMEM((CHIP, D_MODEL), F32),
                pltpu.VMEM((CHIP, KV_LAT + ROPE), F32),
                dma((8,)), dma((2,)), dma((2, 3)), dma((5,)), dma((1,)), dma((2,)),
            ],
            compiler_params=pltpu.CompilerParams(collective_id=0, has_side_effects=True, vmem_limit_bytes=52 * 2**20),
        )
        args = (x_one, pos_one.reshape(1, BLK), x_two, pos_two.reshape(1, BLK), w_qdown, gain_q, w_qup,
                w_kvdown.T, gain_kv, w_kvup, w_out)
        y = call(*(pltpu.with_memory_space_constraint(a, pltpu.HBM) for a in args))
        return store(y)

    return jax.shard_map(local_body, mesh=mesh,
                         in_specs=(tok_spec, idx_spec, idx_spec, tok_spec, idx_spec, idx_spec, P(), P(), P(), P(), P(), P(), P()),
                         out_specs=(tok_spec, tok_spec), check_vma=False)
```
